16 devices in a mesh: dp: 4 (over z, y), dap: 4 (over x, core).
Axes of the slice: x: 2, y: 2, z: 2, core: 2. Of those that a mesh axis runs over, the one named last changes fastest.
Arguments:
- pair_act: bfloat16 [4, 256, 256, 128], P('dp', 'dap')
- pair_mask: int32 [4, 256, 256], P('dp', 'dap')
- true_bin: int32 [4, 256, 256], P('dp', 'dap')
- msa_act: bfloat16 [4, 64, 256, 256], P('dp', None, 'dap')
- msa_true: int32 [4, 64, 256], P('dp', None, 'dap')
- bert_mask: int32 [4, 64, 256], P('dp', None, 'dap')
- w_dist: bfloat16 [128, 64], replicated
- b_dist: float32 [64], replicated
- w_msa: bfloat16 [256, 23], replicated
- b_msa: float32 [23], replicated
Outputs:
- output 1: float32 [], replicated
- output 2: bfloat16 [4, 256, 256, 128], P('dp', 'dap')
- output 3: bfloat16 [4, 64, 256, 256], P('dp', None, 'dap')
- output 4: float32 [128, 64], replicated
- output 5: float32 [64], replicated
- output 6: float32 [256, 23], replicated
- output 7: float32 [23], replicated
All inputs are finite; a program needn't handle non-finite values.
Results may differ from the reference program's by a relative error of at most 0.00736713.
Values are sent between devices in bfloat16 or wider.
A program may use at most 1 GiB of HBM per device.

```python
import math
import jax
import jax.numpy as jnp
from jax import lax

BATCH = 4
RES = 256
SEQS = 64
C_Z = 128
C_M = 256
BINS = 64
CLASSES = 23
ROW_BLOCK = math.gcd(RES, 32)
ROW_STEPS = RES // ROW_BLOCK
LOSS_SCALE = 2.0 ** 16
DIST_WEIGHT = 0.3
MSA_WEIGHT = 2.0
DIST_EPS = 1e-6
MSA_EPS = 1e-8


def setup_inputs(seed: int = 0) -> dict:
    rng_keys = jax.random.split(jax.random.key(seed), 13)
    act_scale = jax.random.uniform(rng_keys[0], (BATCH, 1, 1, 1), minval=0.5, maxval=2.0)
    pair_act = (jax.random.normal(rng_keys[1], (BATCH, RES, RES, C_Z)) * act_scale).astype(jnp.bfloat16)
    lengths = jax.random.randint(rng_keys[2], (BATCH, 1), RES // 2, RES + 1)
    positions = jnp.arange(RES)[None, :]
    present = (jax.random.randint(rng_keys[3], (BATCH, RES), 0, 10) > 0) & (positions < lengths)
    pair_mask = (present[:, :, None] & present[:, None, :]).astype(jnp.int32)
    true_bin = jax.random.randint(rng_keys[4], (BATCH, RES, RES), 0, BINS)
    msa_act = jax.random.normal(rng_keys[5], (BATCH, SEQS, RES, C_M)).astype(jnp.bfloat16)
    msa_true = jax.random.randint(rng_keys[6], (BATCH, SEQS, RES), 0, CLASSES)
    block_rate = jax.random.randint(rng_keys[7], (BATCH, 1, RES // 8), 0, 31)
    mask_rate = jnp.repeat(block_rate, 8, axis=2)
    mask_draw = jax.random.randint(rng_keys[8], (BATCH, SEQS, RES), 0, 100)
    bert_mask = ((mask_draw < mask_rate) & (positions < lengths)[:, None, :]).astype(jnp.int32)
    w_dist = (jax.random.normal(rng_keys[9], (C_Z, BINS)) * (1.5 * C_Z ** -0.5)).astype(jnp.bfloat16)
    b_dist = jax.random.normal(rng_keys[10], (BINS,))
    w_msa = (jax.random.normal(rng_keys[11], (C_M, CLASSES)) * (1.5 * C_M ** -0.5)).astype(jnp.bfloat16)
    b_msa = jax.random.normal(rng_keys[12], (CLASSES,))
    return {'pair_act': pair_act, 'pair_mask': pair_mask, 'true_bin': true_bin, 'msa_act': msa_act,
            'msa_true': msa_true, 'bert_mask': bert_mask, 'w_dist': w_dist, 'b_dist': b_dist,
            'w_msa': w_msa, 'b_msa': b_msa}


def class_terms(logits, labels):
    log_prob = jax.nn.log_softmax(logits, axis=-1)
    onehot = jax.nn.one_hot(labels, logits.shape[-1], dtype=jnp.float32)
    return -jnp.sum(log_prob * onehot, axis=-1), jnp.exp(log_prob) - onehot


def reference(pair_act, pair_mask, true_bin, msa_act, msa_true, bert_mask, w_dist, b_dist, w_msa, b_msa):
    starts = jnp.arange(ROW_STEPS) * ROW_BLOCK

    def protein_terms(operands):
        pair_one, mask_one, bin_one, msa_one, true_one, bert_one = operands
        mask_f = mask_one.astype(jnp.float32)
        pair_den = DIST_EPS + jnp.sum(mask_f)
        msa_den = MSA_EPS + jnp.sum(bert_one.astype(jnp.float32))
        dist_scale = LOSS_SCALE * DIST_WEIGHT / BATCH / pair_den
        msa_scale = LOSS_SCALE * MSA_WEIGHT / BATCH / msa_den

        def dist_rows(row_start):
            pair_rows = lax.dynamic_slice_in_dim(pair_one, row_start, ROW_BLOCK, axis=0)
            pair_cols = lax.dynamic_slice_in_dim(pair_one, row_start, ROW_BLOCK, axis=1)
            mask_rows = lax.dynamic_slice_in_dim(mask_f, row_start, ROW_BLOCK, axis=0)
            bin_rows = lax.dynamic_slice_in_dim(bin_one, row_start, ROW_BLOCK, axis=0)
            direct = jnp.dot(pair_rows.reshape(-1, C_Z), w_dist, preferred_element_type=jnp.float32)
            mirror = jnp.dot(pair_cols.reshape(-1, C_Z), w_dist, preferred_element_type=jnp.float32)
            logits = (direct.reshape(ROW_BLOCK, RES, BINS)
                      + jnp.swapaxes(mirror.reshape(RES, ROW_BLOCK, BINS), 0, 1) + b_dist)
            neg_logp, prob_diff = class_terms(logits, bin_rows)
            grad_rows = (prob_diff * (mask_rows * dist_scale)[:, :, None]).astype(jnp.bfloat16)
            return jnp.sum(neg_logp * mask_rows), grad_rows

        dist_sums, grad_blocks = lax.map(dist_rows, starts)
        grad_pair = grad_blocks.reshape(RES, RES, BINS)

        def back_rows(row_start):
            pair_rows = lax.dynamic_slice_in_dim(pair_one, row_start, ROW_BLOCK, axis=0)
            pair_cols = lax.dynamic_slice_in_dim(pair_one, row_start, ROW_BLOCK, axis=1)
            g_rows = lax.dynamic_slice_in_dim(grad_pair, row_start, ROW_BLOCK, axis=0)
            g_cols = lax.dynamic_slice_in_dim(grad_pair, row_start, ROW_BLOCK, axis=1)
            direct = jnp.dot(g_rows.reshape(-1, BINS), w_dist.T, preferred_element_type=jnp.float32)
            mirror = jnp.dot(g_cols.reshape(-1, BINS), w_dist.T, preferred_element_type=jnp.float32)
            grad_rows = (direct.reshape(ROW_BLOCK, RES, C_Z)
                         + jnp.swapaxes(mirror.reshape(RES, ROW_BLOCK, C_Z), 0, 1)).astype(jnp.bfloat16)
            g_swap = jnp.swapaxes(g_rows, 0, 1).reshape(-1, BINS)
            w_part = (jnp.dot(pair_rows.reshape(-1, C_Z).T, g_rows.reshape(-1, BINS), preferred_element_type=jnp.float32)
                      + jnp.dot(pair_cols.reshape(-1, C_Z).T, g_swap, preferred_element_type=jnp.float32))
            return grad_rows, w_part

        grad_z_blocks, w_blocks = lax.map(back_rows, starts)
        grad_z = grad_z_blocks.reshape(RES, RES, C_Z)

        def msa_rows(row_operands):
            act_row, true_row, bert_row = row_operands
            logits = jnp.dot(act_row, w_msa, preferred_element_type=jnp.float32) + b_msa
            neg_logp, prob_diff = class_terms(logits, true_row)
            bert_f = bert_row.astype(jnp.float32)
            grad_row = (prob_diff * (bert_f * msa_scale)[:, None]).astype(jnp.bfloat16)
            grad_act = jnp.dot(grad_row, w_msa.T, preferred_element_type=jnp.float32).astype(jnp.bfloat16)
            w_part = jnp.dot(act_row.T, grad_row, preferred_element_type=jnp.float32)
            return jnp.sum(neg_logp * bert_f), grad_act, w_part, jnp.sum(grad_row.astype(jnp.float32), axis=0)

        msa_sums, grad_m, msa_w_parts, msa_b_parts = lax.map(msa_rows, (msa_one, true_one, bert_one))
        loss_one = DIST_WEIGHT * jnp.sum(dist_sums) / pair_den + MSA_WEIGHT * jnp.sum(msa_sums) / msa_den
        return (loss_one, grad_z, grad_m, jnp.sum(w_blocks, axis=0),
                jnp.sum(grad_pair.astype(jnp.float32), axis=(0, 1)),
                jnp.sum(msa_w_parts, axis=0), jnp.sum(msa_b_parts, axis=0))

    losses, grad_z, grad_m, dist_w, dist_b, msa_w, msa_b = lax.map(
        protein_terms, (pair_act, pair_mask, true_bin, msa_act, msa_true, bert_mask))
    return (jnp.mean(losses), grad_z, grad_m, jnp.sum(dist_w, axis=0), jnp.sum(dist_b, axis=0),
            jnp.sum(msa_w, axis=0), jnp.sum(msa_b, axis=0))
```

```python
import jax
import jax.numpy as jnp
from jax import lax
from jax.experimental import pallas as pl
from jax.experimental.pallas import tpu as pltpu
from jax.sharding import PartitionSpec as P

LOSS_SCALE = 2.0 ** 16
DIST_WEIGHT = 0.3
MSA_WEIGHT = 2.0
DIST_EPS = 1e-6
MSA_EPS = 1e-8
MESH = pl.DeviceIdType.MESH
DSEM = pltpu.SemaphoreType.DMA
KEEP = True
H = 64
L = 128
N = 256
F32 = jnp.float32
BF16 = jnp.bfloat16
I32 = jnp.int32


def dot(a, b, ca, cb):
    return lax.dot_general(a, b, (((ca,), (cb,)), ((), ())), preferred_element_type=F32)


def eye(n, m):
    return lax.broadcasted_iota(I32, (n, m), 0) == lax.broadcasted_iota(I32, (n, m), 1)


def row_to_col(row, n):
    return jnp.sum(jnp.where(eye(n, row.shape[1]), row, 0.0), axis=1, keepdims=KEEP)


def col_to_row(col, m):
    return jnp.sum(jnp.where(eye(col.shape[0], m), col, 0.0), axis=0, keepdims=KEEP)


def lanes2(ref, i):
    return jnp.concatenate([ref[pl.ds(2 * i, 1), :], ref[pl.ds(2 * i + 1, 1), :]], axis=1)


def make_kernel(batch):
    def kernel(z_h, mask_h, tb_h, m_h, mt_h, bm_h, wd_h, bd_h, wm_h, bmb_h,
               loss_o, dz_o, dm_o, dwd_o, dbd_o, dwm_o, dbm_o,
               zv, mv, mask_v, tb_v, mt_v, bm_v, wd_v, bd_v, wm_v, bmb_v,
               wt2, w2, wmt, bias_c, mbias_c, lab, lts, ltr, l1n, l1f, l2n, l2f, mlab,
               cnt_s, cnt_r, rz, f0, f1, ntn, ntf, dwd_acc, dwm_acc, dbd_acc, dbm_acc, nll_acc,
               ps, pa, ph, pb, pc, pd, pf,
               lsem, cs, cr, ls, lr, zs, zr, ars, arr):
        dp = lax.axis_index("dp")
        d = lax.axis_index("dap")
        chip, core = d // 2, d % 2
        dap_peer = {1: chip * 2 + (1 - core), 2: (1 - chip) * 2 + core, 3: (1 - chip) * 2 + (1 - core)}
        pz, py = dp // 2, dp % 2
        dp_peer = {1: pz * 2 + (1 - py), 2: (1 - pz) * 2 + py, 3: (1 - pz) * 2 + (1 - py)}
        near = pl.multiple_of(chip * L, L)
        far = pl.multiple_of((1 - chip) * L, L)

        loc = []
        for n, (src, dst) in enumerate([(mask_h, mask_v), (tb_h, tb_v), (bm_h, bm_v), (mt_h, mt_v), (wd_h, wd_v),
                                        (bd_h, bd_v), (wm_h, wm_v), (bmb_h, bmb_v), (m_h, mv), (z_h, zv)]):
            c = pltpu.make_async_copy(src, dst, lsem.at[n])
            c.start()
            loc.append(c)

        bar = pltpu.get_barrier_semaphore()
        for k in (1, 2, 3):
            pl.semaphore_signal(bar, inc=1, device_id=(dp, dap_peer[k]), device_id_type=MESH)
            pl.semaphore_signal(bar, inc=1, device_id=(dp_peer[k], d), device_id_type=MESH)

        for n in range(4):
            loc[n].wait()
        maskf = mask_v[:].astype(F32)
        bertf = bm_v[:].astype(F32)
        cd = jnp.sum(jnp.sum(maskf, axis=0, keepdims=KEEP), axis=1, keepdims=KEEP)
        cm = jnp.sum(jnp.sum(bertf, axis=0, keepdims=KEEP), axis=1, keepdims=KEEP)
        cnt_s[0:8, :] = jnp.broadcast_to(cd, (8, L))
        cnt_s[8:16, :] = jnp.broadcast_to(cm, (8, L))
        labv = jnp.where(mask_v[:] > 0, tb_v[:], H)
        lab[:] = labv
        labf = labv.astype(F32)
        lts[:] = jnp.concatenate([labf, labf], axis=0).T

        pl.semaphore_wait(bar, 6)

        def rcopy(src, dst, s, r, dpi, dapi):
            return pltpu.make_async_remote_copy(src_ref=src, dst_ref=dst, send_sem=s, recv_sem=r,
                                                device_id=(dpi, dapi), device_id_type=MESH)

        sends = []
        cc, lc, zc = {}, {}, {}
        for k in (2, 3, 1):
            cc[k] = rcopy(cnt_s, cnt_r.at[k - 1], cs.at[k - 1], cr.at[k - 1], dp, dap_peer[k])
            cc[k].start()
        for k in (2, 3, 1):
            lc[k] = rcopy(lts.at[pl.ds(pl.multiple_of(H * dap_peer[k], H), H), :], ltr.at[k - 1],
                          ls.at[k - 1], lr.at[k - 1], dp, dap_peer[k])
            lc[k].start()
        for q in range(4):
            for k in (2, 3, 1):
                cols = pl.multiple_of(H * dap_peer[k] + 16 * q, 16)
                zc[k, q] = rcopy(z_h.at[:, pl.ds(cols, 16), :], rz.at[k - 1, q],
                                 zs.at[k - 1, q], zr.at[k - 1, q], dp, dap_peer[k])
                zc[k, q].start()


        for n in range(4, 8):
            loc[n].wait()
        wt = wd_v[:]
        wt2[:, 0:L] = wt
        wt2[:, L:N] = wt
        w2[0:H, :] = wt
        w2[H:L, :] = wt
        wmt[:] = jnp.zeros_like(wmt)
        wmt[0:23, :] = wm_v[:]
        bias_c[:] = jnp.broadcast_to(row_to_col(bd_v[:], H), (H, L))
        pad = lax.broadcasted_iota(I32, (32, 1), 0) >= 23
        mbias_c[:] = jnp.broadcast_to(jnp.where(pad, -1e30, row_to_col(bmb_v[:], 32)), (32, L))
        l1n[:] = lab[:, pl.ds(near, L)]
        l1f[:] = lab[:, pl.ds(far, L)]
        mlv = jnp.where(bm_v[:] > 0, mt_v[:], H)
        bm_v[:] = mlv
        mlab[:] = jnp.concatenate([bm_v[pl.ds(0, 32, stride=2), :], bm_v[pl.ds(1, 32, stride=2), :]], axis=1)
        for a in (dwd_acc, dwm_acc, dbd_acc, dbm_acc, nll_acc):
            a[:] = jnp.zeros_like(a)

        for k in (1, 2, 3):
            cc[k].wait_recv()
        tot = (cnt_s[:] + cnt_r[0]) + (cnt_r[1] + cnt_r[2])
        den_d = DIST_EPS + tot[0:1, :]
        den_m = MSA_EPS + tot[8:9, :]
        cvd = (LOSS_SCALE * DIST_WEIGHT / batch) / den_d
        cvm = (LOSS_SCALE * MSA_WEIGHT / batch) / den_m
        cd2 = jnp.concatenate([cvd, cvd], axis=1)
        cm2 = jnp.concatenate([cvm, cvm], axis=1)

        def fold(a):
            return a[:, 0:L] + a[:, L:N]


        loc[8].wait()

        def msa(i, carry):
            m = mv[pl.ds(pl.multiple_of(N * i, N), N), :]
            b = mbias_c[:]
            l = dot(wmt[:], m, 1, 1) + jnp.concatenate([b, b], axis=1)
            t = lanes2(mlab, i)
            mx = jnp.max(l, axis=0, keepdims=KEEP)
            e = jnp.exp(l - mx)
            s = jnp.sum(e, axis=0, keepdims=KEEP)
            eq = lax.broadcasted_iota(I32, (32, N), 0) == t
            mk = (t < H).astype(F32)
            c = cm2 * mk
            h = (e * (c / s) - jnp.where(eq, c, 0.0)).astype(BF16)
            lt = jnp.sum(jnp.where(eq, l, 0.0), axis=0, keepdims=KEEP)
            nll_acc[1:2, :] += fold(mk * (mx + jnp.log(s)) - lt)
            dbm_acc[:] += fold(h.astype(F32))
            dm_o[pl.ds(pl.multiple_of(N * i, N), N), :] = dot(h, wmt[:], 0, 0).astype(BF16)
            dwm_acc[:] += dot(h, m, 1, 0)
            return carry

        lax.fori_loop(0, 16, msa, 0)


        for k in (1, 2, 3):
            lc[k].wait_recv()
        sel = (lax.broadcasted_iota(I32, (H, L), 1) < H) == (core == 0)
        own_lt = lts[pl.ds(pl.multiple_of(H * d, H), H), :]
        l2n[:] = jnp.where(sel, own_lt, ltr[0]).astype(I32)
        l2f[:] = jnp.where(sel, ltr[1], ltr[2]).astype(I32)

        def swap(src, nt, q, off):
            chunk = src.astype(F32)
            f0[:] = chunk[:, 0:8, :].reshape(512, L)
            f1[:] = chunk[:, 8:16, :].reshape(512, L)
            for t in range(8):
                nt[16 * q + t, pl.ds(off, H), :] = f0[pl.ds(t, H, stride=8), :].astype(BF16)
                nt[16 * q + 8 + t, pl.ds(off, H), :] = f1[pl.ds(t, H, stride=8), :].astype(BF16)

        def tile(i, cols, nt, la, lb):
            zx = zv[pl.ds(2 * i, 2), pl.ds(cols, L), :].reshape(N, L)
            nx = nt[pl.ds(2 * i, 2), :, :].reshape(N, L)
            b = bias_c[:]
            l = dot(wt2[:], jnp.concatenate([zx, nx], axis=1), 1, 1) + jnp.concatenate([b, b], axis=1)
            t1 = lanes2(la, i)
            t2 = lanes2(lb, i)
            mx = jnp.max(l, axis=0, keepdims=KEEP)
            e = jnp.exp(l - mx)
            s = jnp.sum(e, axis=0, keepdims=KEEP)
            bins = lax.broadcasted_iota(I32, (H, N), 0)
            eq1 = bins == t1
            m1 = (t1 < H).astype(F32)
            c1 = cd2 * m1
            c2 = cd2 * (t2 < H).astype(F32)
            g1 = (e * (c1 / s) - jnp.where(eq1, c1, 0.0)).astype(BF16)
            g2 = (e * (c2 / s) - jnp.where(bins == t2, c2, 0.0)).astype(BF16)
            lt = jnp.sum(jnp.where(eq1, l, 0.0), axis=0, keepdims=KEEP)
            nll_acc[0:1, :] += fold(m1 * (mx + jnp.log(s)) - lt)
            dbd_acc[:] += fold(g1.astype(F32))
            g = jnp.concatenate([g1, g2], axis=0)
            dz_o[pl.ds(2 * i, 2), pl.ds(cols, L), :] = dot(g, w2[:], 0, 0).astype(BF16).reshape(2, L, L)
            dwd_acc[:] += dot(g, zx, 1, 0)

        own_off = pl.multiple_of(H * core, H)
        oth_off = pl.multiple_of(H * (1 - core), H)
        loc[9].wait()
        for q in range(4):
            swap(zv[:, pl.ds(pl.multiple_of(H * d + 16 * q, 16), 16), :], ntn, q, own_off)
        for q in range(4):
            zc[1, q].wait_recv()
            swap(rz[0, q], ntn, q, oth_off)

        def near_tile(i, carry):
            tile(i, near, ntn, l1n, l2n)
            return carry

        lax.fori_loop(0, 32, near_tile, 0)

        def far_tile(i, carry):
            tile(i, far, ntf, l1f, l2f)
            return carry

        for q in range(4):
            zc[2, q].wait_recv()
            swap(rz[1, q], ntf, q, own_off)
            zc[3, q].wait_recv()
            swap(rz[2, q], ntf, q, oth_off)
            lax.fori_loop(8 * q, 8 * q + 8, far_tile, 0)


        ps[0:H, :] = dwd_acc[0:H, :] + dwd_acc[H:L, :]
        ps[H:88, :] = dwm_acc[0:24, 0:L]
        ps[88:112, :] = dwm_acc[0:24, L:N]
        nd = jnp.sum(nll_acc[0:1, :], axis=1, keepdims=KEEP)
        nm = jnp.sum(nll_acc[1:2, :], axis=1, keepdims=KEEP)
        part = (DIST_WEIGHT * nd / den_d + MSA_WEIGHT * nm / den_m) / batch
        ps[112:113, :] = col_to_row(jnp.sum(dbd_acc[:], axis=1, keepdims=KEEP), L)
        ps[113:114, :] = col_to_row(jnp.sum(dbm_acc[:], axis=1, keepdims=KEEP), L)
        ps[114:115, :] = part
        ps[115:L, :] = jnp.zeros((13, L), F32)

        mine = pl.ds(pl.multiple_of(H * core, H), H)
        other = pl.ds(pl.multiple_of(H * (1 - core), H), H)
        ca = rcopy(ps.at[other, :], pa, ars.at[0], arr.at[0], dp, dap_peer[1])
        ca.start()
        ca.wait_recv()
        ph[:] = ps[mine, :] + pa[:]
        cb = {}
        for k in (3, 1, 2):
            cb[k] = rcopy(ph, pb.at[k - 1], ars.at[k], arr.at[k], dp_peer[k], d)
            cb[k].start()
        for k in (1, 2, 3):
            cb[k].wait_recv()
        pc[0] = (ph[:] + pb[0]) + (pb[1] + pb[2])
        cx = rcopy(pc.at[0], pc.at[1], ars.at[4], arr.at[4], dp, dap_peer[2])
        cx.start()
        cx.wait_recv()
        pd[:] = pc[0] + pc[1]
        ce = rcopy(pd, pf, ars.at[5], arr.at[5], dp, dap_peer[1])
        ce.start()
        ce.wait_recv()
        first = core == 0
        ra = jnp.where(first, pd[:], pf[:])
        rb = jnp.where(first, pf[:], pd[:])
        dwd_o[:] = ra
        dwm_o[:, 0:L] = rb[0:23, :]
        dwm_o[:, L:N] = rb[24:47, :]
        dbd_o[:] = rb[48:49, 0:H]
        dbm_o[:] = rb[49:50, 0:23]
        loss_o[:] = rb[50:51, 0:1]

        for k in (1, 2, 3):
            cc[k].wait_send()
            lc[k].wait_send()
            cb[k].wait_send()
            for q in range(4):
                zc[k, q].wait_send()
        ca.wait_send()
        cx.wait_send()
        ce.wait_send()

    return kernel


def flush_kernel(*refs):
    ins, outs, sem = refs[:7], refs[7:14], refs[14]
    copies = [pltpu.make_async_copy(a, b, sem.at[n]) for n, (a, b) in enumerate(zip(ins, outs))]
    for n in (1, 2, 0, 3, 4, 5, 6):
        copies[n].start()
    for c in copies:
        c.wait()


def solution(mesh):
    dp_size = mesh.shape["dp"]
    pair_spec = P("dp", "dap", None, None)
    pair_int_spec = P("dp", "dap", None)
    msa_spec = P("dp", None, "dap", None)
    msa_int_spec = P("dp", None, "dap")
    V = pltpu.VMEM

    def local_step(z, mask, tb, m, mt, bm, wd, bd, wm, bmb):
        args = (z.reshape(H, N, L), mask.reshape(H, N), tb.reshape(H, N), m.reshape(4096, N),
                mt.reshape(H, H), bm.reshape(H, H), wd.T, bd.reshape(1, H), wm.T, bmb.reshape(1, 23))
        args = tuple(pltpu.with_memory_space_constraint(a, pltpu.HBM) for a in args)
        shapes = [((1, 1), F32), ((H, N, L), BF16), ((4096, N), BF16), ((H, L), F32), ((1, H), F32),
                  ((23, N), F32), ((1, 23), F32)]
        scratch = [
            V((H, N, L), BF16), V((4096, N), BF16), V((H, N), I32), V((H, N), I32), V((H, H), I32),
            V((H, H), I32), V((H, L), BF16), V((1, H), F32), V((23, N), BF16), V((1, 23), F32),
            V((H, N), BF16), V((L, L), BF16), V((32, N), BF16), V((H, L), F32), V((32, L), F32),
            V((H, N), I32), V((N, L), F32), V((3, H, L), F32), V((H, L), I32), V((H, L), I32),
            V((H, L), I32), V((H, L), I32), V((32, L), I32),
            V((16, L), F32), V((3, 16, L), F32), V((3, 4, H, 16, L), BF16), V((512, L), F32), V((512, L), F32),
            V((H, L, L), BF16), V((H, L, L), BF16), V((L, L), F32), V((32, N), F32), V((H, L), F32),
            V((32, L), F32), V((8, L), F32),
            V((L, L), F32), V((H, L), F32), V((H, L), F32), V((3, H, L), F32), V((2, H, L), F32),
            V((H, L), F32), V((H, L), F32),
            DSEM((10,)),
            DSEM((3,)), DSEM((3,)), DSEM((3,)),
            DSEM((3,)), DSEM((3, 4)), DSEM((3, 4)),
            DSEM((6,)), DSEM((6,)),
        ]
        outs = pl.pallas_call(
            make_kernel(dp_size),
            out_shape=[pltpu.VMEM(s, t) for s, t in shapes],
            in_specs=[pl.BlockSpec(memory_space=pltpu.HBM)] * 10,
            out_specs=[pl.BlockSpec(memory_space=pltpu.VMEM)] * 7,
            scratch_shapes=scratch,
            compiler_params=pltpu.CompilerParams(collective_id=0, has_side_effects=True,
                                                 vmem_limit_bytes=44 * 1024 * 1024),
        )(*args)
        outs = pl.pallas_call(
            flush_kernel,
            out_shape=[jax.ShapeDtypeStruct(s, t) for s, t in shapes],
            in_specs=[pl.BlockSpec(memory_space=pltpu.VMEM)] * 7,
            out_specs=[pl.BlockSpec(memory_space=pl.ANY)] * 7,
            scratch_shapes=[DSEM((7,))],
            compiler_params=pltpu.CompilerParams(vmem_limit_bytes=8 * 1024 * 1024),
        )(*outs)
        loss, dz, dm, dwd, dbd, dwm, dbm = outs
        return (loss.reshape(()), dz.reshape(1, H, N, L), dm.reshape(1, H, H, N), dwd.T, dbd.reshape(H),
                dwm.T, dbm.reshape(23))

    return jax.shard_map(local_step, mesh=mesh,
                         in_specs=(pair_spec, pair_int_spec, pair_int_spec, msa_spec, msa_int_spec, msa_int_spec,
                                   P(), P(), P(), P()),
                         out_specs=(P(), pair_spec, msa_spec, P(), P(), P(), P()),
                         check_vma=False)
```

```python
import jax
import jax.numpy as jnp
from jax import lax
from jax.experimental import pallas as pl
from jax.experimental.pallas import tpu as pltpu
from jax.sharding import PartitionSpec as P

LOSS_SCALE = 2.0 ** 16
DIST_WEIGHT = 0.3
MSA_WEIGHT = 2.0
DIST_EPS = 1e-6
MSA_EPS = 1e-8
MESH = pl.DeviceIdType.MESH
DSEM = pltpu.SemaphoreType.DMA
KEEP = True
Q = 32
EARLY = 2
PEERS = (1, 2, 3)
FAR = (2, 3)
BOTH = (0, 1)
QUARTERS = range(4)
H = 64
L = 128
N = 256
F32 = jnp.float32
BF16 = jnp.bfloat16
I32 = jnp.int32


def dot(a, b, ca, cb):
    return lax.dot_general(a, b, (((ca,), (cb,)), ((), ())), preferred_element_type=F32)


def eye(n, m):
    return lax.broadcasted_iota(I32, (n, m), 0) == lax.broadcasted_iota(I32, (n, m), 1)


def row_to_col(row, n):
    return jnp.sum(jnp.where(eye(n, row.shape[1]), row, 0.0), axis=1, keepdims=KEEP)


def col_to_row(col, m):
    return jnp.sum(jnp.where(eye(col.shape[0], m), col, 0.0), axis=0, keepdims=KEEP)


def lanes2(ref, i):
    return jnp.concatenate([ref[pl.ds(2 * i, 1), :], ref[pl.ds(2 * i + 1, 1), :]], axis=1)


def make_kernel(batch):
    def kernel(z_h, mask_h, tb_h, m_h, mt_h, bm_h, wd_h, bd_h, wm_h, bmb_h,
               loss_o, dz_o, dm_o, dwd_o, dbd_o, dwm_o, dbm_o,
               zv, mv, mask_v, tb_v, mt_v, bm_v, wd_v, bd_v, wm_v, bmb_v,
               wt2, w2, wmt, bias_c, mbias_c, lab, lts, ltp, ltr, l1n, l2n, t1o, t2o, t1r, t2r, mlab,
               cnt_s, cnt_r, rn, rz, f0, f1, ntn, ntf, vb, vr, db, dr, dwd_acc, dwm_acc, dbd_acc, dbm_acc, nll_acc,
               ps, pa, ph, px, pb, pc, pd, pf,
               lsem, cs, cr, ls, lr, ns, nr, zs, zr, vs, vrs, ds, drs, ars, arr):
        dp = lax.axis_index("dp")
        d = lax.axis_index("dap")
        chip, core = d // 2, d % 2
        dap_peer = {1: chip * 2 + (1 - core), 2: (1 - chip) * 2 + core, 3: (1 - chip) * 2 + (1 - core)}
        pz, py = dp // 2, dp % 2
        dp_peer = {1: pz * 2 + (1 - py), 2: (1 - pz) * 2 + py, 3: (1 - pz) * 2 + (1 - py)}
        near = pl.multiple_of(chip * L, L)
        far = pl.multiple_of((1 - chip) * L, L)
        half = (chip, 1 - chip)
        phalf = (1 - chip, chip)
        base = {k: pl.multiple_of(H * dap_peer[k], H) for k in PEERS}

        loc = []
        for n, (src, dst) in enumerate([(mask_h, mask_v), (tb_h, tb_v), (bm_h, bm_v), (mt_h, mt_v), (wd_h, wd_v),
                                        (bd_h, bd_v), (wm_h, wm_v), (bmb_h, bmb_v), (m_h, mv), (z_h, zv)]):
            c = pltpu.make_async_copy(src, dst, lsem.at[n])
            c.start()
            loc.append(c)

        bar = pltpu.get_barrier_semaphore()
        for k in PEERS:
            pl.semaphore_signal(bar, inc=1, device_id=(dp, dap_peer[k]), device_id_type=MESH)
            pl.semaphore_signal(bar, inc=1, device_id=(dp_peer[k], d), device_id_type=MESH)

        for n in QUARTERS:
            loc[n].wait()
        maskf = mask_v[:].astype(F32)
        bertf = bm_v[:].astype(F32)
        cd = jnp.sum(jnp.sum(maskf, axis=0, keepdims=KEEP), axis=1, keepdims=KEEP)
        cm = jnp.sum(jnp.sum(bertf, axis=0, keepdims=KEEP), axis=1, keepdims=KEEP)
        cnt_s[0:8, :] = jnp.broadcast_to(cd, (8, L))
        cnt_s[8:16, :] = jnp.broadcast_to(cm, (8, L))
        labv = jnp.where(mask_v[:] > 0, tb_v[:], H)
        lab[:] = labv
        labf = labv.astype(F32)
        lts[:] = jnp.concatenate([labf, labf], axis=0).T
        low = lax.broadcasted_iota(I32, (Q, L), 1) < H
        for p in QUARTERS:
            ltp[p] = jnp.where(low, lts[H * p:H * p + Q, :], lts[H * p + Q:H * p + H, :])

        pl.semaphore_wait(bar, 6)

        def rcopy(src, dst, s, r, dpi, dapi):
            return pltpu.make_async_remote_copy(src_ref=src, dst_ref=dst, send_sem=s, recv_sem=r,
                                                device_id=(dpi, dapi), device_id_type=MESH)

        sends = []
        cc, lc, zc = {}, {}, {}
        for k in (2, 3, 1):
            cc[k] = rcopy(cnt_s, cnt_r.at[k - 1], cs.at[k - 1], cr.at[k - 1], dp, dap_peer[k])
            cc[k].start()
        for k in (2, 3, 1):
            lc[k] = rcopy(ltp.at[dap_peer[k]], ltr.at[k - 1],
                          ls.at[k - 1], lr.at[k - 1], dp, dap_peer[k])
            lc[k].start()
        nc = {}
        for q in QUARTERS:
            nc[q] = rcopy(z_h.at[:, pl.ds(pl.multiple_of(base[1] + 16 * q, 16), 16), :], rn.at[q],
                          ns.at[q], nr.at[q], dp, dap_peer[1])
            for k in FAR:
                for b in BOTH:
                    cols = pl.multiple_of(base[k] + Q * phalf[b] + 8 * q, 8)
                    zc[k, q, b] = rcopy(z_h.at[Q * b:Q * b + Q, pl.ds(cols, 8), :], rz.at[k - 2, q, b],
                                        zs.at[k - 2, q, b], zr.at[k - 2, q, b], dp, dap_peer[k])
                    zc[k, q, b].start()
            nc[q].start()
        for n in range(4, 8):
            loc[n].wait()
        wt = wd_v[:]
        wt2[:, 0:L] = wt
        wt2[:, L:N] = wt
        w2[0:H, :] = wt
        w2[H:L, :] = wt
        wmt[:] = jnp.zeros_like(wmt)
        wmt[0:23, :] = wm_v[:]
        bias_c[:] = jnp.broadcast_to(row_to_col(bd_v[:], H), (H, L))
        pad = lax.broadcasted_iota(I32, (32, 1), 0) >= 23
        mbias_c[:] = jnp.broadcast_to(jnp.where(pad, -1e30, row_to_col(bmb_v[:], 32)), (32, L))
        l1n[:] = lab[:, pl.ds(near, L)]
        mlv = jnp.where(bm_v[:] > 0, mt_v[:], H)
        bm_v[:] = mlv
        mlab[:] = jnp.concatenate([bm_v[pl.ds(0, 32, stride=2), :], bm_v[pl.ds(1, 32, stride=2), :]], axis=1)
        for a in (dwd_acc, dwm_acc, dbd_acc, dbm_acc, nll_acc):
            a[:] = jnp.zeros_like(a)

        for k in PEERS:
            cc[k].wait_recv()
        tot = (cnt_s[:] + cnt_r[0]) + (cnt_r[1] + cnt_r[2])
        den_d = DIST_EPS + tot[0:1, :]
        den_m = MSA_EPS + tot[8:9, :]
        cvd = (LOSS_SCALE * DIST_WEIGHT / batch) / den_d
        cvm = (LOSS_SCALE * MSA_WEIGHT / batch) / den_m
        cd2 = jnp.concatenate([cvd, cvd], axis=1)
        cm2 = jnp.concatenate([cvm, cvm], axis=1)

        def fold(a):
            return a[:, 0:L] + a[:, L:N]


        loc[8].wait()

        def msa(i, carry):
            m = mv[pl.ds(pl.multiple_of(N * i, N), N), :]
            b = mbias_c[:]
            l = dot(wmt[:], m, 1, 1) + jnp.concatenate([b, b], axis=1)
            t = lanes2(mlab, i)
            mx = jnp.max(l, axis=0, keepdims=KEEP)
            e = jnp.exp(l - mx)
            s = jnp.sum(e, axis=0, keepdims=KEEP)
            eq = lax.broadcasted_iota(I32, (32, N), 0) == t
            mk = (t < H).astype(F32)
            c = cm2 * mk
            h = (e * (c / s) - jnp.where(eq, c, 0.0)).astype(BF16)
            lt = jnp.sum(jnp.where(eq, l, 0.0), axis=0, keepdims=KEEP)
            nll_acc[1:2, :] += fold(mk * (mx + jnp.log(s)) - lt)
            dbm_acc[:] += fold(h.astype(F32))
            dm_o[pl.ds(pl.multiple_of(N * i, N), N), :] = dot(h, wmt[:], 0, 0).astype(BF16)
            dwm_acc[:] += dot(h, m, 1, 0)
            return carry

        lax.fori_loop(0, 16, msa, 0)


        for k in PEERS:
            lc[k].wait_recv()
        def turn(a):
            return pltpu.roll(a, H, 1)

        def unpack(p):
            return jnp.concatenate([jnp.where(low, p, turn(p)), jnp.where(low, turn(p), p)], axis=0)

        def paired(a):
            back = jnp.concatenate([pltpu.roll(a[8 * q:8 * q + 8, :], 4, 0) for q in QUARTERS], axis=0)
            return jnp.where(low, a, back).astype(I32)

        lane = lax.broadcasted_iota(I32, (Q, L), 1)
        upper = (lane % H >= Q).astype(I32)
        mine_low = upper == chip
        peer_low = upper == 1 - chip
        wide = lax.broadcasted_iota(I32, (H, L), 1) < H
        own_lt = lts[pl.ds(pl.multiple_of(H * d, H), H), :]
        l2n[:] = jnp.where(wide == (core == 0), own_lt, unpack(ltr[0])).astype(I32)
        l1f = lab[:, pl.ds(far, L)].astype(F32)
        for k in FAR:
            a = jnp.where(wide == (dap_peer[k] % 2 == 0), l1f, turn(l1f))
            t1o[k - 2] = paired(jnp.where(mine_low, a[0:Q, :], a[Q:H, :]))
            got = ltr[k - 1]
            t2o[k - 2] = paired(jnp.where(low == mine_low, got, turn(got)))
            sent = ltp[dap_peer[k]]
            t1r[k - 2] = paired(jnp.where(low == peer_low, sent, turn(sent)))
            u = unpack(got)
            u = jnp.concatenate([u, u], axis=0).T
            t2r[k - 2] = paired(jnp.where(peer_low, u[0:Q, :], u[Q:H, :]))

        def swap(src, nt, q, off):
            chunk = src.astype(F32)
            f0[:] = chunk[:, 0:8, :].reshape(512, L)
            f1[:] = chunk[:, 8:16, :].reshape(512, L)
            for t in range(8):
                nt[16 * q + t, pl.ds(off, H), :] = f0[pl.ds(t, H, stride=8), :].astype(BF16)
                nt[16 * q + 8 + t, pl.ds(off, H), :] = f1[pl.ds(t, H, stride=8), :].astype(BF16)

        bins = lax.broadcasted_iota(I32, (H, N), 0)

        def softmax_terms(zx, nx):
            b = bias_c[:]
            l = dot(wt2[:], jnp.concatenate([zx, nx], axis=1), 1, 1) + jnp.concatenate([b, b], axis=1)
            mx = jnp.max(l, axis=0, keepdims=KEEP)
            e = jnp.exp(l - mx)
            s = jnp.sum(e, axis=0, keepdims=KEEP)
            return l, e, s, mx + jnp.log(s)

        def near_tile(i, carry):
            zx = zv[pl.ds(2 * i, 2), pl.ds(near, L), :].reshape(N, L)
            nx = ntn[pl.ds(2 * i, 2), :, :].reshape(N, L)
            l, e, s, lse = softmax_terms(zx, nx)
            t1 = lanes2(l1n, i)
            t2 = lanes2(l2n, i)
            eq1 = bins == t1
            m1 = (t1 < H).astype(F32)
            c1 = cd2 * m1
            c2 = cd2 * (t2 < H).astype(F32)
            g1 = (e * (c1 / s) - jnp.where(eq1, c1, 0.0)).astype(BF16)
            g2 = (e * (c2 / s) - jnp.where(bins == t2, c2, 0.0)).astype(BF16)
            lt = jnp.sum(jnp.where(eq1, l, 0.0), axis=0, keepdims=KEEP)
            nll_acc[0:1, :] += fold(m1 * lse - lt)
            dbd_acc[:] += fold(g1.astype(F32))
            g = jnp.concatenate([g1, g2], axis=0)
            dz_o[pl.ds(2 * i, 2), pl.ds(near, L), :] = dot(g, w2[:], 0, 0).astype(BF16).reshape(2, L, L)
            dwd_acc[:] += dot(g, zx, 1, 0)
            return carry

        def own_tiles(k, q):
            for b in BOTH:
                zc[k, q, b].wait_recv()
                f0[0:N, :] = rz[k - 2, q, b].astype(F32).reshape(N, L)
                for t in range(8):
                    r = H * (t // 4) + Q * b
                    ntf[k - 2, 4 * q + t % 4, r:r + Q, :] = f0[pl.ds(t, Q, stride=8), :].astype(BF16)

            def body(j, carry):
                spots = [(8 * q + 4 * u + 2 * j + tt + Q * half[b], pl.multiple_of(base[k] + Q * b, Q))
                         for tt in BOTH for u in BOTH for b in BOTH]
                zx = jnp.concatenate([zv[r, pl.ds(c, Q), :] for r, c in spots], axis=0)
                nx = ntf[k - 2, pl.ds(4 * q + 2 * j, 2), :, :].reshape(N, L)
                l, e, s, lse = softmax_terms(zx, nx)
                t1 = lanes2(t1o.at[k - 2], 4 * q + j)
                t2 = lanes2(t2o.at[k - 2], 4 * q + j)
                eq1 = bins == t1
                eq2 = bins == t2
                m1 = (t1 < H).astype(F32)
                m2 = (t2 < H).astype(F32)
                v = e * (cd2 / s)
                w = v - cd2
                d1 = jnp.sum(jnp.where(eq1, w, 0.0), axis=0, keepdims=KEEP)
                d2 = jnp.sum(jnp.where(eq2, w, 0.0), axis=0, keepdims=KEEP)
                g1 = (jnp.where(eq1, w, v) * m1).astype(BF16)
                g2 = (jnp.where(eq2, w, v) * m2).astype(BF16)
                lt = jnp.sum(jnp.where(eq1, l, 0.0) + jnp.where(eq2, l, 0.0), axis=0, keepdims=KEEP)
                nll_acc[0:1, :] += fold((m1 + m2) * lse - lt)
                dbd_acc[:] += fold(g1.astype(F32) + g2.astype(F32))
                vh = v.astype(BF16)
                for tt in BOTH:
                    cut = slice(L * tt, L * tt + L)
                    vb[k - 2, q, 2 * j + tt] = vh[:, cut]
                    db[k - 2, q, pl.ds(2 * j + tt, 1), :] = d1[:, cut]
                    db[k - 2, q, pl.ds(4 + 2 * j + tt, 1), :] = d2[:, cut]
                g = jnp.concatenate([g1, g2], axis=0)
                dz = dot(g, w2[:], 0, 0).astype(BF16)
                for n, (r, c) in enumerate(spots):
                    dz_o[r, pl.ds(c, Q), :] = dz[Q * n:Q * n + Q, :]
                dwd_acc[:] += dot(g, zx, 1, 0) + dot(g, nx, 1, 0)
                return carry

            lax.fori_loop(0, 2, body, 0)

        vc, dc = {}, {}

        def give(k, q):
            vc[k, q] = rcopy(vb.at[k - 2, q], vr.at[k - 2, q], vs.at[k - 2, q], vrs.at[k - 2, q], dp, dap_peer[k])
            dc[k, q] = rcopy(db.at[k - 2, q], dr.at[k - 2, q], ds.at[k - 2, q], drs.at[k - 2, q], dp, dap_peer[k])
            vc[k, q].start()
            dc[k, q].start()

        def take(k, q):
            vc[k, q].wait_recv()
            dc[k, q].wait_recv()
            for j in BOTH:
                v = jnp.concatenate([vr[k - 2, q, 2 * j], vr[k - 2, q, 2 * j + 1]], axis=1).astype(F32)
                gs = []
                for table, row in ((t1r, 4 + 2 * j), (t2r, 2 * j)):
                    t = lanes2(table.at[k - 2], 4 * q + j)
                    on = jnp.concatenate([dr[k - 2, q, row:row + 1, :], dr[k - 2, q, row + 1:row + 2, :]], axis=1)
                    gs.append((jnp.where(bins == t, on, v) * (t < H).astype(F32)).astype(BF16))
                dz = dot(jnp.concatenate(gs, axis=0), w2[:], 0, 0)
                for tt in BOTH:
                    for u in BOTH:
                        for f, r in ((f0, L * tt + H * u), (f1, L * tt + H * u + Q)):
                            f[pl.ds(4 * u + 2 * j + tt, Q, stride=8), :] = dz[r:r + Q, :]
            for b, f in ((0, f0), (1, f1)):
                cols = pl.multiple_of(base[k] + Q * phalf[b] + 8 * q, 8)
                dz_o[Q * b:Q * b + Q, pl.ds(cols, 8), :] = f[0:N, :].reshape(Q, 8, L).astype(BF16)

        own_off = pl.multiple_of(H * core, H)
        oth_off = pl.multiple_of(H * (1 - core), H)
        loc[9].wait()
        for q in QUARTERS:
            swap(zv[:, pl.ds(pl.multiple_of(H * d + 16 * q, 16), 16), :], ntn, q, own_off)
        for q in QUARTERS:
            nc[q].wait_recv()
            swap(rn[q], ntn, q, oth_off)
        lax.fori_loop(0, 32, near_tile, 0)

        for q in QUARTERS:
            for k in FAR:
                own_tiles(k, q)
                if q < EARLY:
                    give(k, q)

        ps[0:H, :] = dwd_acc[0:H, :] + dwd_acc[H:L, :]
        ps[H:88, :] = dwm_acc[0:24, 0:L]
        ps[88:112, :] = dwm_acc[0:24, L:N]
        nd = jnp.sum(nll_acc[0:1, :], axis=1, keepdims=KEEP)
        nm = jnp.sum(nll_acc[1:2, :], axis=1, keepdims=KEEP)
        part = (DIST_WEIGHT * nd / den_d + MSA_WEIGHT * nm / den_m) / batch
        ps[112:113, :] = col_to_row(jnp.sum(dbd_acc[:], axis=1, keepdims=KEEP), L)
        ps[113:114, :] = col_to_row(jnp.sum(dbm_acc[:], axis=1, keepdims=KEEP), L)
        ps[114:115, :] = part
        ps[115:L, :] = jnp.zeros((13, L), F32)

        mine = pl.ds(pl.multiple_of(H * core, H), H)
        other = pl.ds(pl.multiple_of(H * (1 - core), H), H)
        ca = rcopy(ps.at[other, :], pa, ars.at[0], arr.at[0], dp, dap_peer[1])
        ca.start()
        ca.wait_recv()
        ph[:] = ps[mine, :] + pa[:]
        cx = rcopy(ph, px, ars.at[4], arr.at[4], dp, dap_peer[2])
        cx.start()
        for q in range(EARLY, 4):
            for k in FAR:
                give(k, q)
        for q in BOTH:
            for k in FAR:
                take(k, q)
        cx.wait_recv()
        pc[:] = ph[:] + px[:]
        cb = {}
        for k in (3, 1, 2):
            cb[k] = rcopy(pc, pb.at[k - 1], ars.at[k], arr.at[k], dp_peer[k], d)
            cb[k].start()
        for k in FAR:
            take(k, 2)
        for k in PEERS:
            cb[k].wait_recv()
        pd[:] = (pc[:] + pb[0]) + (pb[1] + pb[2])
        ce = rcopy(pd, pf, ars.at[5], arr.at[5], dp, dap_peer[1])
        ce.start()
        for k in FAR:
            take(k, 3)
        ce.wait_recv()
        first = core == 0
        ra = jnp.where(first, pd[:], pf[:])
        rb = jnp.where(first, pf[:], pd[:])
        dwd_o[:] = ra
        dwm_o[:, 0:L] = rb[0:23, :]
        dwm_o[:, L:N] = rb[24:47, :]
        dbd_o[:] = rb[48:49, 0:H]
        dbm_o[:] = rb[49:50, 0:23]
        loss_o[:] = rb[50:51, 0:1]

        for k in PEERS:
            cc[k].wait_send()
            lc[k].wait_send()
            cb[k].wait_send()
        for c in (*nc.values(), *zc.values(), *vc.values(), *dc.values()):
            c.wait_send()
        ca.wait_send()
        cx.wait_send()
        ce.wait_send()

    return kernel


def flush_kernel(*refs):
    ins, outs, sem = refs[:7], refs[7:14], refs[14]
    copies = [pltpu.make_async_copy(a, b, sem.at[n]) for n, (a, b) in enumerate(zip(ins, outs))]
    for n in (1, 2, 0, 3, 4, 5, 6):
        copies[n].start()
    for c in copies:
        c.wait()


def solution(mesh):
    dp_size = mesh.shape["dp"]
    pair_spec = P("dp", "dap", None, None)
    pair_int_spec = P("dp", "dap", None)
    msa_spec = P("dp", None, "dap", None)
    msa_int_spec = P("dp", None, "dap")
    V = pltpu.VMEM

    def local_step(z, mask, tb, m, mt, bm, wd, bd, wm, bmb):
        args = (z.reshape(H, N, L), mask.reshape(H, N), tb.reshape(H, N), m.reshape(4096, N),
                mt.reshape(H, H), bm.reshape(H, H), wd.T, bd.reshape(1, H), wm.T, bmb.reshape(1, 23))
        args = tuple(pltpu.with_memory_space_constraint(a, pltpu.HBM) for a in args)
        shapes = [((1, 1), F32), ((H, N, L), BF16), ((4096, N), BF16), ((H, L), F32), ((1, H), F32),
                  ((23, N), F32), ((1, 23), F32)]
        scratch = [
            V((H, N, L), BF16), V((4096, N), BF16), V((H, N), I32), V((H, N), I32), V((H, H), I32),
            V((H, H), I32), V((H, L), BF16), V((1, H), F32), V((23, N), BF16), V((1, 23), F32),
            V((H, N), BF16), V((L, L), BF16), V((32, N), BF16), V((H, L), F32), V((32, L), F32),
            V((H, N), I32), V((N, L), F32), V((4, Q, L), F32), V((3, Q, L), F32), V((H, L), I32), V((H, L), I32),
            V((2, Q, L), I32), V((2, Q, L), I32), V((2, Q, L), I32), V((2, Q, L), I32), V((32, L), I32),
            V((16, L), F32), V((3, 16, L), F32), V((4, H, 16, L), BF16), V((2, 4, 2, Q, 8, L), BF16),
            V((512, L), F32), V((512, L), F32), V((H, L, L), BF16), V((2, 16, L, L), BF16),
            V((2, 4, 4, H, L), BF16), V((2, 4, 4, H, L), BF16), V((2, 4, 8, L), F32), V((2, 4, 8, L), F32),
            V((L, L), F32), V((32, N), F32), V((H, L), F32), V((32, L), F32), V((8, L), F32),
            V((L, L), F32), V((H, L), F32), V((H, L), F32), V((H, L), F32), V((3, H, L), F32), V((H, L), F32),
            V((H, L), F32), V((H, L), F32),
            DSEM((10,)), DSEM((3,)), DSEM((3,)), DSEM((3,)), DSEM((3,)), DSEM((4,)), DSEM((4,)),
            DSEM((2, 4, 2)), DSEM((2, 4, 2)), DSEM((2, 4)), DSEM((2, 4)), DSEM((2, 4)), DSEM((2, 4)),
            DSEM((6,)), DSEM((6,)),
        ]
        outs = pl.pallas_call(
            make_kernel(dp_size),
            out_shape=[pltpu.VMEM(s, t) for s, t in shapes],
            in_specs=[pl.BlockSpec(memory_space=pltpu.HBM)] * 10,
            out_specs=[pl.BlockSpec(memory_space=pltpu.VMEM)] * 7,
            scratch_shapes=scratch,
            compiler_params=pltpu.CompilerParams(collective_id=0, has_side_effects=True,
                                                 vmem_limit_bytes=44 * 1024 * 1024),
        )(*args)
        outs = pl.pallas_call(
            flush_kernel,
            out_shape=[jax.ShapeDtypeStruct(s, t) for s, t in shapes],
            in_specs=[pl.BlockSpec(memory_space=pltpu.VMEM)] * 7,
            out_specs=[pl.BlockSpec(memory_space=pl.ANY)] * 7,
            scratch_shapes=[DSEM((7,))],
            compiler_params=pltpu.CompilerParams(vmem_limit_bytes=8 * 1024 * 1024),
        )(*outs)
        loss, dz, dm, dwd, dbd, dwm, dbm = outs
        return (loss.reshape(()), dz.reshape(1, H, N, L), dm.reshape(1, H, H, N), dwd.T, dbd.reshape(H),
                dwm.T, dbm.reshape(23))

    return jax.shard_map(local_step, mesh=mesh,
                         in_specs=(pair_spec, pair_int_spec, pair_int_spec, msa_spec, msa_int_spec, msa_int_spec,
                                   P(), P(), P(), P()),
                         out_specs=(P(), pair_spec, msa_spec, P(), P(), P(), P()),
                         check_vma=False)
```

```python
import jax
import jax.numpy as jnp
from jax import lax
from jax.experimental import pallas as pl
from jax.experimental.pallas import tpu as pltpu
from jax.sharding import PartitionSpec as P

LOSS_SCALE = 2.0 ** 16
DIST_WEIGHT = 0.3
MSA_WEIGHT = 2.0
DIST_EPS = 1e-6
MSA_EPS = 1e-8
MESH = pl.DeviceIdType.MESH
DSEM = pltpu.SemaphoreType.DMA
KEEP = True
Q = 32
EARLY = 2
PEERS = (1, 2, 3)
FAR = (2, 3)
BOTH = (0, 1)
QUARTERS = range(4)
H = 64
L = 128
N = 256
F32 = jnp.float32
BF16 = jnp.bfloat16
I32 = jnp.int32


def dot(a, b, ca, cb):
    return lax.dot_general(a, b, (((ca,), (cb,)), ((), ())), preferred_element_type=F32)


def eye(n, m):
    return lax.broadcasted_iota(I32, (n, m), 0) == lax.broadcasted_iota(I32, (n, m), 1)


def row_to_col(row, n):
    return jnp.sum(jnp.where(eye(n, row.shape[1]), row, 0.0), axis=1, keepdims=KEEP)


def col_to_row(col, m):
    return jnp.sum(jnp.where(eye(col.shape[0], m), col, 0.0), axis=0, keepdims=KEEP)


def lanes2(ref, i):
    return jnp.concatenate([ref[pl.ds(2 * i, 1), :], ref[pl.ds(2 * i + 1, 1), :]], axis=1)


def make_kernel(batch):
    def kernel(z_h, mask_h, tb_h, m_h, mt_h, bm_h, wd_h, bd_h, wm_h, bmb_h,
               loss_o, dz_o, dm_o, dwd_o, dbd_o, dwm_o, dbm_o,
               zv, mv, mask_v, tb_v, mt_v, bm_v, wd_v, bd_v, wm_v, bmb_v,
               wt2, w2, wmt, bias_c, mbias_c, lab, lts, ltp, ltr, l1n, l2n, t1o, t2o, t1r, t2r, mlab,
               cnt_s, cnt_r, rn, rz, f0, f1, ntn, ntf, vb, vr, db, dr, dwd_acc, dwm_acc, dbd_acc, dbm_acc, nll_acc,
               ps, pa, ph, px, pb, pc, pd, pf,
               lsem, cs, cr, ls, lr, ns, nr, zs, zr, vs, vrs, ds, drs, ars, arr):
        dp = lax.axis_index("dp")
        d = lax.axis_index("dap")
        chip, core = d // 2, d % 2
        dap_peer = {1: chip * 2 + (1 - core), 2: (1 - chip) * 2 + core, 3: (1 - chip) * 2 + (1 - core)}
        pz, py = dp // 2, dp % 2
        dp_peer = {1: pz * 2 + (1 - py), 2: (1 - pz) * 2 + py, 3: (1 - pz) * 2 + (1 - py)}
        near = pl.multiple_of(chip * L, L)
        far = pl.multiple_of((1 - chip) * L, L)
        half = (chip, 1 - chip)
        phalf = (1 - chip, chip)
        base = {k: pl.multiple_of(H * dap_peer[k], H) for k in PEERS}

        loc = []
        for n, (src, dst) in enumerate([(mask_h, mask_v), (tb_h, tb_v), (bm_h, bm_v), (mt_h, mt_v), (wd_h, wd_v),
                                        (bd_h, bd_v), (wm_h, wm_v), (bmb_h, bmb_v), (m_h, mv), (z_h, zv)]):
            c = pltpu.make_async_copy(src, dst, lsem.at[n])
            c.start()
            loc.append(c)

        bar = pltpu.get_barrier_semaphore()
        for k in PEERS:
            pl.semaphore_signal(bar, inc=1, device_id=(dp, dap_peer[k]), device_id_type=MESH)
            pl.semaphore_signal(bar, inc=1, device_id=(dp_peer[k], d), device_id_type=MESH)

        for n in QUARTERS:
            loc[n].wait()
        maskf = mask_v[:].astype(F32)
        bertf = bm_v[:].astype(F32)
        cd = jnp.sum(jnp.sum(maskf, axis=0, keepdims=KEEP), axis=1, keepdims=KEEP)
        cm = jnp.sum(jnp.sum(bertf, axis=0, keepdims=KEEP), axis=1, keepdims=KEEP)
        cnt_s[0:8, :] = jnp.broadcast_to(cd, (8, L))
        cnt_s[8:16, :] = jnp.broadcast_to(cm, (8, L))
        labv = jnp.where(mask_v[:] > 0, tb_v[:], H)
        lab[:] = labv
        labf = labv.astype(F32)
        lts[:] = jnp.concatenate([labf, labf], axis=0).T
        low = lax.broadcasted_iota(I32, (Q, L), 1) < H
        for p in QUARTERS:
            ltp[p] = jnp.where(low, lts[H * p:H * p + Q, :], lts[H * p + Q:H * p + H, :])

        pl.semaphore_wait(bar, 6)

        def rcopy(src, dst, s, r, dpi, dapi):
            return pltpu.make_async_remote_copy(src_ref=src, dst_ref=dst, send_sem=s, recv_sem=r,
                                                device_id=(dpi, dapi), device_id_type=MESH)

        sends = []
        cc, lc, zc = {}, {}, {}
        for k in (2, 3, 1):
            cc[k] = rcopy(cnt_s, cnt_r.at[k - 1], cs.at[k - 1], cr.at[k - 1], dp, dap_peer[k])
            cc[k].start()
        for k in (2, 3, 1):
            lc[k] = rcopy(ltp.at[dap_peer[k]], ltr.at[k - 1],
                          ls.at[k - 1], lr.at[k - 1], dp, dap_peer[k])
            lc[k].start()
        nc = {}
        for q in QUARTERS:
            nc[q] = rcopy(z_h.at[:, pl.ds(pl.multiple_of(base[1] + 16 * q, 16), 16), :], rn.at[q],
                          ns.at[q], nr.at[q], dp, dap_peer[1])
            for k in FAR:
                for b in BOTH:
                    cols = pl.multiple_of(base[k] + Q * phalf[b] + 8 * q, 8)
                    zc[k, q, b] = rcopy(z_h.at[Q * b:Q * b + Q, pl.ds(cols, 8), :], rz.at[k - 2, q, b],
                                        zs.at[k - 2, q, b], zr.at[k - 2, q, b], dp, dap_peer[k])
                    zc[k, q, b].start()
            nc[q].start()
        for n in range(4, 8):
            loc[n].wait()
        wt = wd_v[:]
        wt2[:, 0:L] = wt
        wt2[:, L:N] = wt
        w2[0:H, :] = wt
        w2[H:L, :] = wt
        wmt[:] = jnp.zeros_like(wmt)
        wmt[0:23, :] = wm_v[:]
        bias_c[:] = jnp.broadcast_to(row_to_col(bd_v[:], H), (H, L))
        pad = lax.broadcasted_iota(I32, (32, 1), 0) >= 23
        mbias_c[:] = jnp.broadcast_to(jnp.where(pad, -1e30, row_to_col(bmb_v[:], 32)), (32, L))
        l1n[:] = lab[:, pl.ds(near, L)]
        mlv = jnp.where(bm_v[:] > 0, mt_v[:], H)
        bm_v[:] = mlv
        mlab[:] = jnp.concatenate([bm_v[pl.ds(0, 32, stride=2), :], bm_v[pl.ds(1, 32, stride=2), :]], axis=1)
        for a in (dwd_acc, dwm_acc, dbd_acc, dbm_acc, nll_acc):
            a[:] = jnp.zeros_like(a)

        for k in PEERS:
            cc[k].wait_recv()
        tot = (cnt_s[:] + cnt_r[0]) + (cnt_r[1] + cnt_r[2])
        den_d = DIST_EPS + tot[0:1, :]
        den_m = MSA_EPS + tot[8:9, :]
        cvd = (LOSS_SCALE * DIST_WEIGHT / batch) / den_d
        cvm = (LOSS_SCALE * MSA_WEIGHT / batch) / den_m
        cd2 = jnp.concatenate([cvd, cvd], axis=1)
        cm2 = jnp.concatenate([cvm, cvm], axis=1)

        def fold(a):
            return a[:, 0:L] + a[:, L:N]


        loc[8].wait()

        def msa(i, carry):
            m = mv[pl.ds(pl.multiple_of(N * i, N), N), :]
            b = mbias_c[:]
            l = dot(wmt[:], m, 1, 1) + jnp.concatenate([b, b], axis=1)
            t = lanes2(mlab, i)
            mx = jnp.max(l, axis=0, keepdims=KEEP)
            e = jnp.exp(l - mx)
            s = jnp.sum(e, axis=0, keepdims=KEEP)
            eq = lax.broadcasted_iota(I32, (32, N), 0) == t
            mk = (t < H).astype(F32)
            c = cm2 * mk
            h = (e * (c / s) - jnp.where(eq, c, 0.0)).astype(BF16)
            lt = jnp.sum(jnp.where(eq, l, 0.0), axis=0, keepdims=KEEP)
            nll_acc[1:2, :] += fold(mk * (mx + jnp.log(s)) - lt)
            dbm_acc[:] += fold(h.astype(F32))
            dm_o[pl.ds(pl.multiple_of(N * i, N), N), :] = dot(h, wmt[:], 0, 0).astype(BF16)
            dwm_acc[:] += dot(h, m, 1, 0)
            return carry

        lax.fori_loop(0, 16, msa, 0, unroll=4)


        for k in PEERS:
            lc[k].wait_recv()
        def turn(a):
            return pltpu.roll(a, H, 1)

        def unpack(p):
            return jnp.concatenate([jnp.where(low, p, turn(p)), jnp.where(low, turn(p), p)], axis=0)

        def paired(a):
            back = jnp.concatenate([pltpu.roll(a[8 * q:8 * q + 8, :], 4, 0) for q in QUARTERS], axis=0)
            return jnp.where(low, a, back).astype(I32)

        lane = lax.broadcasted_iota(I32, (Q, L), 1)
        upper = (lane % H >= Q).astype(I32)
        mine_low = upper == chip
        peer_low = upper == 1 - chip
        wide = lax.broadcasted_iota(I32, (H, L), 1) < H
        own_lt = lts[pl.ds(pl.multiple_of(H * d, H), H), :]
        l2n[:] = jnp.where(wide == (core == 0), own_lt, unpack(ltr[0])).astype(I32)
        l1f = lab[:, pl.ds(far, L)].astype(F32)
        for k in FAR:
            a = jnp.where(wide == (dap_peer[k] % 2 == 0), l1f, turn(l1f))
            t1o[k - 2] = paired(jnp.where(mine_low, a[0:Q, :], a[Q:H, :]))
            got = ltr[k - 1]
            t2o[k - 2] = paired(jnp.where(low == mine_low, got, turn(got)))
            sent = ltp[dap_peer[k]]
            t1r[k - 2] = paired(jnp.where(low == peer_low, sent, turn(sent)))
            u = unpack(got)
            u = jnp.concatenate([u, u], axis=0).T
            t2r[k - 2] = paired(jnp.where(peer_low, u[0:Q, :], u[Q:H, :]))

        def swap(src, nt, q, off):
            chunk = src.astype(F32)
            f0[:] = chunk[:, 0:8, :].reshape(512, L)
            f1[:] = chunk[:, 8:16, :].reshape(512, L)
            for t in range(8):
                nt[16 * q + t, pl.ds(off, H), :] = f0[pl.ds(t, H, stride=8), :].astype(BF16)
                nt[16 * q + 8 + t, pl.ds(off, H), :] = f1[pl.ds(t, H, stride=8), :].astype(BF16)

        bins = lax.broadcasted_iota(I32, (H, N), 0)

        def softmax_terms(zx, nx):
            b = bias_c[:]
            l = dot(wt2[:], jnp.concatenate([zx, nx], axis=1), 1, 1) + jnp.concatenate([b, b], axis=1)
            mx = jnp.max(l, axis=0, keepdims=KEEP)
            e = jnp.exp(l - mx)
            s = jnp.sum(e, axis=0, keepdims=KEEP)
            return l, e, s, mx + jnp.log(s)

        def near_tile(i, carry):
            zx = zv[pl.ds(2 * i, 2), pl.ds(near, L), :].reshape(N, L)
            nx = ntn[pl.ds(2 * i, 2), :, :].reshape(N, L)
            l, e, s, lse = softmax_terms(zx, nx)
            t1 = lanes2(l1n, i)
            t2 = lanes2(l2n, i)
            eq1 = bins == t1
            m1 = (t1 < H).astype(F32)
            c1 = cd2 * m1
            c2 = cd2 * (t2 < H).astype(F32)
            g1 = (e * (c1 / s) - jnp.where(eq1, c1, 0.0)).astype(BF16)
            g2 = (e * (c2 / s) - jnp.where(bins == t2, c2, 0.0)).astype(BF16)
            lt = jnp.sum(jnp.where(eq1, l, 0.0), axis=0, keepdims=KEEP)
            nll_acc[0:1, :] += fold(m1 * lse - lt)
            dbd_acc[:] += fold(g1.astype(F32))
            g = jnp.concatenate([g1, g2], axis=0)
            dz_o[pl.ds(2 * i, 2), pl.ds(near, L), :] = dot(g, w2[:], 0, 0).astype(BF16).reshape(2, L, L)
            dwd_acc[:] += dot(g, zx, 1, 0)
            return carry

        def own_tiles(k, q):
            for b in BOTH:
                zc[k, q, b].wait_recv()
                f0[0:N, :] = rz[k - 2, q, b].astype(F32).reshape(N, L)
                for t in range(8):
                    r = H * (t // 4) + Q * b
                    ntf[k - 2, 4 * q + t % 4, r:r + Q, :] = f0[pl.ds(t, Q, stride=8), :].astype(BF16)

            def body(j, carry):
                spots = [(8 * q + 4 * u + 2 * j + tt + Q * half[b], pl.multiple_of(base[k] + Q * b, Q))
                         for tt in BOTH for u in BOTH for b in BOTH]
                zx = jnp.concatenate([zv[r, pl.ds(c, Q), :] for r, c in spots], axis=0)
                nx = ntf[k - 2, pl.ds(4 * q + 2 * j, 2), :, :].reshape(N, L)
                l, e, s, lse = softmax_terms(zx, nx)
                t1 = lanes2(t1o.at[k - 2], 4 * q + j)
                t2 = lanes2(t2o.at[k - 2], 4 * q + j)
                eq1 = bins == t1
                eq2 = bins == t2
                m1 = (t1 < H).astype(F32)
                m2 = (t2 < H).astype(F32)
                v = e * (cd2 / s)
                w = v - cd2
                d1 = jnp.sum(jnp.where(eq1, w, 0.0), axis=0, keepdims=KEEP)
                d2 = jnp.sum(jnp.where(eq2, w, 0.0), axis=0, keepdims=KEEP)
                g1 = (jnp.where(eq1, w, v) * m1).astype(BF16)
                g2 = (jnp.where(eq2, w, v) * m2).astype(BF16)
                lt = jnp.sum(jnp.where(eq1, l, 0.0) + jnp.where(eq2, l, 0.0), axis=0, keepdims=KEEP)
                nll_acc[0:1, :] += fold((m1 + m2) * lse - lt)
                dbd_acc[:] += fold(g1.astype(F32) + g2.astype(F32))
                vh = v.astype(BF16)
                for tt in BOTH:
                    cut = slice(L * tt, L * tt + L)
                    vb[k - 2, q, 2 * j + tt] = vh[:, cut]
                    db[k - 2, q, pl.ds(2 * j + tt, 1), :] = d1[:, cut]
                    db[k - 2, q, pl.ds(4 + 2 * j + tt, 1), :] = d2[:, cut]
                g = jnp.concatenate([g1, g2], axis=0)
                dz = dot(g, w2[:], 0, 0).astype(BF16)
                for n, (r, c) in enumerate(spots):
                    dz_o[r, pl.ds(c, Q), :] = dz[Q * n:Q * n + Q, :]
                dwd_acc[:] += dot(g, zx, 1, 0) + dot(g, nx, 1, 0)
                return carry

            lax.fori_loop(0, 2, body, 0, unroll=2)

        vc, dc = {}, {}

        def give(k, q):
            vc[k, q] = rcopy(vb.at[k - 2, q], vr.at[k - 2, q], vs.at[k - 2, q], vrs.at[k - 2, q], dp, dap_peer[k])
            dc[k, q] = rcopy(db.at[k - 2, q], dr.at[k - 2, q], ds.at[k - 2, q], drs.at[k - 2, q], dp, dap_peer[k])
            vc[k, q].start()
            dc[k, q].start()

        def take(k, q):
            vc[k, q].wait_recv()
            dc[k, q].wait_recv()
            for j in BOTH:
                v = jnp.concatenate([vr[k - 2, q, 2 * j], vr[k - 2, q, 2 * j + 1]], axis=1).astype(F32)
                gs = []
                for table, row in ((t1r, 4 + 2 * j), (t2r, 2 * j)):
                    t = lanes2(table.at[k - 2], 4 * q + j)
                    on = jnp.concatenate([dr[k - 2, q, row:row + 1, :], dr[k - 2, q, row + 1:row + 2, :]], axis=1)
                    gs.append((jnp.where(bins == t, on, v) * (t < H).astype(F32)).astype(BF16))
                dz = dot(jnp.concatenate(gs, axis=0), w2[:], 0, 0)
                for tt in BOTH:
                    for u in BOTH:
                        for f, r in ((f0, L * tt + H * u), (f1, L * tt + H * u + Q)):
                            f[pl.ds(4 * u + 2 * j + tt, Q, stride=8), :] = dz[r:r + Q, :]
            for b, f in ((0, f0), (1, f1)):
                cols = pl.multiple_of(base[k] + Q * phalf[b] + 8 * q, 8)
                dz_o[Q * b:Q * b + Q, pl.ds(cols, 8), :] = f[0:N, :].reshape(Q, 8, L).astype(BF16)

        own_off = pl.multiple_of(H * core, H)
        oth_off = pl.multiple_of(H * (1 - core), H)
        loc[9].wait()
        for q in QUARTERS:
            swap(zv[:, pl.ds(pl.multiple_of(H * d + 16 * q, 16), 16), :], ntn, q, own_off)
        for q in QUARTERS:
            nc[q].wait_recv()
            swap(rn[q], ntn, q, oth_off)
        lax.fori_loop(0, 32, near_tile, 0, unroll=4)

        for q in QUARTERS:
            for k in FAR:
                own_tiles(k, q)
                if q < EARLY:
                    give(k, q)

        ps[0:H, :] = dwd_acc[0:H, :] + dwd_acc[H:L, :]
        ps[H:88, :] = dwm_acc[0:24, 0:L]
        ps[88:112, :] = dwm_acc[0:24, L:N]
        nd = jnp.sum(nll_acc[0:1, :], axis=1, keepdims=KEEP)
        nm = jnp.sum(nll_acc[1:2, :], axis=1, keepdims=KEEP)
        part = (DIST_WEIGHT * nd / den_d + MSA_WEIGHT * nm / den_m) / batch
        ps[112:113, :] = col_to_row(jnp.sum(dbd_acc[:], axis=1, keepdims=KEEP), L)
        ps[113:114, :] = col_to_row(jnp.sum(dbm_acc[:], axis=1, keepdims=KEEP), L)
        ps[114:115, :] = part
        ps[115:L, :] = jnp.zeros((13, L), F32)

        mine = pl.ds(pl.multiple_of(H * core, H), H)
        other = pl.ds(pl.multiple_of(H * (1 - core), H), H)
        ca = rcopy(ps.at[other, :], pa, ars.at[0], arr.at[0], dp, dap_peer[1])
        ca.start()
        ca.wait_recv()
        ph[:] = ps[mine, :] + pa[:]
        cx = rcopy(ph, px, ars.at[4], arr.at[4], dp, dap_peer[2])
        cx.start()
        for q in range(EARLY, 4):
            for k in FAR:
                give(k, q)
        for q in BOTH:
            for k in FAR:
                take(k, q)
        cx.wait_recv()
        pc[:] = ph[:] + px[:]
        cb = {}
        for k in (3, 1, 2):
            cb[k] = rcopy(pc, pb.at[k - 1], ars.at[k], arr.at[k], dp_peer[k], d)
            cb[k].start()
        for k in FAR:
            take(k, 2)
        for k in PEERS:
            cb[k].wait_recv()
        pd[:] = (pc[:] + pb[0]) + (pb[1] + pb[2])
        ce = rcopy(pd, pf, ars.at[5], arr.at[5], dp, dap_peer[1])
        ce.start()
        for k in FAR:
            take(k, 3)
        ce.wait_recv()
        first = core == 0
        ra = jnp.where(first, pd[:], pf[:])
        rb = jnp.where(first, pf[:], pd[:])
        dwd_o[:] = ra
        dwm_o[:, 0:L] = rb[0:23, :]
        dwm_o[:, L:N] = rb[24:47, :]
        dbd_o[:] = rb[48:49, 0:H]
        dbm_o[:] = rb[49:50, 0:23]
        loss_o[:] = rb[50:51, 0:1]

        for k in PEERS:
            cc[k].wait_send()
            lc[k].wait_send()
            cb[k].wait_send()
        for c in (*nc.values(), *zc.values(), *vc.values(), *dc.values()):
            c.wait_send()
        ca.wait_send()
        cx.wait_send()
        ce.wait_send()

    return kernel


def flush_kernel(*refs):
    ins, outs, sem = refs[:7], refs[7:14], refs[14]
    copies = [pltpu.make_async_copy(a, b, sem.at[n]) for n, (a, b) in enumerate(zip(ins, outs))]
    for n in (1, 2, 0, 3, 4, 5, 6):
        copies[n].start()
    for c in copies:
        c.wait()


def solution(mesh):
    dp_size = mesh.shape["dp"]
    pair_spec = P("dp", "dap", None, None)
    pair_int_spec = P("dp", "dap", None)
    msa_spec = P("dp", None, "dap", None)
    msa_int_spec = P("dp", None, "dap")
    V = pltpu.VMEM

    def local_step(z, mask, tb, m, mt, bm, wd, bd, wm, bmb):
        args = (z.reshape(H, N, L), mask.reshape(H, N), tb.reshape(H, N), m.reshape(4096, N),
                mt.reshape(H, H), bm.reshape(H, H), wd.T, bd.reshape(1, H), wm.T, bmb.reshape(1, 23))
        args = tuple(pltpu.with_memory_space_constraint(a, pltpu.HBM) for a in args)
        shapes = [((1, 1), F32), ((H, N, L), BF16), ((4096, N), BF16), ((H, L), F32), ((1, H), F32),
                  ((23, N), F32), ((1, 23), F32)]
        scratch = [
            V((H, N, L), BF16), V((4096, N), BF16), V((H, N), I32), V((H, N), I32), V((H, H), I32),
            V((H, H), I32), V((H, L), BF16), V((1, H), F32), V((23, N), BF16), V((1, 23), F32),
            V((H, N), BF16), V((L, L), BF16), V((32, N), BF16), V((H, L), F32), V((32, L), F32),
            V((H, N), I32), V((N, L), F32), V((4, Q, L), F32), V((3, Q, L), F32), V((H, L), I32), V((H, L), I32),
            V((2, Q, L), I32), V((2, Q, L), I32), V((2, Q, L), I32), V((2, Q, L), I32), V((32, L), I32),
            V((16, L), F32), V((3, 16, L), F32), V((4, H, 16, L), BF16), V((2, 4, 2, Q, 8, L), BF16),
            V((512, L), F32), V((512, L), F32), V((H, L, L), BF16), V((2, 16, L, L), BF16),
            V((2, 4, 4, H, L), BF16), V((2, 4, 4, H, L), BF16), V((2, 4, 8, L), F32), V((2, 4, 8, L), F32),
            V((L, L), F32), V((32, N), F32), V((H, L), F32), V((32, L), F32), V((8, L), F32),
            V((L, L), F32), V((H, L), F32), V((H, L), F32), V((H, L), F32), V((3, H, L), F32), V((H, L), F32),
            V((H, L), F32), V((H, L), F32),
            DSEM((10,)), DSEM((3,)), DSEM((3,)), DSEM((3,)), DSEM((3,)), DSEM((4,)), DSEM((4,)),
            DSEM((2, 4, 2)), DSEM((2, 4, 2)), DSEM((2, 4)), DSEM((2, 4)), DSEM((2, 4)), DSEM((2, 4)),
            DSEM((6,)), DSEM((6,)),
        ]
        outs = pl.pallas_call(
            make_kernel(dp_size),
            out_shape=[pltpu.VMEM(s, t) for s, t in shapes],
            in_specs=[pl.BlockSpec(memory_space=pltpu.HBM)] * 10,
            out_specs=[pl.BlockSpec(memory_space=pltpu.VMEM)] * 7,
            scratch_shapes=scratch,
            compiler_params=pltpu.CompilerParams(collective_id=0, has_side_effects=True,
                                                 vmem_limit_bytes=44 * 1024 * 1024),
        )(*args)
        outs = pl.pallas_call(
            flush_kernel,
            out_shape=[jax.ShapeDtypeStruct(s, t) for s, t in shapes],
            in_specs=[pl.BlockSpec(memory_space=pltpu.VMEM)] * 7,
            out_specs=[pl.BlockSpec(memory_space=pl.ANY)] * 7,
            scratch_shapes=[DSEM((7,))],
            compiler_params=pltpu.CompilerParams(vmem_limit_bytes=8 * 1024 * 1024),
        )(*outs)
        loss, dz, dm, dwd, dbd, dwm, dbm = outs
        return (loss.reshape(()), dz.reshape(1, H, N, L), dm.reshape(1, H, H, N), dwd.T, dbd.reshape(H),
                dwm.T, dbm.reshape(23))

    return jax.shard_map(local_step, mesh=mesh,
                         in_specs=(pair_spec, pair_int_spec, pair_int_spec, msa_spec, msa_int_spec, msa_int_spec,
                                   P(), P(), P(), P()),
                         out_specs=(P(), pair_spec, msa_spec, P(), P(), P(), P()),
                         check_vma=False)
```

```python
import jax
import jax.numpy as jnp
from jax import lax
from jax.experimental import pallas as pl
from jax.experimental.pallas import tpu as pltpu
from jax.sharding import PartitionSpec as P

LOSS_SCALE = 2.0 ** 16
DIST_WEIGHT = 0.3
MSA_WEIGHT = 2.0
DIST_EPS = 1e-6
MSA_EPS = 1e-8
MESH = pl.DeviceIdType.MESH
DSEM = pltpu.SemaphoreType.DMA
KEEP = True
Q = 32
EARLY = 2
PEERS = (1, 2, 3)
FAR = (2, 3)
BOTH = (0, 1)
QUARTERS = range(4)
KIB = 1024
LAST = 3
S = 56
H = 64
L = 128
N = 256
F32 = jnp.float32
BF16 = jnp.bfloat16
I32 = jnp.int32


def dot(a, b, ca, cb):
    return lax.dot_general(a, b, (((ca,), (cb,)), ((), ())), preferred_element_type=F32)


def eye(n, m):
    return lax.broadcasted_iota(I32, (n, m), 0) == lax.broadcasted_iota(I32, (n, m), 1)


def row_to_col(row, n):
    return jnp.sum(jnp.where(eye(n, row.shape[1]), row, 0.0), axis=1, keepdims=KEEP)


def col_to_row(col, m):
    return jnp.sum(jnp.where(eye(col.shape[0], m), col, 0.0), axis=0, keepdims=KEEP)


def lanes2(ref, i):
    return jnp.concatenate([ref[pl.ds(2 * i, 1), :], ref[pl.ds(2 * i + 1, 1), :]], axis=1)


def returned_pairs(v_ref, d_ref, mine, peers, first, w2, f0, f1):
    bins = lax.broadcasted_iota(I32, (H, N), 0)
    dv = d_ref[:].astype(F32)
    for j in BOTH:
        v = jnp.concatenate([v_ref[2 * j], v_ref[2 * j + 1]], axis=1).astype(F32)
        gs = []
        for table, row in ((mine, 4 + 2 * j), (peers, 2 * j)):
            t = lanes2(table, first + j)
            on = jnp.concatenate([dv[row:row + 1, :], dv[row + 1:row + 2, :]], axis=1)
            gs.append((jnp.where(bins == t, on, v) * (t < H).astype(F32)).astype(BF16))
        dz = dot(jnp.concatenate(gs, axis=0), w2[:], 0, 0)
        for tt in BOTH:
            for u in BOTH:
                for f, r in ((f0, L * tt + H * u), (f1, L * tt + H * u + Q)):
                    f[pl.ds(4 * u + 2 * j + tt, Q, stride=8), :] = dz[r:r + Q, :]


def make_kernel(batch):
    def kernel(z_h, mask_h, tb_h, m_h, mt_h, bm_h, wd_h, bd_h, wm_h, bmb_h,
               loss_o, dz_o, dm_o, dwd_o, dbd_o, dwm_o, dbm_o, vl_o, dl_o, tl_o, w2,
               zv, mv, mask_v, tb_v, mt_v, bm_v, wd_v, bd_v, wm_v, bmb_v,
               wt2, wmt, wmn, bias_c, mbias_c, lab, lts, ltp, ltr, l1n, l2n, t1o, t2o, t1r, t2r, mlab,
               cnt_s, cnt_r, rn, rz, f0, f1, ntn, ntf, vb, vr, db, dbh, dr, dwd_acc, dwm_acc, dbd_acc, dbm_acc, nll_acc,
               ps, pa, ph, px, pb, pc, pd, pf,
               lsem, cs, cr, ls, lr, ns, nr, zs, zr, vs, vrs, ds, drs, ars, arr):
        dp = lax.axis_index("dp")
        d = lax.axis_index("dap")
        chip, core = d // 2, d % 2
        dap_peer = {1: chip * 2 + (1 - core), 2: (1 - chip) * 2 + core, 3: (1 - chip) * 2 + (1 - core)}
        pz, py = dp // 2, dp % 2
        dp_peer = {1: pz * 2 + (1 - py), 2: (1 - pz) * 2 + py, 3: (1 - pz) * 2 + (1 - py)}
        near = pl.multiple_of(chip * L, L)
        far = pl.multiple_of((1 - chip) * L, L)
        half = (chip, 1 - chip)
        phalf = (1 - chip, chip)
        base = {k: pl.multiple_of(H * dap_peer[k], H) for k in PEERS}

        loc = []
        for n, (src, dst) in enumerate([(mask_h, mask_v), (tb_h, tb_v), (bm_h, bm_v), (mt_h, mt_v), (wd_h, wd_v),
                                        (bd_h, bd_v), (wm_h, wm_v), (bmb_h, bmb_v), (m_h, mv), (z_h, zv)]):
            c = pltpu.make_async_copy(src, dst, lsem.at[n])
            c.start()
            loc.append(c)

        bar = pltpu.get_barrier_semaphore()
        for k in PEERS:
            pl.semaphore_signal(bar, inc=1, device_id=(dp, dap_peer[k]), device_id_type=MESH)
            pl.semaphore_signal(bar, inc=1, device_id=(dp_peer[k], d), device_id_type=MESH)

        for n in QUARTERS:
            loc[n].wait()
        maskf = mask_v[:].astype(F32)
        bertf = bm_v[:].astype(F32)
        cd = jnp.sum(jnp.sum(maskf, axis=0, keepdims=KEEP), axis=1, keepdims=KEEP)
        cm = jnp.sum(jnp.sum(bertf, axis=0, keepdims=KEEP), axis=1, keepdims=KEEP)
        cnt_s[0:8, :] = jnp.broadcast_to(cd, (8, L))
        cnt_s[8:16, :] = jnp.broadcast_to(cm, (8, L))
        labv = jnp.where(mask_v[:] > 0, tb_v[:], H)
        lab[:] = labv
        labf = labv.astype(F32)
        lts[:] = jnp.concatenate([labf, labf], axis=0).T
        low = lax.broadcasted_iota(I32, (Q, L), 1) < H
        for p in QUARTERS:
            ltp[p] = jnp.where(low, lts[H * p:H * p + Q, :], lts[H * p + Q:H * p + H, :])

        pl.semaphore_wait(bar, 6)

        def rcopy(src, dst, s, r, dpi, dapi):
            return pltpu.make_async_remote_copy(src_ref=src, dst_ref=dst, send_sem=s, recv_sem=r,
                                                device_id=(dpi, dapi), device_id_type=MESH)

        sends = []
        cc, lc, zc = {}, {}, {}
        for k in (2, 3, 1):
            cc[k] = rcopy(cnt_s, cnt_r.at[k - 1], cs.at[k - 1], cr.at[k - 1], dp, dap_peer[k])
            cc[k].start()
        for k in (2, 3, 1):
            lc[k] = rcopy(ltp.at[dap_peer[k]], ltr.at[k - 1],
                          ls.at[k - 1], lr.at[k - 1], dp, dap_peer[k])
            lc[k].start()
        nc = {}
        for q in QUARTERS:
            nc[q] = rcopy(z_h.at[:, pl.ds(pl.multiple_of(base[1] + 16 * q, 16), 16), :], rn.at[q],
                          ns.at[q], nr.at[q], dp, dap_peer[1])
            for k in FAR:
                for b in BOTH:
                    cols = pl.multiple_of(base[k] + Q * phalf[b] + 8 * q, 8)
                    zc[k, q, b] = rcopy(z_h.at[Q * b:Q * b + Q, pl.ds(cols, 8), :], rz.at[k - 2, q, b],
                                        zs.at[k - 2, q, b], zr.at[k - 2, q, b], dp, dap_peer[k])
                    zc[k, q, b].start()
            nc[q].start()
        for n in range(4, 8):
            loc[n].wait()
        wt = wd_v[:]
        nat = wt.astype(F32).T.astype(BF16)
        wt2[0:L, :] = nat
        wt2[L:N, :] = nat
        w2[0:H, :] = wt
        w2[H:L, :] = wt
        wmt[:] = jnp.zeros_like(wmt)
        wmt[0:23, :] = wm_v[:]
        wmn[:] = wmt[:].astype(F32).T.astype(BF16)
        bias_c[:] = jnp.broadcast_to(row_to_col(bd_v[:], H), (H, L))
        pad = lax.broadcasted_iota(I32, (32, 1), 0) >= 23
        mbias_c[:] = jnp.broadcast_to(jnp.where(pad, -1e30, row_to_col(bmb_v[:], 32)), (32, L))
        l1n[:] = lab[:, pl.ds(near, L)]
        mlv = jnp.where(bm_v[:] > 0, mt_v[:], H)
        bm_v[:] = mlv
        mlab[:] = jnp.concatenate([bm_v[pl.ds(0, 32, stride=2), :], bm_v[pl.ds(1, 32, stride=2), :]], axis=1)
        for a in (dwd_acc, dwm_acc, dbd_acc, dbm_acc, nll_acc):
            a[:] = jnp.zeros_like(a)

        for k in PEERS:
            cc[k].wait_recv()
        tot = (cnt_s[:] + cnt_r[0]) + (cnt_r[1] + cnt_r[2])
        den_d = DIST_EPS + tot[0:1, :]
        den_m = MSA_EPS + tot[8:9, :]
        cvd = (LOSS_SCALE * DIST_WEIGHT / batch) / den_d
        cvm = (LOSS_SCALE * MSA_WEIGHT / batch) / den_m
        cd2 = jnp.concatenate([cvd, cvd], axis=1)
        cm2 = jnp.concatenate([cvm, cvm], axis=1)

        def fold(a):
            return a[:, 0:L] + a[:, L:N]


        loc[8].wait()

        def msa(i, carry):
            m = mv[pl.ds(pl.multiple_of(N * i, N), N), :]
            b = mbias_c[:]
            l = dot(m, wmn[:], 1, 0).T + jnp.concatenate([b, b], axis=1)
            t = lanes2(mlab, i)
            mx = jnp.max(l, axis=0, keepdims=KEEP)
            e = jnp.exp(l - mx)
            s = jnp.sum(e, axis=0, keepdims=KEEP)
            eq = lax.broadcasted_iota(I32, (32, N), 0) == t
            mk = (t < H).astype(F32)
            c = cm2 * mk
            h = (e * (c / s) - jnp.where(eq, c, 0.0)).astype(BF16)
            lt = jnp.sum(jnp.where(eq, l, 0.0), axis=0, keepdims=KEEP)
            nll_acc[1:2, :] += fold(mk * (mx + jnp.log(s)) - lt)
            dbm_acc[:] += fold(h.astype(F32))
            dm_o[pl.ds(pl.multiple_of(N * i, N), N), :] = dot(h, wmt[:], 0, 0).astype(BF16)
            dwm_acc[:] += dot(h, m, 1, 0)
            return carry

        lax.fori_loop(0, 16, msa, 0, unroll=4)


        for k in PEERS:
            lc[k].wait_recv()
        def turn(a):
            return pltpu.roll(a, H, 1)

        def unpack(p):
            return jnp.concatenate([jnp.where(low, p, turn(p)), jnp.where(low, turn(p), p)], axis=0)

        def paired(a):
            back = jnp.concatenate([pltpu.roll(a[8 * q:8 * q + 8, :], 4, 0) for q in QUARTERS], axis=0)
            return jnp.where(low, a, back).astype(I32)

        lane = lax.broadcasted_iota(I32, (Q, L), 1)
        upper = (lane % H >= Q).astype(I32)
        mine_low = upper == chip
        peer_low = upper == 1 - chip
        wide = lax.broadcasted_iota(I32, (H, L), 1) < H
        own_lt = lts[pl.ds(pl.multiple_of(H * d, H), H), :]
        l2n[:] = jnp.where(wide == (core == 0), own_lt, unpack(ltr[0])).astype(I32)
        l1f = lab[:, pl.ds(far, L)].astype(F32)
        for k in FAR:
            a = jnp.where(wide == (dap_peer[k] % 2 == 0), l1f, turn(l1f))
            t1o[k - 2] = paired(jnp.where(mine_low, a[0:Q, :], a[Q:H, :]))
            got = ltr[k - 1]
            t2o[k - 2] = paired(jnp.where(low == mine_low, got, turn(got)))
            sent = ltp[dap_peer[k]]
            t1r[k - 2] = paired(jnp.where(low == peer_low, sent, turn(sent)))
            u = unpack(got)
            u = jnp.concatenate([u, u], axis=0).T
            t2r[k - 2] = paired(jnp.where(peer_low, u[0:Q, :], u[Q:H, :]))
            tl_o[0, k - 2] = t1r[k - 2, 8 * LAST:Q, :]
            tl_o[1, k - 2] = t2r[k - 2, 8 * LAST:Q, :]

        def swap(src, nt, q, off):
            chunk = src.astype(F32)
            f0[:] = chunk[:, 0:8, :].reshape(512, L)
            f1[:] = chunk[:, 8:16, :].reshape(512, L)
            for t in range(8):
                nt[16 * q + t, pl.ds(off, H), :] = f0[pl.ds(t, H, stride=8), :].astype(BF16)
                nt[16 * q + 8 + t, pl.ds(off, H), :] = f1[pl.ds(t, H, stride=8), :].astype(BF16)

        bins = lax.broadcasted_iota(I32, (H, N), 0)

        def softmax_terms(zx, nx):
            b = bias_c[:]
            l = dot(jnp.concatenate([zx, nx], axis=1), wt2[:], 1, 0).T + jnp.concatenate([b, b], axis=1)
            mx = jnp.max(l, axis=0, keepdims=KEEP)
            e = jnp.exp(l - mx)
            s = jnp.sum(e, axis=0, keepdims=KEEP)
            return l, e, s, mx + jnp.log(s)

        def near_tile(i, carry):
            zx = zv[pl.ds(2 * i, 2), pl.ds(near, L), :].reshape(N, L)
            nx = ntn[pl.ds(2 * i, 2), :, :].reshape(N, L)
            l, e, s, lse = softmax_terms(zx, nx)
            t1 = lanes2(l1n, i)
            t2 = lanes2(l2n, i)
            eq1 = bins == t1
            m1 = (t1 < H).astype(F32)
            c1 = cd2 * m1
            c2 = cd2 * (t2 < H).astype(F32)
            g1 = (e * (c1 / s) - jnp.where(eq1, c1, 0.0)).astype(BF16)
            g2 = (e * (c2 / s) - jnp.where(bins == t2, c2, 0.0)).astype(BF16)
            lt = jnp.sum(jnp.where(eq1, l, 0.0), axis=0, keepdims=KEEP)
            nll_acc[0:1, :] += fold(m1 * lse - lt)
            dbd_acc[:] += fold(g1.astype(F32))
            g = jnp.concatenate([g1, g2], axis=0)
            dz_o[pl.ds(2 * i, 2), pl.ds(near, L), :] = dot(g, w2[:], 0, 0).astype(BF16).reshape(2, L, L)
            dwd_acc[:] += dot(g, zx, 1, 0)
            return carry

        def own_tiles(k, q):
            for b in BOTH:
                zc[k, q, b].wait_recv()
                f0[0:N, :] = rz[k - 2, q, b].astype(F32).reshape(N, L)
                for t in range(8):
                    r = H * (t // 4) + Q * b
                    ntf[k - 2, 4 * q + t % 4, r:r + Q, :] = f0[pl.ds(t, Q, stride=8), :].astype(BF16)

            def body(j, carry):
                spots = [(8 * q + 4 * u + 2 * j + tt + Q * half[b], pl.multiple_of(base[k] + Q * b, Q))
                         for tt in BOTH for u in BOTH for b in BOTH]
                zx = jnp.concatenate([zv[r, pl.ds(c, Q), :] for r, c in spots], axis=0)
                nx = ntf[k - 2, pl.ds(4 * q + 2 * j, 2), :, :].reshape(N, L)
                l, e, s, lse = softmax_terms(zx, nx)
                t1 = lanes2(t1o.at[k - 2], 4 * q + j)
                t2 = lanes2(t2o.at[k - 2], 4 * q + j)
                eq1 = bins == t1
                eq2 = bins == t2
                m1 = (t1 < H).astype(F32)
                m2 = (t2 < H).astype(F32)
                v = e * (cd2 / s)
                w = v - cd2
                d1 = jnp.sum(jnp.where(eq1, w, 0.0), axis=0, keepdims=KEEP)
                d2 = jnp.sum(jnp.where(eq2, w, 0.0), axis=0, keepdims=KEEP)
                g1 = (jnp.where(eq1, w, v) * m1).astype(BF16)
                g2 = (jnp.where(eq2, w, v) * m2).astype(BF16)
                lt = jnp.sum(jnp.where(eq1, l, 0.0) + jnp.where(eq2, l, 0.0), axis=0, keepdims=KEEP)
                nll_acc[0:1, :] += fold((m1 + m2) * lse - lt)
                dbd_acc[:] += fold(g1.astype(F32) + g2.astype(F32))
                vh = v.astype(BF16)
                for tt in BOTH:
                    cut = slice(L * tt, L * tt + L)
                    vb[k - 2, q, 2 * j + tt] = vh[:, cut]
                    db[k - 2, q, pl.ds(2 * j + tt, 1), :] = d1[:, cut]
                    db[k - 2, q, pl.ds(4 + 2 * j + tt, 1), :] = d2[:, cut]
                g = jnp.concatenate([g1, g2], axis=0)
                dz = dot(g, w2[:], 0, 0).astype(BF16)
                for n, (r, c) in enumerate(spots):
                    dz_o[r, pl.ds(c, Q), :] = dz[Q * n:Q * n + Q, :]
                dwd_acc[:] += dot(g, zx, 1, 0) + dot(g, nx, 1, 0)
                return carry

            lax.fori_loop(0, 2, body, 0, unroll=2)
            dbh[k - 2, q] = db[k - 2, q].astype(BF16)

        vc, dc = {}, {}

        def give(k, q):
            v_to, d_to = (vr.at[k - 2, q], dr.at[k - 2, q]) if q < LAST else (vl_o.at[k - 2], dl_o.at[k - 2])
            vc[k, q] = rcopy(vb.at[k - 2, q], v_to, vs.at[k - 2, q], vrs.at[k - 2, q], dp, dap_peer[k])
            dc[k, q] = rcopy(dbh.at[k - 2, q], d_to, ds.at[k - 2, q], drs.at[k - 2, q], dp, dap_peer[k])
            vc[k, q].start()
            dc[k, q].start()

        def take(k, q):
            vc[k, q].wait_recv()
            dc[k, q].wait_recv()
            returned_pairs(vr.at[k - 2, q], dr.at[k - 2, q], t1r.at[k - 2], t2r.at[k - 2], 4 * q, w2, f0, f1)
            for b, f in ((0, f0), (1, f1)):
                cols = pl.multiple_of(base[k] + Q * phalf[b] + 8 * q, 8)
                dz_o[Q * b:Q * b + Q, pl.ds(cols, 8), :] = f[0:N, :].reshape(Q, 8, L).astype(BF16)

        own_off = pl.multiple_of(H * core, H)
        oth_off = pl.multiple_of(H * (1 - core), H)
        loc[9].wait()
        for q in QUARTERS:
            swap(zv[:, pl.ds(pl.multiple_of(H * d + 16 * q, 16), 16), :], ntn, q, own_off)
        for q in QUARTERS:
            nc[q].wait_recv()
            swap(rn[q], ntn, q, oth_off)
        lax.fori_loop(0, 32, near_tile, 0, unroll=4)

        for q in QUARTERS:
            for k in FAR:
                own_tiles(k, q)
                if q < EARLY:
                    give(k, q)

        ps[0:H, :] = dwd_acc[0:H, :] + dwd_acc[H:L, :]
        ps[H:87, :] = dwm_acc[0:23, 0:L]
        ps[87:110, :] = dwm_acc[0:23, L:N]
        nd = jnp.sum(nll_acc[0:1, :], axis=1, keepdims=KEEP)
        nm = jnp.sum(nll_acc[1:2, :], axis=1, keepdims=KEEP)
        part = (DIST_WEIGHT * nd / den_d + MSA_WEIGHT * nm / den_m) / batch
        dbd = col_to_row(jnp.sum(dbd_acc[:], axis=1, keepdims=KEEP), L)
        dbm = col_to_row(jnp.sum(dbm_acc[:], axis=1, keepdims=KEEP), L)
        end = lax.broadcasted_iota(I32, (1, L), 1) == L - 1
        ps[110:111, :] = dbd + turn(dbm) + jnp.where(end, part, 0.0)
        ps[111:112, :] = jnp.zeros((1, L), F32)

        mine = pl.ds(pl.multiple_of(S * core, S), S)
        other = pl.ds(pl.multiple_of(S * (1 - core), S), S)
        ca = rcopy(ps.at[other, :], pa, ars.at[0], arr.at[0], dp, dap_peer[1])
        ca.start()
        ca.wait_recv()
        ph[:] = ps[mine, :] + pa[:]
        cx = rcopy(ph, px, ars.at[4], arr.at[4], dp, dap_peer[2])
        cx.start()
        for q in range(EARLY, 4):
            for k in FAR:
                give(k, q)
        for q in BOTH:
            for k in FAR:
                take(k, q)
        cx.wait_recv()
        pc[:] = ph[:] + px[:]
        cb = {}
        for k in (3, 1, 2):
            cb[k] = rcopy(pc, pb.at[k - 1], ars.at[k], arr.at[k], dp_peer[k], d)
            cb[k].start()
        for k in FAR:
            take(k, 2)
        for k in PEERS:
            cb[k].wait_recv()
        total = (pc[:] + pb[0]) + (pb[1] + pb[2])
        pd[:] = total
        pf[mine, :] = total
        ce = rcopy(pd, pf.at[mine, :], ars.at[5], arr.at[5], dp, dap_peer[1])
        ce.start()
        for k in FAR:
            vc[k, LAST].wait_recv()
            dc[k, LAST].wait_recv()
        ce.wait_recv()
        dwd_o[:] = pf[0:H, :]
        dwm_o[:, 0:L] = pf[H:87, :]
        dwm_o[:, L:N] = pf[87:110, :]
        row = pf[110:111, :]
        dbd_o[:] = row[:, 0:H]
        dbm_o[:] = turn(row)[:, 0:23]
        loss_o[:] = pltpu.roll(row, 1, 1)[:, 0:1]

        for k in PEERS:
            cc[k].wait_send()
            lc[k].wait_send()
            cb[k].wait_send()
        for c in (*nc.values(), *zc.values(), *vc.values(), *dc.values()):
            c.wait_send()
        ca.wait_send()
        cx.wait_send()
        ce.wait_send()

    return kernel


def flush_kernel(loss_i, dz_i, dm_i, dwd_i, dbd_i, dwm_i, dbm_i, vl, dl, tl, w2,
                 loss_o, dz_o, dm_o, dwd_o, dbd_o, dwm_o, dbm_o, f0, f1, late, sem):
    d = lax.axis_index("dap")
    chip, core = d // 2, d % 2
    phalf = (1 - chip, chip)
    copies = []

    def put(src, dst):
        c = pltpu.make_async_copy(src, dst, sem.at[len(copies)])
        c.start()
        copies.append(c)

    def put_dz(r, rows, c, cols):
        put(dz_i.at[pl.ds(r, rows), pl.ds(c, cols), :], dz_o.at[pl.ds(r, rows), pl.ds(c, cols), :])

    for n in QUARTERS:
        put_dz(16 * n, 16, pl.multiple_of(L * chip, L), L)
    spots = {}
    for k, there in ((0, core), (1, 1 - core)):
        start = pl.multiple_of((1 - chip) * L + H * there, H)
        for b in BOTH:
            mid = pl.multiple_of(start + Q * phalf[b], Q)
            put_dz(Q * b, Q, mid, 24)
            put_dz(Q * b, Q, pl.multiple_of(start + Q * phalf[1 - b], Q), Q)
            spots[k, b] = pl.multiple_of(mid + 24, 8)
    for n in QUARTERS:
        put(dm_i.at[pl.ds(KIB * n, KIB), :], dm_o.at[pl.ds(KIB * n, KIB), :])
    for src, dst in ((loss_i, loss_o), (dwd_i, dwd_o), (dbd_i, dbd_o), (dwm_i, dwm_o), (dbm_i, dbm_o)):
        put(src, dst)
    for k in BOTH:
        returned_pairs(vl.at[k], dl.at[k], tl.at[0, k], tl.at[1, k], 0, w2, f0, f1)
        for b, f in ((0, f0), (1, f1)):
            late[k, b] = f[:].reshape(Q, 8, L).astype(BF16)
            put(late.at[k, b], dz_o.at[pl.ds(Q * b, Q), pl.ds(spots[k, b], 8), :])
    for c in copies:
        c.wait()


def solution(mesh):
    dp_size = mesh.shape["dp"]
    pair_spec = P("dp", "dap", None, None)
    pair_int_spec = P("dp", "dap", None)
    msa_spec = P("dp", None, "dap", None)
    msa_int_spec = P("dp", None, "dap")
    V = pltpu.VMEM

    def local_step(z, mask, tb, m, mt, bm, wd, bd, wm, bmb):
        args = (z.reshape(H, N, L), mask.reshape(H, N), tb.reshape(H, N), m.reshape(4096, N),
                mt.reshape(H, H), bm.reshape(H, H), wd.T, bd.reshape(1, H), wm.T, bmb.reshape(1, 23))
        args = tuple(pltpu.with_memory_space_constraint(a, pltpu.HBM) for a in args)
        shapes = [((1, 1), F32), ((H, N, L), BF16), ((4096, N), BF16), ((H, L), F32), ((1, H), F32),
                  ((23, N), F32), ((1, 23), F32)]
        scratch = [
            V((H, N, L), BF16), V((4096, N), BF16), *[V((H, N), I32)] * 2, V((H, H), I32),
            V((H, H), I32), V((H, L), BF16), V((1, H), F32), V((23, N), BF16), V((1, 23), F32),
            V((N, H), BF16), V((32, N), BF16), V((N, 32), BF16), V((H, L), F32), V((32, L), F32),
            V((H, N), I32), V((N, L), F32), V((4, Q, L), F32), V((3, Q, L), F32), V((H, L), I32), V((H, L), I32),
            *[V((2, Q, L), I32)] * 4, V((32, L), I32),
            V((16, L), F32), V((3, 16, L), F32), V((4, H, 16, L), BF16), V((2, 4, 2, Q, 8, L), BF16),
            V((512, L), F32), V((512, L), F32), V((H, L, L), BF16), V((2, 16, L, L), BF16),
            V((2, 4, 4, H, L), BF16), V((2, 3, 4, H, L), BF16), V((2, 4, 8, L), F32), V((2, 4, 8, L), BF16), V((2, 3, 8, L), BF16),
            V((L, L), F32), V((32, N), F32), V((H, L), F32), V((32, L), F32), V((8, L), F32),
            V((2 * S, L), F32), V((S, L), F32), V((S, L), F32), V((S, L), F32), V((3, S, L), F32), V((S, L), F32),
            V((S, L), F32), V((2 * S, L), F32),
            DSEM((10,)), *[DSEM((3,))] * 4, DSEM((4,)), DSEM((4,)),
            *[DSEM((2, 4, 2))] * 2, *[DSEM((2, 4))] * 4,
            DSEM((6,)), DSEM((6,)),
        ]
        extra = [((2, 4, H, L), BF16), ((2, 8, L), BF16), ((2, 2, 8, L), I32), ((L, L), BF16)]
        vmem = [pl.BlockSpec(memory_space=pltpu.VMEM)]
        hbm = [pl.BlockSpec(memory_space=pltpu.HBM)]
        outs = pl.pallas_call(
            make_kernel(dp_size),
            out_shape=[pltpu.VMEM(s, t) for s, t in shapes + extra],
            in_specs=hbm * 10,
            out_specs=vmem * 11,
            scratch_shapes=scratch,
            compiler_params=pltpu.CompilerParams(collective_id=0, has_side_effects=True,
                                                 vmem_limit_bytes=44 * KIB * KIB),
        )(*args)
        outs = pl.pallas_call(
            flush_kernel,
            out_shape=[jax.ShapeDtypeStruct(s, t) for s, t in shapes],
            in_specs=vmem * 11,
            out_specs=hbm * 7,
            scratch_shapes=[V((N, L), F32), V((N, L), F32), V((2, 2, Q, 8, L), BF16), DSEM((25,))],
            compiler_params=pltpu.CompilerParams(vmem_limit_bytes=8 * KIB * KIB),
        )(*outs)
        loss, dz, dm, dwd, dbd, dwm, dbm = outs
        return (loss.reshape(()), dz.reshape(1, H, N, L), dm.reshape(1, H, H, N), dwd.T, dbd.reshape(H),
                dwm.T, dbm.reshape(23))

    return jax.shard_map(local_step, mesh=mesh,
                         in_specs=(pair_spec, pair_int_spec, pair_int_spec, msa_spec, msa_int_spec, msa_int_spec,
                                   P(), P(), P(), P()),
                         out_specs=(P(), pair_spec, msa_spec, P(), P(), P(), P()),
                         check_vma=False)
```

```python
import jax
import jax.numpy as jnp
from jax import lax
from jax.experimental import pallas as pl
from jax.experimental.pallas import tpu as pltpu
from jax.sharding import PartitionSpec as P

LOSS_SCALE = 2.0 ** 16
DIST_WEIGHT = 0.3
MSA_WEIGHT = 2.0
DIST_EPS = 1e-6
MSA_EPS = 1e-8
MESH = pl.DeviceIdType.MESH
DSEM = pltpu.SemaphoreType.DMA
KEEP = True
Q = 32
EARLY = 4
PEERS = (1, 2, 3)
FAR = (2, 3)
BOTH = (0, 1)
QUARTERS = range(4)
KIB = 1024
LAST = 3
S = 56
H = 64
L = 128
N = 256
F32 = jnp.float32
BF16 = jnp.bfloat16
I32 = jnp.int32


def dot(a, b, ca, cb):
    return lax.dot_general(a, b, (((ca,), (cb,)), ((), ())), preferred_element_type=F32)


def eye(n, m):
    return lax.broadcasted_iota(I32, (n, m), 0) == lax.broadcasted_iota(I32, (n, m), 1)


def row_to_col(row, n):
    return jnp.sum(jnp.where(eye(n, row.shape[1]), row, 0.0), axis=1, keepdims=KEEP)


def col_to_row(col, m):
    return jnp.sum(jnp.where(eye(col.shape[0], m), col, 0.0), axis=0, keepdims=KEEP)


def lanes2(ref, i):
    return jnp.concatenate([ref[pl.ds(2 * i, 1), :], ref[pl.ds(2 * i + 1, 1), :]], axis=1)


def returned_pairs(v_ref, d_ref, mine, peers, first, w2, f0, f1):
    bins = lax.broadcasted_iota(I32, (H, N), 0)
    dv = d_ref[:].astype(F32)
    for j in BOTH:
        v = jnp.concatenate([v_ref[2 * j], v_ref[2 * j + 1]], axis=1).astype(F32)
        gs = []
        for table, row in ((mine, 4 + 2 * j), (peers, 2 * j)):
            t = lanes2(table, first + j)
            on = jnp.concatenate([dv[row:row + 1, :], dv[row + 1:row + 2, :]], axis=1)
            gs.append((jnp.where(bins == t, on, v) * (t < H).astype(F32)).astype(BF16))
        dz = dot(jnp.concatenate(gs, axis=0), w2[:], 0, 0)
        for tt in BOTH:
            for u in BOTH:
                for f, r in ((f0, L * tt + H * u), (f1, L * tt + H * u + Q)):
                    f[pl.ds(4 * u + 2 * j + tt, Q, stride=8), :] = dz[r:r + Q, :]


def make_kernel(batch):
    def kernel(z_h, mask_h, tb_h, m_h, mt_h, bm_h, wd_h, bd_h, wm_h, bmb_h,
               loss_o, dz_o, dm_o, dwd_o, dbd_o, dwm_o, dbm_o, vl_o, dl_o, tl_o, w2,
               zv, mv, mask_v, tb_v, mt_v, bm_v, wd_v, bd_v, wm_v, bmb_v,
               wt2, wmt, wmn, bias_c, mbias_c, lab, lts, ltp, ltr, l1n, l2n, t1o, t2o, t1r, t2r, mlab,
               cnt_s, cnt_r, rn, rz, f0, f1, ntn, ntf, vb, vr, db, dbh, dr, dwd_acc, dwm_acc, dbd_acc, dbm_acc, nll_acc,
               ps, pa, ph, px, pb, pc, pf,
               lsem, cs, cr, ls, lr, ns, nr, zs, zr, vs, vrs, ds, drs, ars, arr):
        dp = lax.axis_index("dp")
        d = lax.axis_index("dap")
        chip, core = d // 2, d % 2
        dap_peer = {1: chip * 2 + (1 - core), 2: (1 - chip) * 2 + core, 3: (1 - chip) * 2 + (1 - core)}
        pz, py = dp // 2, dp % 2
        dp_peer = {1: pz * 2 + (1 - py), 2: (1 - pz) * 2 + py, 3: (1 - pz) * 2 + (1 - py)}
        near = pl.multiple_of(chip * L, L)
        far = pl.multiple_of((1 - chip) * L, L)
        half = (chip, 1 - chip)
        phalf = (1 - chip, chip)
        base = {k: pl.multiple_of(H * dap_peer[k], H) for k in PEERS}

        loc = []
        for n, (src, dst) in enumerate([(mask_h, mask_v), (tb_h, tb_v), (bm_h, bm_v), (mt_h, mt_v), (wd_h, wd_v),
                                        (bd_h, bd_v), (wm_h, wm_v), (bmb_h, bmb_v), (m_h, mv), (z_h, zv)]):
            c = pltpu.make_async_copy(src, dst, lsem.at[n])
            c.start()
            loc.append(c)

        bar = pltpu.get_barrier_semaphore()
        for k in PEERS:
            pl.semaphore_signal(bar, inc=1, device_id=(dp, dap_peer[k]), device_id_type=MESH)
        for k in (1, 2):
            for there in (d, dap_peer[1]):
                pl.semaphore_signal(bar, inc=1, device_id=(dp_peer[k], there), device_id_type=MESH)

        for n in QUARTERS:
            loc[n].wait()
        maskf = mask_v[:].astype(F32)
        bertf = bm_v[:].astype(F32)
        cd = jnp.sum(jnp.sum(maskf, axis=0, keepdims=KEEP), axis=1, keepdims=KEEP)
        cm = jnp.sum(jnp.sum(bertf, axis=0, keepdims=KEEP), axis=1, keepdims=KEEP)
        cnt_s[0:8, :] = jnp.broadcast_to(cd, (8, L))
        cnt_s[8:16, :] = jnp.broadcast_to(cm, (8, L))
        labv = jnp.where(mask_v[:] > 0, tb_v[:], H)
        lab[:] = labv
        labf = labv.astype(F32)
        lts[:] = jnp.concatenate([labf, labf], axis=0).T
        low = lax.broadcasted_iota(I32, (Q, L), 1) < H
        for p in QUARTERS:
            ltp[p] = jnp.where(low, lts[H * p:H * p + Q, :], lts[H * p + Q:H * p + H, :])

        pl.semaphore_wait(bar, 7)

        def rcopy(src, dst, s, r, dpi, dapi):
            return pltpu.make_async_remote_copy(src_ref=src, dst_ref=dst, send_sem=s, recv_sem=r,
                                                device_id=(dpi, dapi), device_id_type=MESH)

        sends = []
        cc, lc, zc = {}, {}, {}
        for k in (2, 3, 1):
            cc[k] = rcopy(cnt_s, cnt_r.at[k - 1], cs.at[k - 1], cr.at[k - 1], dp, dap_peer[k])
            cc[k].start()
        for k in (2, 3, 1):
            lc[k] = rcopy(ltp.at[dap_peer[k]], ltr.at[k - 1],
                          ls.at[k - 1], lr.at[k - 1], dp, dap_peer[k])
            lc[k].start()
        nc = {}
        for q in QUARTERS:
            nc[q] = rcopy(z_h.at[:, pl.ds(pl.multiple_of(base[1] + 16 * q, 16), 16), :], rn.at[q],
                          ns.at[q], nr.at[q], dp, dap_peer[1])
            for k in FAR:
                for b in BOTH:
                    cols = pl.multiple_of(base[k] + Q * phalf[b] + 8 * q, 8)
                    zc[k, q, b] = rcopy(z_h.at[Q * b:Q * b + Q, pl.ds(cols, 8), :], rz.at[k - 2, q, b],
                                        zs.at[k - 2, q, b], zr.at[k - 2, q, b], dp, dap_peer[k])
                    zc[k, q, b].start()
            nc[q].start()
        for n in range(4, 8):
            loc[n].wait()
        wt = wd_v[:]
        nat = wt.astype(F32).T.astype(BF16)
        wt2[0:L, :] = nat
        wt2[L:N, :] = nat
        w2[0:H, :] = wt
        w2[H:L, :] = wt
        wmt[:] = jnp.zeros_like(wmt)
        wmt[0:23, :] = wm_v[:]
        wmn[:] = wmt[:].astype(F32).T.astype(BF16)
        bias_c[:] = jnp.broadcast_to(row_to_col(bd_v[:], H), (H, L))
        pad = lax.broadcasted_iota(I32, (32, 1), 0) >= 23
        mbias_c[:] = jnp.broadcast_to(jnp.where(pad, -1e30, row_to_col(bmb_v[:], 32)), (32, L))
        l1n[:] = lab[:, pl.ds(near, L)]
        mlv = jnp.where(bm_v[:] > 0, mt_v[:], H)
        bm_v[:] = mlv
        mlab[:] = jnp.concatenate([bm_v[pl.ds(0, 32, stride=2), :], bm_v[pl.ds(1, 32, stride=2), :]], axis=1)
        for a in (dwd_acc, dwm_acc, dbd_acc, dbm_acc, nll_acc):
            a[:] = jnp.zeros_like(a)

        for k in PEERS:
            cc[k].wait_recv()
        tot = (cnt_s[:] + cnt_r[0]) + (cnt_r[1] + cnt_r[2])
        den_d = DIST_EPS + tot[0:1, :]
        den_m = MSA_EPS + tot[8:9, :]
        cvd = (LOSS_SCALE * DIST_WEIGHT / batch) / den_d
        cvm = (LOSS_SCALE * MSA_WEIGHT / batch) / den_m
        cd2 = jnp.concatenate([cvd, cvd], axis=1)
        cm2 = jnp.concatenate([cvm, cvm], axis=1)

        def fold(a):
            return a[:, 0:L] + a[:, L:N]


        loc[8].wait()

        def msa(i, carry):
            m = mv[pl.ds(pl.multiple_of(N * i, N), N), :]
            b = mbias_c[:]
            l = dot(m, wmn[:], 1, 0).T + jnp.concatenate([b, b], axis=1)
            t = lanes2(mlab, i)
            mx = jnp.max(l, axis=0, keepdims=KEEP)
            e = jnp.exp(l - mx)
            s = jnp.sum(e, axis=0, keepdims=KEEP)
            eq = lax.broadcasted_iota(I32, (32, N), 0) == t
            mk = (t < H).astype(F32)
            c = cm2 * mk
            h = (e * (c / s) - jnp.where(eq, c, 0.0)).astype(BF16)
            lt = jnp.sum(jnp.where(eq, l, 0.0), axis=0, keepdims=KEEP)
            nll_acc[1:2, :] += fold(mk * (mx + jnp.log(s)) - lt)
            dbm_acc[:] += fold(h.astype(F32))
            dm_o[pl.ds(pl.multiple_of(N * i, N), N), :] = dot(h, wmt[:], 0, 0).astype(BF16)
            dwm_acc[:] += dot(h, m, 1, 0)
            return carry

        lax.fori_loop(0, 16, msa, 0, unroll=4)


        for k in PEERS:
            lc[k].wait_recv()
        def turn(a):
            return pltpu.roll(a, H, 1)

        def unpack(p):
            return jnp.concatenate([jnp.where(low, p, turn(p)), jnp.where(low, turn(p), p)], axis=0)

        def paired(a):
            back = jnp.concatenate([pltpu.roll(a[8 * q:8 * q + 8, :], 4, 0) for q in QUARTERS], axis=0)
            return jnp.where(low, a, back).astype(I32)

        lane = lax.broadcasted_iota(I32, (Q, L), 1)
        upper = (lane % H >= Q).astype(I32)
        mine_low = upper == chip
        peer_low = upper == 1 - chip
        wide = lax.broadcasted_iota(I32, (H, L), 1) < H
        own_lt = lts[pl.ds(pl.multiple_of(H * d, H), H), :]
        l2n[:] = jnp.where(wide == (core == 0), own_lt, unpack(ltr[0])).astype(I32)
        l1f = lab[:, pl.ds(far, L)].astype(F32)
        for k in FAR:
            a = jnp.where(wide == (dap_peer[k] % 2 == 0), l1f, turn(l1f))
            t1o[k - 2] = paired(jnp.where(mine_low, a[0:Q, :], a[Q:H, :]))
            got = ltr[k - 1]
            t2o[k - 2] = paired(jnp.where(low == mine_low, got, turn(got)))
            sent = ltp[dap_peer[k]]
            t1r[k - 2] = paired(jnp.where(low == peer_low, sent, turn(sent)))
            u = unpack(got)
            u = jnp.concatenate([u, u], axis=0).T
            t2r[k - 2] = paired(jnp.where(peer_low, u[0:Q, :], u[Q:H, :]))
            tl_o[0, k - 2] = t1r[k - 2, 8 * LAST:Q, :]
            tl_o[1, k - 2] = t2r[k - 2, 8 * LAST:Q, :]

        def swap(src, nt, q, off):
            chunk = src.astype(F32)
            f0[:] = chunk[:, 0:8, :].reshape(512, L)
            f1[:] = chunk[:, 8:16, :].reshape(512, L)
            for t in range(8):
                nt[16 * q + t, pl.ds(off, H), :] = f0[pl.ds(t, H, stride=8), :].astype(BF16)
                nt[16 * q + 8 + t, pl.ds(off, H), :] = f1[pl.ds(t, H, stride=8), :].astype(BF16)

        bins = lax.broadcasted_iota(I32, (H, N), 0)

        def softmax_terms(zx, nx):
            b = bias_c[:]
            l = dot(jnp.concatenate([zx, nx], axis=1), wt2[:], 1, 0).T + jnp.concatenate([b, b], axis=1)
            mx = jnp.max(l, axis=0, keepdims=KEEP)
            e = jnp.exp(l - mx)
            s = jnp.sum(e, axis=0, keepdims=KEEP)
            return l, e, s, mx + jnp.log(s)

        def near_tile(i, carry):
            zx = zv[pl.ds(2 * i, 2), pl.ds(near, L), :].reshape(N, L)
            nx = ntn[pl.ds(2 * i, 2), :, :].reshape(N, L)
            l, e, s, lse = softmax_terms(zx, nx)
            t1 = lanes2(l1n, i)
            t2 = lanes2(l2n, i)
            eq1 = bins == t1
            m1 = (t1 < H).astype(F32)
            c1 = cd2 * m1
            c2 = cd2 * (t2 < H).astype(F32)
            g1 = (e * (c1 / s) - jnp.where(eq1, c1, 0.0)).astype(BF16)
            g2 = (e * (c2 / s) - jnp.where(bins == t2, c2, 0.0)).astype(BF16)
            lt = jnp.sum(jnp.where(eq1, l, 0.0), axis=0, keepdims=KEEP)
            nll_acc[0:1, :] += fold(m1 * lse - lt)
            dbd_acc[:] += fold(g1.astype(F32))
            g = jnp.concatenate([g1, g2], axis=0)
            dz_o[pl.ds(2 * i, 2), pl.ds(near, L), :] = dot(g, w2[:], 0, 0).astype(BF16).reshape(2, L, L)
            dwd_acc[:] += dot(g, zx, 1, 0)
            return carry

        def own_tiles(k, q):
            for b in BOTH:
                zc[k, q, b].wait_recv()
                f0[0:N, :] = rz[k - 2, q, b].astype(F32).reshape(N, L)
                for t in range(8):
                    r = H * (t // 4) + Q * b
                    ntf[k - 2, 4 * q + t % 4, r:r + Q, :] = f0[pl.ds(t, Q, stride=8), :].astype(BF16)

            def body(j, carry):
                spots = [(8 * q + 4 * u + 2 * j + tt + Q * half[b], pl.multiple_of(base[k] + Q * b, Q))
                         for tt in BOTH for u in BOTH for b in BOTH]
                zx = jnp.concatenate([zv[r, pl.ds(c, Q), :] for r, c in spots], axis=0)
                nx = ntf[k - 2, pl.ds(4 * q + 2 * j, 2), :, :].reshape(N, L)
                l, e, s, lse = softmax_terms(zx, nx)
                t1 = lanes2(t1o.at[k - 2], 4 * q + j)
                t2 = lanes2(t2o.at[k - 2], 4 * q + j)
                eq1 = bins == t1
                eq2 = bins == t2
                m1 = (t1 < H).astype(F32)
                m2 = (t2 < H).astype(F32)
                v = e * (cd2 / s)
                w = v - cd2
                d1 = jnp.sum(jnp.where(eq1, w, 0.0), axis=0, keepdims=KEEP)
                d2 = jnp.sum(jnp.where(eq2, w, 0.0), axis=0, keepdims=KEEP)
                g1 = (jnp.where(eq1, w, v) * m1).astype(BF16)
                g2 = (jnp.where(eq2, w, v) * m2).astype(BF16)
                lt = jnp.sum(jnp.where(eq1, l, 0.0) + jnp.where(eq2, l, 0.0), axis=0, keepdims=KEEP)
                nll_acc[0:1, :] += fold((m1 + m2) * lse - lt)
                dbd_acc[:] += fold(g1.astype(F32) + g2.astype(F32))
                vh = v.astype(BF16)
                for tt in BOTH:
                    cut = slice(L * tt, L * tt + L)
                    vb[k - 2, q, 2 * j + tt] = vh[:, cut]
                    db[k - 2, q, pl.ds(2 * j + tt, 1), :] = d1[:, cut]
                    db[k - 2, q, pl.ds(4 + 2 * j + tt, 1), :] = d2[:, cut]
                g = jnp.concatenate([g1, g2], axis=0)
                dz = dot(g, w2[:], 0, 0).astype(BF16)
                for n, (r, c) in enumerate(spots):
                    dz_o[r, pl.ds(c, Q), :] = dz[Q * n:Q * n + Q, :]
                dwd_acc[:] += dot(g, zx, 1, 0) + dot(g, nx, 1, 0)
                return carry

            lax.fori_loop(0, 2, body, 0, unroll=2)
            dbh[k - 2, q] = db[k - 2, q].astype(BF16)

        vc, dc = {}, {}

        def give(k, q):
            v_to, d_to = (vr.at[k - 2, q], dr.at[k - 2, q]) if q < LAST else (vl_o.at[k - 2], dl_o.at[k - 2])
            vc[k, q] = rcopy(vb.at[k - 2, q], v_to, vs.at[k - 2, q], vrs.at[k - 2, q], dp, dap_peer[k])
            dc[k, q] = rcopy(dbh.at[k - 2, q], d_to, ds.at[k - 2, q], drs.at[k - 2, q], dp, dap_peer[k])
            vc[k, q].start()
            dc[k, q].start()

        def take(k, q):
            vc[k, q].wait_recv()
            dc[k, q].wait_recv()
            returned_pairs(vr.at[k - 2, q], dr.at[k - 2, q], t1r.at[k - 2], t2r.at[k - 2], 4 * q, w2, f0, f1)
            for b, f in ((0, f0), (1, f1)):
                cols = pl.multiple_of(base[k] + Q * phalf[b] + 8 * q, 8)
                dz_o[Q * b:Q * b + Q, pl.ds(cols, 8), :] = f[0:N, :].reshape(Q, 8, L).astype(BF16)

        own_off = pl.multiple_of(H * core, H)
        oth_off = pl.multiple_of(H * (1 - core), H)
        loc[9].wait()
        for q in QUARTERS:
            swap(zv[:, pl.ds(pl.multiple_of(H * d + 16 * q, 16), 16), :], ntn, q, own_off)
        for q in QUARTERS:
            nc[q].wait_recv()
            swap(rn[q], ntn, q, oth_off)
        lax.fori_loop(0, 32, near_tile, 0, unroll=4)

        for q in QUARTERS:
            for k in FAR:
                own_tiles(k, q)
                if 2 * q + k - 2 < EARLY:
                    give(k, q)

        ps[0:H, :] = dwd_acc[0:H, :] + dwd_acc[H:L, :]
        ps[H:87, :] = dwm_acc[0:23, 0:L]
        ps[87:110, :] = dwm_acc[0:23, L:N]
        nd = jnp.sum(nll_acc[0:1, :], axis=1, keepdims=KEEP)
        nm = jnp.sum(nll_acc[1:2, :], axis=1, keepdims=KEEP)
        part = (DIST_WEIGHT * nd / den_d + MSA_WEIGHT * nm / den_m) / batch
        dbd = col_to_row(jnp.sum(dbd_acc[:], axis=1, keepdims=KEEP), L)
        dbm = col_to_row(jnp.sum(dbm_acc[:], axis=1, keepdims=KEEP), L)
        end = lax.broadcasted_iota(I32, (1, L), 1) == L - 1
        ps[110:111, :] = dbd + turn(dbm) + jnp.where(end, part, 0.0)
        ps[111:112, :] = jnp.zeros((1, L), F32)

        mine = pl.ds(pl.multiple_of(S * core, S), S)
        other = pl.ds(pl.multiple_of(S * (1 - core), S), S)
        def trio(halves, src, dst, first, k):
            there = ((dp, dap_peer[1]), (dp_peer[k], d), (dp_peer[k], dap_peer[1]))
            group = [rcopy(src.at[rows, :], dst.at[n], ars.at[first + n], arr.at[first + n], *to)
                     for n, (rows, to) in enumerate(zip(halves, there))]
            for c in group:
                c.start()
            return group

        sums = trio((other, mine, other), ps, pa, 0, 1)
        for c in sums:
            c.wait_recv()
        ph[:] = (ps[mine, :] + pa[0]) + (pa[1] + pa[2])
        cx = rcopy(ph, px, ars.at[6], arr.at[6], dp, dap_peer[2])
        cx.start()
        for q in QUARTERS:
            for k in FAR:
                if 2 * q + k - 2 >= EARLY:
                    give(k, q)
        for k in FAR:
            take(k, 0)
        cx.wait_recv()
        pc[:] = ph[:] + px[:]
        everything = pl.ds(0, S)
        last_sums = trio((everything,) * 3, pc, pb, 3, 2)
        for k in FAR:
            take(k, 1)
        for c in last_sums:
            c.wait_recv()
        pf[mine, :] = pc[:] + pb[1]
        pf[other, :] = pb[0] + pb[2]
        for k in FAR:
            take(k, 2)
        for k in FAR:
            vc[k, LAST].wait_recv()
            dc[k, LAST].wait_recv()
        dwd_o[:] = pf[0:H, :]
        dwm_o[:, 0:L] = pf[H:87, :]
        dwm_o[:, L:N] = pf[87:110, :]
        row = pf[110:111, :]
        dbd_o[:] = row[:, 0:H]
        dbm_o[:] = turn(row)[:, 0:23]
        loss_o[:] = pltpu.roll(row, 1, 1)[:, 0:1]

        for k in PEERS:
            cc[k].wait_send()
            lc[k].wait_send()
        for c in (*nc.values(), *zc.values(), *vc.values(), *dc.values(), *sums, *last_sums):
            c.wait_send()
        cx.wait_send()

    return kernel


def flush_kernel(loss_i, dz_i, dm_i, dwd_i, dbd_i, dwm_i, dbm_i, vl, dl, tl, w2,
                 loss_o, dz_o, dm_o, dwd_o, dbd_o, dwm_o, dbm_o, f0, f1, late, sem):
    d = lax.axis_index("dap")
    chip, core = d // 2, d % 2
    phalf = (1 - chip, chip)
    copies = []

    def put(src, dst):
        c = pltpu.make_async_copy(src, dst, sem.at[len(copies)])
        c.start()
        copies.append(c)

    def put_dz(r, rows, c, cols):
        put(dz_i.at[pl.ds(r, rows), pl.ds(c, cols), :], dz_o.at[pl.ds(r, rows), pl.ds(c, cols), :])

    for n in QUARTERS:
        put_dz(16 * n, 16, pl.multiple_of(L * chip, L), L)
    spots = {}
    for k, there in ((0, core), (1, 1 - core)):
        start = pl.multiple_of((1 - chip) * L + H * there, H)
        for b in BOTH:
            mid = pl.multiple_of(start + Q * phalf[b], Q)
            put_dz(Q * b, Q, mid, 24)
            put_dz(Q * b, Q, pl.multiple_of(start + Q * phalf[1 - b], Q), Q)
            spots[k, b] = pl.multiple_of(mid + 24, 8)
    for n in QUARTERS:
        put(dm_i.at[pl.ds(KIB * n, KIB), :], dm_o.at[pl.ds(KIB * n, KIB), :])
    for src, dst in ((loss_i, loss_o), (dwd_i, dwd_o), (dbd_i, dbd_o), (dwm_i, dwm_o), (dbm_i, dbm_o)):
        put(src, dst)
    for k in BOTH:
        returned_pairs(vl.at[k], dl.at[k], tl.at[0, k], tl.at[1, k], 0, w2, f0, f1)
        for b, f in ((0, f0), (1, f1)):
            late[k, b] = f[:].reshape(Q, 8, L).astype(BF16)
            put(late.at[k, b], dz_o.at[pl.ds(Q * b, Q), pl.ds(spots[k, b], 8), :])
    for c in copies:
        c.wait()


def solution(mesh):
    dp_size = mesh.shape["dp"]
    pair_spec = P("dp", "dap", None, None)
    pair_int_spec = P("dp", "dap", None)
    msa_spec = P("dp", None, "dap", None)
    msa_int_spec = P("dp", None, "dap")
    V = pltpu.VMEM

    def local_step(z, mask, tb, m, mt, bm, wd, bd, wm, bmb):
        args = (z.reshape(H, N, L), mask.reshape(H, N), tb.reshape(H, N), m.reshape(4096, N),
                mt.reshape(H, H), bm.reshape(H, H), wd.T, bd.reshape(1, H), wm.T, bmb.reshape(1, 23))
        args = tuple(pltpu.with_memory_space_constraint(a, pltpu.HBM) for a in args)
        shapes = [((1, 1), F32), ((H, N, L), BF16), ((4096, N), BF16), ((H, L), F32), ((1, H), F32),
                  ((23, N), F32), ((1, 23), F32)]
        scratch = [
            V((H, N, L), BF16), V((4096, N), BF16), *[V((H, N), I32)] * 2, V((H, H), I32),
            V((H, H), I32), V((H, L), BF16), V((1, H), F32), V((23, N), BF16), V((1, 23), F32),
            V((N, H), BF16), V((32, N), BF16), V((N, 32), BF16), V((H, L), F32), V((32, L), F32),
            V((H, N), I32), V((N, L), F32), V((4, Q, L), F32), V((3, Q, L), F32), V((H, L), I32), V((H, L), I32),
            *[V((2, Q, L), I32)] * 4, V((32, L), I32),
            V((16, L), F32), V((3, 16, L), F32), V((4, H, 16, L), BF16), V((2, 4, 2, Q, 8, L), BF16),
            V((512, L), F32), V((512, L), F32), V((H, L, L), BF16), V((2, 16, L, L), BF16),
            V((2, 4, 4, H, L), BF16), V((2, 3, 4, H, L), BF16), V((2, 4, 8, L), F32), V((2, 4, 8, L), BF16), V((2, 3, 8, L), BF16),
            V((L, L), F32), V((32, N), F32), V((H, L), F32), V((32, L), F32), V((8, L), F32),
            V((2 * S, L), F32), V((3, S, L), F32), V((S, L), F32), V((S, L), F32), V((3, S, L), F32), V((S, L), F32),
            V((2 * S, L), F32),
            DSEM((10,)), *[DSEM((3,))] * 4, DSEM((4,)), DSEM((4,)),
            *[DSEM((2, 4, 2))] * 2, *[DSEM((2, 4))] * 4,
            DSEM((7,)), DSEM((7,)),
        ]
        extra = [((2, 4, H, L), BF16), ((2, 8, L), BF16), ((2, 2, 8, L), I32), ((L, L), BF16)]
        vmem = [pl.BlockSpec(memory_space=pltpu.VMEM)]
        hbm = [pl.BlockSpec(memory_space=pltpu.HBM)]
        outs = pl.pallas_call(
            make_kernel(dp_size),
            out_shape=[pltpu.VMEM(s, t) for s, t in shapes + extra],
            in_specs=hbm * 10,
            out_specs=vmem * 11,
            scratch_shapes=scratch,
            compiler_params=pltpu.CompilerParams(collective_id=0, has_side_effects=True,
                                                 vmem_limit_bytes=44 * KIB * KIB),
        )(*args)
        outs = pl.pallas_call(
            flush_kernel,
            out_shape=[jax.ShapeDtypeStruct(s, t) for s, t in shapes],
            in_specs=vmem * 11,
            out_specs=hbm * 7,
            scratch_shapes=[V((N, L), F32), V((N, L), F32), V((2, 2, Q, 8, L), BF16), DSEM((25,))],
            compiler_params=pltpu.CompilerParams(vmem_limit_bytes=8 * KIB * KIB),
        )(*outs)
        loss, dz, dm, dwd, dbd, dwm, dbm = outs
        return (loss.reshape(()), dz.reshape(1, H, N, L), dm.reshape(1, H, H, N), dwd.T, dbd.reshape(H),
                dwm.T, dbm.reshape(23))

    return jax.shard_map(local_step, mesh=mesh,
                         in_specs=(pair_spec, pair_int_spec, pair_int_spec, msa_spec, msa_int_spec, msa_int_spec,
                                   P(), P(), P(), P()),
                         out_specs=(P(), pair_spec, msa_spec, P(), P(), P(), P()),
                         check_vma=False)
```

```python
import jax
import jax.numpy as jnp
from jax import lax
from jax.experimental import pallas as pl
from jax.experimental.pallas import tpu as pltpu
from jax.sharding import PartitionSpec as P

LOSS_SCALE = 2.0 ** 16
DIST_WEIGHT = 0.3
MSA_WEIGHT = 2.0
DIST_EPS = 1e-6
MSA_EPS = 1e-8
MESH = pl.DeviceIdType.MESH
DSEM = pltpu.SemaphoreType.DMA
KEEP = True
CLS = 23
Q = 32
EARLY = 4
SPLIT = (4,)
SENT, KEPT = True, False
PEERS = (1, 2, 3)
FAR = (2, 3)
BOTH = (0, 1)
QUARTERS = range(4)
KIB = 1024
LAST = 3
H = 64
L = 128
N = 256
F32 = jnp.float32
BF16 = jnp.bfloat16
I32 = jnp.int32


def dot(a, b, ca, cb):
    return lax.dot_general(a, b, (((ca,), (cb,)), ((), ())), preferred_element_type=F32)


def eye(n, m):
    return lax.broadcasted_iota(I32, (n, m), 0) == lax.broadcasted_iota(I32, (n, m), 1)


def row_to_col(row, n):
    return jnp.sum(jnp.where(eye(n, row.shape[1]), row, 0.0), axis=1, keepdims=KEEP)


def col_to_row(col, m):
    return jnp.sum(jnp.where(eye(col.shape[0], m), col, 0.0), axis=0, keepdims=KEEP)


def lanes2(ref, i):
    return jnp.concatenate([ref[pl.ds(2 * i, 1), :], ref[pl.ds(2 * i + 1, 1), :]], axis=1)


def returned_pairs(v_ref, d_ref, mine, peers, first, w2, f0, f1):
    bins = lax.broadcasted_iota(I32, (H, N), 0)
    dv = d_ref[:].astype(F32)
    for j in BOTH:
        v = jnp.concatenate([v_ref[2 * j], v_ref[2 * j + 1]], axis=1).astype(F32)
        gs = []
        for table, row in ((mine, 4 + 2 * j), (peers, 2 * j)):
            t = lanes2(table, first + j)
            on = jnp.concatenate([dv[row:row + 1, :], dv[row + 1:row + 2, :]], axis=1)
            gs.append((jnp.where(bins == t, on, v) * (t < H).astype(F32)).astype(BF16))
        dz = dot(jnp.concatenate(gs, axis=0), w2[:], 0, 0)
        for tt in BOTH:
            for u in BOTH:
                for f, r in ((f0, L * tt + H * u), (f1, L * tt + H * u + Q)):
                    f[pl.ds(4 * u + 2 * j + tt, Q, stride=8), :] = dz[r:r + Q, :]


def make_kernel(batch):
    def kernel(z_h, mask_h, tb_h, m_h, mt_h, bm_h, wd_h, bd_h, wm_h, bmb_h,
               loss_o, dz_o, dm_o, dwd_o, dbd_o, dwm_o, dbm_o, vl_o, dl_o, tl_o, w2,
               zv, mv, mask_v, tb_v, mt_v, bm_v, wd_v, bd_v, wm_v, bmb_v,
               wt2, wmt, wmn, bias_c, mbias_c, lab, lts, ltp, ltr, l1n, l2n, t1o, t2o, t1r, t2r, mlab,
               cnt_s, cnt_r, rn, rz, f0, f1, ntn, ntf, vb, vr, db, dbh, dr, dwd_acc, dwm_acc, dbd_acc, dbm_acc, nll_acc,
               ps, pa, ph, px, pc, pb, pf, es, ea, eh, ex, ec, eb, ef,
               lsem, cs, cr, ls, lr, ns, nr, zs, zr, vs, vrs, ds, drs, ars, arr, ready):
        dp = lax.axis_index("dp")
        d = lax.axis_index("dap")
        chip, core = d // 2, d % 2
        dap_peer = {1: chip * 2 + (1 - core), 2: (1 - chip) * 2 + core, 3: (1 - chip) * 2 + (1 - core)}
        pz, py = dp // 2, dp % 2
        dp_peer = {1: pz * 2 + (1 - py), 2: (1 - pz) * 2 + py, 3: (1 - pz) * 2 + (1 - py)}
        near = pl.multiple_of(chip * L, L)
        far = pl.multiple_of((1 - chip) * L, L)
        half = (chip, 1 - chip)
        phalf = (1 - chip, chip)
        base = {k: pl.multiple_of(H * dap_peer[k], H) for k in PEERS}

        loc = []
        for n, (src, dst) in enumerate([(mask_h, mask_v), (tb_h, tb_v), (bm_h, bm_v), (mt_h, mt_v), (wd_h, wd_v),
                                        (bd_h, bd_v), (wm_h, wm_v), (bmb_h, bmb_v), (m_h, mv), (z_h, zv)]):
            c = pltpu.make_async_copy(src, dst, lsem.at[n])
            c.start()
            loc.append(c)

        bar = pltpu.get_barrier_semaphore()
        for k in PEERS:
            pl.semaphore_signal(bar, inc=1, device_id=(dp, dap_peer[k]), device_id_type=MESH)
        for k in (1, 2):
            @pl.when(dp_peer[k] > 0)
            def _():
                for there in (d, dap_peer[1]):
                    pl.semaphore_signal(bar, inc=1, device_id=(dp_peer[k], there), device_id_type=MESH)

        for n in QUARTERS:
            loc[n].wait()
        maskf = mask_v[:].astype(F32)
        bertf = bm_v[:].astype(F32)
        cd = jnp.sum(jnp.sum(maskf, axis=0, keepdims=KEEP), axis=1, keepdims=KEEP)
        cm = jnp.sum(jnp.sum(bertf, axis=0, keepdims=KEEP), axis=1, keepdims=KEEP)
        cnt_s[:8, :] = jnp.broadcast_to(cd, (8, L))
        cnt_s[8:16, :] = jnp.broadcast_to(cm, (8, L))
        labv = jnp.where(mask_v[:] > 0, tb_v[:], H)
        lab[:] = labv
        labf = labv.astype(F32)
        lts[:] = jnp.concatenate([labf, labf], axis=0).T
        low = lax.broadcasted_iota(I32, (Q, L), 1) < H
        for p in QUARTERS:
            ltp[p] = jnp.where(low, lts[H * p:H * p + Q, :], lts[H * p + Q:H * p + H, :])

        pl.semaphore_wait(bar, 3 + 4 * ((dp + 3) // 4))
        for k in (1, 2):
            @pl.when(dp_peer[k] == 0)
            def _():
                for there in (d, dap_peer[1]):
                    pl.semaphore_signal(ready, inc=1, device_id=(dp_peer[k], there), device_id_type=MESH)

        def rcopy(src, dst, s, r, dpi, dapi):
            return pltpu.make_async_remote_copy(src_ref=src, dst_ref=dst, send_sem=s, recv_sem=r,
                                                device_id=(dpi, dapi), device_id_type=MESH)

        cc, lc, zc = {}, {}, {}
        for k in (2, 3, 1):
            cc[k] = rcopy(cnt_s, cnt_r.at[k - 1], cs.at[k - 1], cr.at[k - 1], dp, dap_peer[k])
            cc[k].start()
        for k in (2, 3, 1):
            lc[k] = rcopy(ltp.at[dap_peer[k]], ltr.at[k - 1],
                          ls.at[k - 1], lr.at[k - 1], dp, dap_peer[k])
            lc[k].start()
        nc = {}
        for q in QUARTERS:
            nc[q] = rcopy(z_h.at[:, pl.ds(pl.multiple_of(base[1] + 16 * q, 16), 16), :], rn.at[q],
                          ns.at[q], nr.at[q], dp, dap_peer[1])
            for k in FAR:
                for b in BOTH:
                    cols = pl.multiple_of(base[k] + Q * phalf[b] + 8 * q, 8)
                    zc[k, q, b] = rcopy(z_h.at[Q * b:Q * b + Q, pl.ds(cols, 8), :], rz.at[k - 2, q, b],
                                        zs.at[k - 2, q, b], zr.at[k - 2, q, b], dp, dap_peer[k])
                    zc[k, q, b].start()
            nc[q].start()
        for n in range(4, 8):
            loc[n].wait()
        wt = wd_v[:]
        nat = wt.astype(F32).T.astype(BF16)
        wt2[:L, :] = nat
        wt2[L:N, :] = nat
        w2[:H, :] = wt
        w2[H:L, :] = wt
        wmt[:] = jnp.zeros_like(wmt)
        wmt[:CLS, :] = wm_v[:]
        wmn[:] = wmt[:].astype(F32).T.astype(BF16)
        bias_c[:] = jnp.broadcast_to(row_to_col(bd_v[:], H), (H, L))
        pad = lax.broadcasted_iota(I32, (Q, 1), 0) >= CLS
        mbias_c[:] = jnp.broadcast_to(jnp.where(pad, -1e30, row_to_col(bmb_v[:], Q)), (Q, L))
        l1n[:] = lab[:, pl.ds(near, L)]
        mlv = jnp.where(bm_v[:] > 0, mt_v[:], H)
        bm_v[:] = mlv
        mlab[:] = jnp.concatenate([bm_v[pl.ds(0, Q, stride=2), :], bm_v[pl.ds(1, Q, stride=2), :]], axis=1)
        for a in (dwd_acc, dwm_acc, dbd_acc, dbm_acc, nll_acc):
            a[:] = jnp.zeros_like(a)

        for k in PEERS:
            cc[k].wait_recv()
        tot = (cnt_s[:] + cnt_r[0]) + (cnt_r[1] + cnt_r[2])
        den_d = DIST_EPS + tot[:1, :]
        den_m = MSA_EPS + tot[8:9, :]
        cvd = (LOSS_SCALE * DIST_WEIGHT / batch) / den_d
        cvm = (LOSS_SCALE * MSA_WEIGHT / batch) / den_m
        cd2 = jnp.concatenate([cvd, cvd], axis=1)
        cm2 = jnp.concatenate([cvm, cvm], axis=1)

        def fold(a):
            return a[:, :L] + a[:, L:N]


        loc[8].wait()

        def msa(i, carry):
            m = mv[pl.ds(pl.multiple_of(N * i, N), N), :]
            b = mbias_c[:]
            l = dot(m, wmn[:], 1, 0).T + jnp.concatenate([b, b], axis=1)
            t = lanes2(mlab, i)
            mx = jnp.max(l, axis=0, keepdims=KEEP)
            e = jnp.exp(l - mx)
            s = jnp.sum(e, axis=0, keepdims=KEEP)
            eq = lax.broadcasted_iota(I32, (Q, N), 0) == t
            mk = (t < H).astype(F32)
            c = cm2 * mk
            h = (e * (c / s) - jnp.where(eq, c, 0.0)).astype(BF16)
            lt = jnp.sum(jnp.where(eq, l, 0.0), axis=0, keepdims=KEEP)
            nll_acc[1:2, :] += fold(mk * (mx + jnp.log(s)) - lt)
            dbm_acc[:] += fold(h.astype(F32))
            dm_o[pl.ds(pl.multiple_of(N * i, N), N), :] = dot(h, wmt[:], 0, 0).astype(BF16)
            dwm_acc[:] += dot(h, m, 1, 0)
            return carry

        lax.fori_loop(0, 16, msa, 0, unroll=4)


        for k in PEERS:
            lc[k].wait_recv()
        def turn(a):
            return pltpu.roll(a, H, 1)

        def unpack(p):
            return jnp.concatenate([jnp.where(low, p, turn(p)), jnp.where(low, turn(p), p)], axis=0)

        def paired(a):
            back = jnp.concatenate([pltpu.roll(a[8 * q:8 * q + 8, :], 4, 0) for q in QUARTERS], axis=0)
            return jnp.where(low, a, back).astype(I32)

        lane = lax.broadcasted_iota(I32, (Q, L), 1)
        upper = (lane % H >= Q).astype(I32)
        mine_low = upper == chip
        peer_low = upper == 1 - chip
        wide = lax.broadcasted_iota(I32, (H, L), 1) < H
        own_lt = lts[pl.ds(pl.multiple_of(H * d, H), H), :]
        l2n[:] = jnp.where(wide == (core == 0), own_lt, unpack(ltr[0])).astype(I32)
        l1f = lab[:, pl.ds(far, L)].astype(F32)
        for k in FAR:
            a = jnp.where(wide == (dap_peer[k] % 2 == 0), l1f, turn(l1f))
            t1o[k - 2] = paired(jnp.where(mine_low, a[:Q, :], a[Q:H, :]))
            got = ltr[k - 1]
            t2o[k - 2] = paired(jnp.where(low == mine_low, got, turn(got)))
            sent = ltp[dap_peer[k]]
            t1r[k - 2] = paired(jnp.where(low == peer_low, sent, turn(sent)))
            u = unpack(got)
            u = jnp.concatenate([u, u], axis=0).T
            t2r[k - 2] = paired(jnp.where(peer_low, u[:Q, :], u[Q:H, :]))
            tl_o[0, k - 2] = t1r[k - 2, 8 * LAST:Q, :]
            tl_o[1, k - 2] = t2r[k - 2, 8 * LAST:Q, :]

        def swap(src, nt, q, off):
            chunk = src.astype(F32)
            f0[:] = chunk[:, :8, :].reshape(512, L)
            f1[:] = chunk[:, 8:16, :].reshape(512, L)
            for t in range(8):
                nt[16 * q + t, pl.ds(off, H), :] = f0[pl.ds(t, H, stride=8), :].astype(BF16)
                nt[16 * q + 8 + t, pl.ds(off, H), :] = f1[pl.ds(t, H, stride=8), :].astype(BF16)

        bins = lax.broadcasted_iota(I32, (H, N), 0)

        def softmax_terms(zx, nx):
            b = bias_c[:]
            l = dot(jnp.concatenate([zx, nx], axis=1), wt2[:], 1, 0).T + jnp.concatenate([b, b], axis=1)
            mx = jnp.max(l, axis=0, keepdims=KEEP)
            e = jnp.exp(l - mx)
            s = jnp.sum(e, axis=0, keepdims=KEEP)
            return l, e, s, mx + jnp.log(s)

        def near_tile(i, carry):
            zx = zv[pl.ds(2 * i, 2), pl.ds(near, L), :].reshape(N, L)
            nx = ntn[pl.ds(2 * i, 2), :, :].reshape(N, L)
            l, e, s, lse = softmax_terms(zx, nx)
            t1 = lanes2(l1n, i)
            t2 = lanes2(l2n, i)
            eq1 = bins == t1
            m1 = (t1 < H).astype(F32)
            c1 = cd2 * m1
            c2 = cd2 * (t2 < H).astype(F32)
            g1 = (e * (c1 / s) - jnp.where(eq1, c1, 0.0)).astype(BF16)
            g2 = (e * (c2 / s) - jnp.where(bins == t2, c2, 0.0)).astype(BF16)
            lt = jnp.sum(jnp.where(eq1, l, 0.0), axis=0, keepdims=KEEP)
            nll_acc[:1, :] += fold(m1 * lse - lt)
            dbd_acc[:] += fold(g1.astype(F32))
            g = jnp.concatenate([g1, g2], axis=0)
            dz_o[pl.ds(2 * i, 2), pl.ds(near, L), :] = dot(g, w2[:], 0, 0).astype(BF16).reshape(2, L, L)
            dwd_acc[:] += dot(g, zx, 1, 0)
            return carry

        def own_tiles(k, q):
            for b in BOTH:
                zc[k, q, b].wait_recv()
                f0[:N, :] = rz[k - 2, q, b].astype(F32).reshape(N, L)
                for t in range(8):
                    r = H * (t // 4) + Q * b
                    ntf[k - 2, 4 * q + t % 4, r:r + Q, :] = f0[pl.ds(t, Q, stride=8), :].astype(BF16)

            def body(j, carry):
                spots = [(8 * q + 4 * u + 2 * j + tt + Q * half[b], pl.multiple_of(base[k] + Q * b, Q))
                         for tt in BOTH for u in BOTH for b in BOTH]
                zx = jnp.concatenate([zv[r, pl.ds(c, Q), :] for r, c in spots], axis=0)
                nx = ntf[k - 2, pl.ds(4 * q + 2 * j, 2), :, :].reshape(N, L)
                l, e, s, lse = softmax_terms(zx, nx)
                t1 = lanes2(t1o.at[k - 2], 4 * q + j)
                t2 = lanes2(t2o.at[k - 2], 4 * q + j)
                eq1 = bins == t1
                eq2 = bins == t2
                m1 = (t1 < H).astype(F32)
                m2 = (t2 < H).astype(F32)
                v = e * (cd2 / s)
                w = v - cd2
                d1 = jnp.sum(jnp.where(eq1, w, 0.0), axis=0, keepdims=KEEP)
                d2 = jnp.sum(jnp.where(eq2, w, 0.0), axis=0, keepdims=KEEP)
                g1 = (jnp.where(eq1, w, v) * m1).astype(BF16)
                g2 = (jnp.where(eq2, w, v) * m2).astype(BF16)
                lt = jnp.sum(jnp.where(eq1, l, 0.0) + jnp.where(eq2, l, 0.0), axis=0, keepdims=KEEP)
                nll_acc[:1, :] += fold((m1 + m2) * lse - lt)
                dbd_acc[:] += fold(g1.astype(F32) + g2.astype(F32))
                vh = v.astype(BF16)
                for tt in BOTH:
                    cut = slice(L * tt, L * tt + L)
                    vb[k - 2, q, 2 * j + tt] = vh[:, cut]
                    db[k - 2, q, pl.ds(2 * j + tt, 1), :] = d1[:, cut]
                    db[k - 2, q, pl.ds(4 + 2 * j + tt, 1), :] = d2[:, cut]
                g = jnp.concatenate([g1, g2], axis=0)
                dz = dot(g, w2[:], 0, 0).astype(BF16)
                for n, (r, c) in enumerate(spots):
                    dz_o[r, pl.ds(c, Q), :] = dz[Q * n:Q * n + Q, :]
                dwd_acc[:] += dot(g, zx, 1, 0) + dot(g, nx, 1, 0)
                return carry

            lax.fori_loop(0, 2, body, 0, unroll=2)
            dbh[k - 2, q] = db[k - 2, q].astype(BF16)

        vc, dc = {}, {}

        def give(k, q, when):
            unit = 2 * q + k - 2
            if when == SENT:
                v_to, d_to = (vr.at[k - 2, q], dr.at[k - 2, q]) if q < LAST else (vl_o.at[k - 2], dl_o.at[k - 2])
                vc[k, q] = rcopy(vb.at[k - 2, q], v_to, vs.at[k - 2, q], vrs.at[k - 2, q], dp, dap_peer[k])
                dc[k, q] = rcopy(dbh.at[k - 2, q], d_to, ds.at[k - 2, q], drs.at[k - 2, q], dp, dap_peer[k])

            def start():
                vc[k, q].start()
                dc[k, q].start()

            if (unit < EARLY) == when and unit not in SPLIT:
                start()
            if unit in SPLIT:
                pl.when((dp == 0) if when == SENT else (dp > 0))(start)

        def take(k, q):
            vc[k, q].wait_recv()
            dc[k, q].wait_recv()
            returned_pairs(vr.at[k - 2, q], dr.at[k - 2, q], t1r.at[k - 2], t2r.at[k - 2], 4 * q, w2, f0, f1)
            for b, f in ((0, f0), (1, f1)):
                cols = pl.multiple_of(base[k] + Q * phalf[b] + 8 * q, 8)
                dz_o[Q * b:Q * b + Q, pl.ds(cols, 8), :] = f[:N, :].reshape(Q, 8, L).astype(BF16)

        def reduction(src, ra, rh, rx, rc, rb, full, first):
            n = rh.shape[0]
            mine = pl.ds(pl.multiple_of(n * core, 8), n)
            other = pl.ds(pl.multiple_of(n * (1 - core), 8), n)

            def trio(halves, a, dst, sem, k):
                there = ((dp, dap_peer[1]), (dp_peer[k], d), (dp_peer[k], dap_peer[1]))
                group = [rcopy(a.at[rows, :], dst.at[m], ars.at[sem + m], arr.at[sem + m], *to)
                         for m, (rows, to) in enumerate(zip(halves, there))]
                for c in group:
                    c.start()
                return group

            one = trio((other, mine, other), src, ra, first, 1)
            yield
            for c in one:
                c.wait_recv()
            rh[:] = (src[mine, :] + ra[0]) + (ra[1] + ra[2])
            two = rcopy(rh, rx, ars.at[first + 6], arr.at[first + 6], dp, dap_peer[2])
            two.start()
            yield
            two.wait_recv()
            rc[:] = rh[:] + rx[:]
            three = trio((pl.ds(0, n),) * 3, rc, rb, first + 3, 2)
            yield
            for c in three:
                c.wait_recv()
            full[mine, :] = rc[:] + rb[1]
            full[other, :] = rb[0] + rb[2]
            for c in (*one, two, *three):
                c.wait_send()
            yield

        end = lax.broadcasted_iota(I32, (1, L), 1) == L - 1
        es[:CLS, :] = dwm_acc[:CLS, :L]
        es[CLS:2 * CLS, :] = dwm_acc[:CLS, L:N]
        nm = jnp.sum(nll_acc[1:2, :], axis=1, keepdims=KEEP)
        part = MSA_WEIGHT * nm / den_m / batch
        es[2 * CLS:47, :] = col_to_row(jnp.sum(dbm_acc[:], axis=1, keepdims=KEEP), L) + jnp.where(end, part, 0.0)
        es[47:48, :] = jnp.zeros((1, L), F32)

        @pl.when(dp == 0)
        def _():
            pl.semaphore_wait(ready, 4)

        soon = reduction(es, ea, eh, ex, ec, eb, ef, 7)
        next(soon)

        own_off = pl.multiple_of(H * core, H)
        oth_off = pl.multiple_of(H * (1 - core), H)
        loc[9].wait()
        for q in QUARTERS:
            swap(zv[:, pl.ds(pl.multiple_of(H * d + 16 * q, 16), 16), :], ntn, q, own_off)
        for q in QUARTERS:
            nc[q].wait_recv()
            swap(rn[q], ntn, q, oth_off)
        lax.fori_loop(0, Q, near_tile, 0, unroll=4)

        next(soon)
        for q in QUARTERS:
            for k in FAR:
                own_tiles(k, q)
                give(k, q, SENT)

        wd = ps.shape[0]
        ps[:H, :] = dwd_acc[:H, :] + dwd_acc[H:L, :]
        ps[H:wd, :] = jnp.zeros((wd - H, L), F32)
        nd = jnp.sum(nll_acc[:1, :], axis=1, keepdims=KEEP)
        part = DIST_WEIGHT * nd / den_d / batch
        ps[H:H + 1, :] = col_to_row(jnp.sum(dbd_acc[:], axis=1, keepdims=KEEP), L) + jnp.where(end, part, 0.0)
        late = reduction(ps, pa, ph, px, pc, pb, pf, 0)
        next(late)
        next(soon)
        next(late)
        for q in QUARTERS:
            for k in FAR:
                give(k, q, KEPT)
        for k in FAR:
            take(k, 0)
        next(soon)
        next(late)
        for k in FAR:
            take(k, 1)
        next(late)
        for k in FAR:
            take(k, 2)
        for k in FAR:
            vc[k, LAST].wait_recv()
            dc[k, LAST].wait_recv()
        dwd_o[:] = pf[:H, :]
        dwm_o[:, :L] = ef[:CLS, :]
        dwm_o[:, L:N] = ef[CLS:2 * CLS, :]
        row = pf[H:H + 1, :]
        mrow = ef[2 * CLS:47, :]
        dbd_o[:] = row[:, :H]
        dbm_o[:] = mrow[:, :CLS]
        loss_o[:] = pltpu.roll(row + mrow, 1, 1)[:, :1]

        for k in PEERS:
            cc[k].wait_send()
            lc[k].wait_send()
        for c in (*nc.values(), *zc.values(), *vc.values(), *dc.values()):
            c.wait_send()

    return kernel


def flush_kernel(loss_i, dz_i, dm_i, dwd_i, dbd_i, dwm_i, dbm_i, vl, dl, tl, w2,
                 loss_o, dz_o, dm_o, dwd_o, dbd_o, dwm_o, dbm_o, f0, f1, late, sem):
    d = lax.axis_index("dap")
    chip, core = d // 2, d % 2
    phalf = (1 - chip, chip)
    copies = []

    def put(src, dst):
        c = pltpu.make_async_copy(src, dst, sem.at[len(copies)])
        c.start()
        copies.append(c)

    def put_dz(r, rows, c, cols):
        put(dz_i.at[pl.ds(r, rows), pl.ds(c, cols), :], dz_o.at[pl.ds(r, rows), pl.ds(c, cols), :])

    for n in QUARTERS:
        put(dm_i.at[pl.ds(KIB * n, KIB), :], dm_o.at[pl.ds(KIB * n, KIB), :])
    for n in QUARTERS:
        put_dz(16 * n, 16, pl.multiple_of(L * chip, L), L)
    spots = {}
    for k, there in ((0, core), (1, 1 - core)):
        start = pl.multiple_of((1 - chip) * L + H * there, H)
        for b in BOTH:
            mid = pl.multiple_of(start + Q * phalf[b], Q)
            put_dz(Q * b, Q, mid, 24)
            put_dz(Q * b, Q, pl.multiple_of(start + Q * phalf[1 - b], Q), Q)
            spots[k, b] = pl.multiple_of(mid + 24, 8)
    for src, dst in ((loss_i, loss_o), (dwd_i, dwd_o), (dbd_i, dbd_o), (dwm_i, dwm_o), (dbm_i, dbm_o)):
        put(src, dst)
    for k in BOTH:
        returned_pairs(vl.at[k], dl.at[k], tl.at[0, k], tl.at[1, k], 0, w2, f0, f1)
        for b, f in ((0, f0), (1, f1)):
            late[k, b] = f[:].reshape(Q, 8, L).astype(BF16)
            put(late.at[k, b], dz_o.at[pl.ds(Q * b, Q), pl.ds(spots[k, b], 8), :])
    for c in copies:
        c.wait()


def solution(mesh):
    dp_size = mesh.shape["dp"]
    pair_spec = P("dp", "dap", None, None)
    pair_int_spec = P("dp", "dap", None)
    msa_spec = P("dp", None, "dap", None)
    msa_int_spec = P("dp", None, "dap")
    V = pltpu.VMEM

    def local_step(z, mask, tb, m, mt, bm, wd, bd, wm, bmb):
        args = (z.reshape(H, N, L), mask.reshape(H, N), tb.reshape(H, N), m.reshape(4096, N),
                mt.reshape(H, H), bm.reshape(H, H), wd.T, bd.reshape(1, H), wm.T, bmb.reshape(1, CLS))
        args = tuple(pltpu.with_memory_space_constraint(a, pltpu.HBM) for a in args)
        shapes = [((1, 1), F32), ((H, N, L), BF16), ((4096, N), BF16), ((H, L), F32), ((1, H), F32),
                  ((CLS, N), F32), ((1, CLS), F32)]
        scratch = [
            V((H, N, L), BF16), V((4096, N), BF16), *[V((H, N), I32)] * 2, V((H, H), I32),
            V((H, H), I32), V((H, L), BF16), V((1, H), F32), V((CLS, N), BF16), V((1, CLS), F32),
            V((N, H), BF16), V((Q, N), BF16), V((N, Q), BF16), V((H, L), F32), V((Q, L), F32),
            V((H, N), I32), V((N, L), F32), V((4, Q, L), F32), V((3, Q, L), F32), V((H, L), I32), V((H, L), I32),
            *[V((2, Q, L), I32)] * 4, V((Q, L), I32),
            V((16, L), F32), V((3, 16, L), F32), V((4, H, 16, L), BF16), V((2, 4, 2, Q, 8, L), BF16),
            V((512, L), F32), V((512, L), F32), V((H, L, L), BF16), V((2, 16, L, L), BF16),
            V((2, 4, 4, H, L), BF16), V((2, 3, 4, H, L), BF16), V((2, 4, 8, L), F32), V((2, 4, 8, L), BF16), V((2, 3, 8, L), BF16),
            V((L, L), F32), V((Q, N), F32), V((H, L), F32), V((Q, L), F32), V((8, L), F32),
            *(V((*lead, rows * n, L), F32) for n in (40, 24)
              for lead, rows in (((), 2), ((3,), 1), ((), 1), ((), 1), ((), 1), ((3,), 1), ((), 2))),
            DSEM((10,)), *[DSEM((3,))] * 4, DSEM((4,)), DSEM((4,)),
            *[DSEM((2, 4, 2))] * 2, *[DSEM((2, 4))] * 4,
            *[DSEM((14,))] * 2, pltpu.SemaphoreType.REGULAR,
        ]
        extra = [((2, 4, H, L), BF16), ((2, 8, L), BF16), ((2, 2, 8, L), I32), ((L, L), BF16)]
        vmem = [pl.BlockSpec(memory_space=pltpu.VMEM)]
        hbm = [pl.BlockSpec(memory_space=pltpu.HBM)]
        outs = pl.pallas_call(
            make_kernel(dp_size),
            out_shape=[pltpu.VMEM(s, t) for s, t in shapes + extra],
            in_specs=hbm * 10,
            out_specs=vmem * 11,
            scratch_shapes=scratch,
            compiler_params=pltpu.CompilerParams(collective_id=0, has_side_effects=True,
                                                 vmem_limit_bytes=44 * KIB * KIB),
        )(*args)
        outs = pl.pallas_call(
            flush_kernel,
            out_shape=[jax.ShapeDtypeStruct(s, t) for s, t in shapes],
            in_specs=vmem * 11,
            out_specs=hbm * 7,
            scratch_shapes=[V((N, L), F32), V((N, L), F32), V((2, 2, Q, 8, L), BF16), DSEM((25,))],
            compiler_params=pltpu.CompilerParams(vmem_limit_bytes=8 * KIB * KIB),
        )(*outs)
        loss, dz, dm, dwd, dbd, dwm, dbm = outs
        return (loss.reshape(()), dz.reshape(1, H, N, L), dm.reshape(1, H, H, N), dwd.T, dbd.reshape(H),
                dwm.T, dbm.reshape(CLS))

    return jax.shard_map(local_step, mesh=mesh,
                         in_specs=(pair_spec, pair_int_spec, pair_int_spec, msa_spec, msa_int_spec, msa_int_spec,
                                   P(), P(), P(), P()),
                         out_specs=(P(), pair_spec, msa_spec, P(), P(), P(), P()),
                         check_vma=False)
```

```python
import jax
import jax.numpy as jnp
from jax import lax
from jax.experimental import pallas as pl
from jax.experimental.pallas import tpu as pltpu
from jax.sharding import PartitionSpec as P

LOSS_SCALE = 2.0 ** 16
DIST_WEIGHT = 0.3
MSA_WEIGHT = 2.0
DIST_EPS = 1e-6
MSA_EPS = 1e-8
MESH = pl.DeviceIdType.MESH
DSEM = pltpu.SemaphoreType.DMA
KEEP = True
CLS = 23
Q = 32
EARLY = 4
SPLIT = (4,)
SENT, KEPT = True, False
PEERS = (1, 2, 3)
FAR = (2, 3)
BOTH = (0, 1)
QUARTERS = range(4)
KIB = 1024
LAST = 3
H = 64
L = 128
N = 256
F32 = jnp.float32
BF16 = jnp.bfloat16
I32 = jnp.int32


def dot(a, b, ca, cb):
    return lax.dot_general(a, b, (((ca,), (cb,)), ((), ())), preferred_element_type=F32)


def eye(n, m):
    return lax.broadcasted_iota(I32, (n, m), 0) == lax.broadcasted_iota(I32, (n, m), 1)


def row_to_col(row, n):
    return jnp.sum(jnp.where(eye(n, row.shape[1]), row, 0.0), axis=1, keepdims=KEEP)


def col_to_row(col, m):
    return jnp.sum(jnp.where(eye(col.shape[0], m), col, 0.0), axis=0, keepdims=KEEP)


def lanes2(ref, i):
    return jnp.concatenate([ref[pl.ds(2 * i, 1), :], ref[pl.ds(2 * i + 1, 1), :]], axis=1)


def returned_pairs(v_ref, d_ref, mine, peers, first, w2, f0, f1):
    bins = lax.broadcasted_iota(I32, (H, N), 0)
    dv = d_ref[:].astype(F32)
    for j in BOTH:
        v = jnp.concatenate([v_ref[2 * j], v_ref[2 * j + 1]], axis=1).astype(F32)
        gs = []
        for table, row in ((mine, 4 + 2 * j), (peers, 2 * j)):
            t = lanes2(table, first + j)
            on = jnp.concatenate([dv[row:row + 1, :], dv[row + 1:row + 2, :]], axis=1)
            gs.append((jnp.where(bins == t, on, v) * (t < H).astype(F32)).astype(BF16))
        dz = dot(jnp.concatenate(gs, axis=0), w2[:], 0, 0)
        for tt in BOTH:
            for u in BOTH:
                for f, r in ((f0, L * tt + H * u), (f1, L * tt + H * u + Q)):
                    f[pl.ds(4 * u + 2 * j + tt, Q, stride=8), :] = dz[r:r + Q, :]


def make_kernel(batch):
    def kernel(z_h, mask_h, tb_h, m_h, mt_h, bm_h, wd_h, bd_h, wm_h, bmb_h,
               loss_o, dz_o, dm_o, dwd_o, dbd_o, dwm_o, dbm_o, vl_o, dl_o, tl_o, w2,
               zv, mv, mask_v, tb_v, mt_v, bm_v, wd_v, bd_v, wm_v, bmb_v,
               wt2, wmt, wmn, bias_c, mbias_c, lab, lts, ltp, ltr, l1n, l2n, t1o, t2o, t1r, t2r, mlab,
               cnt_s, cnt_r, rn, rz, f0, f1, ntn, ntf, vb, vr, db, dbh, dr, dwd_acc, dwm_acc, dbd_acc, dbm_acc, nll_acc,
               ps, pa, ph, px, pc, pb, pf, es, ea, eh, ex, ec, eb, ef,
               lsem, cs, cr, ls, lr, ns, nr, zs, zr, vs, vrs, ds, drs, ars, arr, ready):
        dp = lax.axis_index("dp")
        d = lax.axis_index("dap")
        chip, core = d // 2, d % 2
        dap_peer = {1: chip * 2 + (1 - core), 2: (1 - chip) * 2 + core, 3: (1 - chip) * 2 + (1 - core)}
        pz, py = dp // 2, dp % 2
        dp_peer = {1: pz * 2 + (1 - py), 2: (1 - pz) * 2 + py, 3: (1 - pz) * 2 + (1 - py)}
        near = pl.multiple_of(chip * L, L)
        far = pl.multiple_of((1 - chip) * L, L)
        half = (chip, 1 - chip)
        phalf = (1 - chip, chip)
        base = {k: pl.multiple_of(H * dap_peer[k], H) for k in PEERS}

        loc = []
        for n, (src, dst) in enumerate([(mask_h, mask_v), (tb_h, tb_v), (bm_h, bm_v), (mt_h, mt_v), (wd_h, wd_v),
                                        (bd_h, bd_v), (wm_h, wm_v), (bmb_h, bmb_v), (m_h, mv), (z_h, zv)]):
            c = pltpu.make_async_copy(src, dst, lsem.at[n])
            c.start()
            loc.append(c)

        bar = pltpu.get_barrier_semaphore()
        for k in PEERS:
            pl.semaphore_signal(bar, inc=1, device_id=(dp, dap_peer[k]), device_id_type=MESH)
        for k in (1, 2):
            @pl.when(dp_peer[k] > 0)
            def _():
                for there in (d, dap_peer[1]):
                    pl.semaphore_signal(bar, inc=1, device_id=(dp_peer[k], there), device_id_type=MESH)

        for n in QUARTERS:
            loc[n].wait()
        maskf = mask_v[:].astype(F32)
        bertf = bm_v[:].astype(F32)
        cd = jnp.sum(jnp.sum(maskf, axis=0, keepdims=KEEP), axis=1, keepdims=KEEP)
        cm = jnp.sum(jnp.sum(bertf, axis=0, keepdims=KEEP), axis=1, keepdims=KEEP)
        cnt_s[:8, :] = jnp.broadcast_to(cd, (8, L))
        cnt_s[8:16, :] = jnp.broadcast_to(cm, (8, L))
        labv = jnp.where(mask_v[:] > 0, tb_v[:], H)
        lab[:] = labv
        labf = labv.astype(F32)
        lts[:] = jnp.concatenate([labf, labf], axis=0).T
        low = lax.broadcasted_iota(I32, (Q, L), 1) < H
        for p in QUARTERS:
            ltp[p] = jnp.where(low, lts[H * p:H * p + Q, :], lts[H * p + Q:H * p + H, :])

        pl.semaphore_wait(bar, 3 + 4 * ((dp + 3) // 4))
        for k in (1, 2):
            @pl.when(dp_peer[k] == 0)
            def _():
                for there in (d, dap_peer[1]):
                    pl.semaphore_signal(ready, inc=1, device_id=(dp_peer[k], there), device_id_type=MESH)

        def rcopy(src, dst, s, r, dpi, dapi):
            return pltpu.make_async_remote_copy(src_ref=src, dst_ref=dst, send_sem=s, recv_sem=r,
                                                device_id=(dpi, dapi), device_id_type=MESH)

        cc, lc, zc = {}, {}, {}
        for k in (2, 3, 1):
            cc[k] = rcopy(cnt_s, cnt_r.at[k - 1], cs.at[k - 1], cr.at[k - 1], dp, dap_peer[k])
            cc[k].start()
        for k in (2, 3, 1):
            lc[k] = rcopy(ltp.at[dap_peer[k]], ltr.at[k - 1],
                          ls.at[k - 1], lr.at[k - 1], dp, dap_peer[k])
            lc[k].start()
        nc = {}
        for q in QUARTERS:
            nc[q] = rcopy(z_h.at[:, pl.ds(pl.multiple_of(base[1] + 16 * q, 16), 16), :], rn.at[q],
                          ns.at[q], nr.at[q], dp, dap_peer[1])
            for k in FAR:
                for b in BOTH:
                    cols = pl.multiple_of(base[k] + Q * phalf[b] + 8 * q, 8)
                    zc[k, q, b] = rcopy(z_h.at[Q * b:Q * b + Q, pl.ds(cols, 8), :], rz.at[k - 2, q, b],
                                        zs.at[k - 2, q, b], zr.at[k - 2, q, b], dp, dap_peer[k])
                    zc[k, q, b].start()
            nc[q].start()
        for n in range(4, 8):
            loc[n].wait()
        wt = wd_v[:]
        nat = wt.astype(F32).T.astype(BF16)
        wt2[:L, :] = nat
        wt2[L:N, :] = nat
        w2[:H, :] = wt
        w2[H:L, :] = wt
        wmt[:] = jnp.zeros_like(wmt)
        wmt[:CLS, :] = wm_v[:]
        wmn[:] = wmt[:].astype(F32).T.astype(BF16)
        bias_c[:] = jnp.broadcast_to(row_to_col(bd_v[:], H), (H, L))
        pad = lax.broadcasted_iota(I32, (Q, 1), 0) >= CLS
        mbias_c[:] = jnp.broadcast_to(jnp.where(pad, -1e30, row_to_col(bmb_v[:], Q)), (Q, L))
        l1n[:] = lab[:, pl.ds(near, L)]
        mlv = jnp.where(bm_v[:] > 0, mt_v[:], H)
        bm_v[:] = mlv
        mlab[:] = jnp.concatenate([bm_v[pl.ds(0, Q, stride=2), :], bm_v[pl.ds(1, Q, stride=2), :]], axis=1)
        for a in (dwd_acc, dwm_acc, dbd_acc, dbm_acc, nll_acc):
            a[:] = jnp.zeros_like(a)

        for k in PEERS:
            cc[k].wait_recv()
        tot = (cnt_s[:] + cnt_r[0]) + (cnt_r[1] + cnt_r[2])
        den_d = DIST_EPS + tot[:1, :]
        den_m = MSA_EPS + tot[8:9, :]
        cvd = (LOSS_SCALE * DIST_WEIGHT / batch) / den_d
        cvm = (LOSS_SCALE * MSA_WEIGHT / batch) / den_m
        cd2 = jnp.concatenate([cvd, cvd], axis=1)
        cm2 = jnp.concatenate([cvm, cvm], axis=1)

        def fold(a):
            return a[:, :L] + a[:, L:N]


        loc[8].wait()

        def msa(i, carry):
            m = mv[pl.ds(pl.multiple_of(N * i, N), N), :]
            b = mbias_c[:]
            l = dot(m, wmn[:], 1, 0).T + jnp.concatenate([b, b], axis=1)
            t = lanes2(mlab, i)
            mx = jnp.max(l, axis=0, keepdims=KEEP)
            e = jnp.exp(l - mx)
            s = jnp.sum(e, axis=0, keepdims=KEEP)
            eq = lax.broadcasted_iota(I32, (Q, N), 0) == t
            mk = (t < H).astype(F32)
            c = cm2 * mk
            h = (e * (c / s) - jnp.where(eq, c, 0.0)).astype(BF16)
            lt = jnp.sum(jnp.where(eq, l, 0.0), axis=0, keepdims=KEEP)
            nll_acc[1:2, :] += fold(mk * (mx + jnp.log(s)) - lt)
            dbm_acc[:] += fold(h.astype(F32))
            dm_o[pl.ds(pl.multiple_of(N * i, N), N), :] = dot(h, wmt[:], 0, 0).astype(BF16)
            dwm_acc[:] += dot(h, m, 1, 0)
            return carry

        lax.fori_loop(0, 16, msa, 0, unroll=4)


        for k in PEERS:
            lc[k].wait_recv()
        def turn(a):
            return pltpu.roll(a, H, 1)

        def unpack(p):
            return jnp.concatenate([jnp.where(low, p, turn(p)), jnp.where(low, turn(p), p)], axis=0)

        def paired(a):
            back = jnp.concatenate([pltpu.roll(a[8 * q:8 * q + 8, :], 4, 0) for q in QUARTERS], axis=0)
            return jnp.where(low, a, back).astype(I32)

        lane = lax.broadcasted_iota(I32, (Q, L), 1)
        upper = (lane % H >= Q).astype(I32)
        mine_low = upper == chip
        peer_low = upper == 1 - chip
        wide = lax.broadcasted_iota(I32, (H, L), 1) < H
        own_lt = lts[pl.ds(pl.multiple_of(H * d, H), H), :]
        l2n[:] = jnp.where(wide == (core == 0), own_lt, unpack(ltr[0])).astype(I32)
        l1f = lab[:, pl.ds(far, L)].astype(F32)
        for k in FAR:
            a = jnp.where(wide == (dap_peer[k] % 2 == 0), l1f, turn(l1f))
            t1o[k - 2] = paired(jnp.where(mine_low, a[:Q, :], a[Q:H, :]))
            got = ltr[k - 1]
            t2o[k - 2] = paired(jnp.where(low == mine_low, got, turn(got)))
            sent = ltp[dap_peer[k]]
            t1r[k - 2] = paired(jnp.where(low == peer_low, sent, turn(sent)))
            u = unpack(got)
            u = jnp.concatenate([u, u], axis=0).T
            t2r[k - 2] = paired(jnp.where(peer_low, u[:Q, :], u[Q:H, :]))
            tl_o[0, k - 2] = t1r[k - 2, 8 * LAST:Q, :]
            tl_o[1, k - 2] = t2r[k - 2, 8 * LAST:Q, :]

        def swap(src, nt, q, off):
            chunk = src.astype(F32)
            f0[:] = chunk[:, :8, :].reshape(512, L)
            f1[:] = chunk[:, 8:16, :].reshape(512, L)
            for t in range(8):
                nt[16 * q + t, pl.ds(off, H), :] = f0[pl.ds(t, H, stride=8), :].astype(BF16)
                nt[16 * q + 8 + t, pl.ds(off, H), :] = f1[pl.ds(t, H, stride=8), :].astype(BF16)

        bins = lax.broadcasted_iota(I32, (H, N), 0)

        def softmax_terms(zx, nx):
            b = bias_c[:]
            l = dot(jnp.concatenate([zx, nx], axis=1), wt2[:], 1, 0).T + jnp.concatenate([b, b], axis=1)
            mx = jnp.max(l, axis=0, keepdims=KEEP)
            e = jnp.exp(l - mx)
            s = jnp.sum(e, axis=0, keepdims=KEEP)
            return l, e, s, mx + jnp.log(s)

        def near_tile(i, carry):
            zx = zv[pl.ds(2 * i, 2), pl.ds(near, L), :].reshape(N, L)
            nx = ntn[pl.ds(2 * i, 2), :, :].reshape(N, L)
            l, e, s, lse = softmax_terms(zx, nx)
            t1 = lanes2(l1n, i)
            t2 = lanes2(l2n, i)
            eq1 = bins == t1
            m1 = (t1 < H).astype(F32)
            c1 = cd2 * m1
            c2 = cd2 * (t2 < H).astype(F32)
            g1 = (e * (c1 / s) - jnp.where(eq1, c1, 0.0)).astype(BF16)
            g2 = (e * (c2 / s) - jnp.where(bins == t2, c2, 0.0)).astype(BF16)
            lt = jnp.sum(jnp.where(eq1, l, 0.0), axis=0, keepdims=KEEP)
            nll_acc[:1, :] += fold(m1 * lse - lt)
            dbd_acc[:] += fold(g1.astype(F32))
            g = jnp.concatenate([g1, g2], axis=0)
            dz_o[pl.ds(2 * i, 2), pl.ds(near, L), :] = dot(g, w2[:], 0, 0).astype(BF16).reshape(2, L, L)
            dwd_acc[:] += dot(g, zx, 1, 0)
            return carry

        def own_tiles(k, q):
            for b in BOTH:
                zc[k, q, b].wait_recv()
                f0[:N, :] = rz[k - 2, q, b].astype(F32).reshape(N, L)
                for t in range(8):
                    r = H * (t // 4) + Q * b
                    ntf[k - 2, 4 * q + t % 4, r:r + Q, :] = f0[pl.ds(t, Q, stride=8), :].astype(BF16)

            def body(j, carry):
                spots = [(8 * q + 4 * u + 2 * j + tt + Q * half[b], pl.multiple_of(base[k] + Q * b, Q))
                         for tt in BOTH for u in BOTH for b in BOTH]
                zx = jnp.concatenate([zv[r, pl.ds(c, Q), :] for r, c in spots], axis=0)
                nx = ntf[k - 2, pl.ds(4 * q + 2 * j, 2), :, :].reshape(N, L)
                l, e, s, lse = softmax_terms(zx, nx)
                t1 = lanes2(t1o.at[k - 2], 4 * q + j)
                t2 = lanes2(t2o.at[k - 2], 4 * q + j)
                eq1 = bins == t1
                eq2 = bins == t2
                m1 = (t1 < H).astype(F32)
                m2 = (t2 < H).astype(F32)
                v = e * (cd2 / s)
                w = v - cd2
                d1 = jnp.sum(jnp.where(eq1, w, 0.0), axis=0, keepdims=KEEP)
                d2 = jnp.sum(jnp.where(eq2, w, 0.0), axis=0, keepdims=KEEP)
                g1 = (jnp.where(eq1, w, v) * m1).astype(BF16)
                g2 = (jnp.where(eq2, w, v) * m2).astype(BF16)
                lt = jnp.sum(jnp.where(eq1, l, 0.0) + jnp.where(eq2, l, 0.0), axis=0, keepdims=KEEP)
                nll_acc[:1, :] += fold((m1 + m2) * lse - lt)
                dbd_acc[:] += fold(g1.astype(F32) + g2.astype(F32))
                vh = v.astype(BF16)
                for tt in BOTH:
                    cut = slice(L * tt, L * tt + L)
                    vb[k - 2, q, 2 * j + tt] = vh[:, cut]
                    db[k - 2, q, pl.ds(2 * j + tt, 1), :] = d1[:, cut]
                    db[k - 2, q, pl.ds(4 + 2 * j + tt, 1), :] = d2[:, cut]
                g = jnp.concatenate([g1, g2], axis=0)
                dz = dot(g, w2[:], 0, 0).astype(BF16)
                for n, (r, c) in enumerate(spots):
                    dz_o[r, pl.ds(c, Q), :] = dz[Q * n:Q * n + Q, :]
                dwd_acc[:] += dot(g, zx, 1, 0) + dot(g, nx, 1, 0)
                return carry

            lax.fori_loop(0, 2, body, 0, unroll=2)
            dbh[k - 2, q] = db[k - 2, q].astype(BF16)

        vc, dc = {}, {}

        def give(k, q, when):
            unit = 2 * q + k - 2
            if when == SENT:
                v_to, d_to = (vr.at[k - 2, q], dr.at[k - 2, q]) if q < LAST else (vl_o.at[k - 2], dl_o.at[k - 2])
                vc[k, q] = rcopy(vb.at[k - 2, q], v_to, vs.at[k - 2, q], vrs.at[k - 2, q], dp, dap_peer[k])
                dc[k, q] = rcopy(dbh.at[k - 2, q], d_to, ds.at[k - 2, q], drs.at[k - 2, q], dp, dap_peer[k])

            def start():
                vc[k, q].start()
                dc[k, q].start()

            if (unit < EARLY) == when and unit not in SPLIT:
                start()
            if unit in SPLIT:
                pl.when((dp == 0) if when == SENT else (dp > 0))(start)

        def take(k, q):
            vc[k, q].wait_recv()
            dc[k, q].wait_recv()
            returned_pairs(vr.at[k - 2, q], dr.at[k - 2, q], t1r.at[k - 2], t2r.at[k - 2], 4 * q, w2, f0, f1)
            for b, f in ((0, f0), (1, f1)):
                cols = pl.multiple_of(base[k] + Q * phalf[b] + 8 * q, 8)
                dz_o[Q * b:Q * b + Q, pl.ds(cols, 8), :] = f[:N, :].reshape(Q, 8, L).astype(BF16)

        def reduction(src, ra, rh, rx, rc, rb, full, first):
            n = rh.shape[0]
            mine = pl.ds(pl.multiple_of(n * core, 8), n)
            other = pl.ds(pl.multiple_of(n * (1 - core), 8), n)

            def trio(halves, a, dst, sem, k):
                there = ((dp, dap_peer[1]), (dp_peer[k], d), (dp_peer[k], dap_peer[1]))
                group = [rcopy(a.at[rows, :], dst.at[m], ars.at[sem + m], arr.at[sem + m], *to)
                         for m, (rows, to) in enumerate(zip(halves, there))]
                for c in group:
                    c.start()
                return group

            one = trio((other, mine, other), src, ra, first, 1)
            yield
            for c in one:
                c.wait_recv()
            rh[:] = (src[mine, :] + ra[0]) + (ra[1] + ra[2])
            two = rcopy(rh, rx, ars.at[first + 6], arr.at[first + 6], dp, dap_peer[2])
            two.start()
            yield
            two.wait_recv()
            rc[:] = rh[:] + rx[:]
            three = trio((pl.ds(0, n),) * 3, rc, rb, first + 3, 2)
            yield
            for c in three:
                c.wait_recv()
            full[mine, :] = rc[:] + rb[1]
            full[other, :] = rb[0] + rb[2]
            for c in (*one, two, *three):
                c.wait_send()
            yield

        end = lax.broadcasted_iota(I32, (1, L), 1) == L - 1
        es[:CLS, :] = dwm_acc[:CLS, :L]
        es[CLS:2 * CLS, :] = dwm_acc[:CLS, L:N]
        nm = jnp.sum(nll_acc[1:2, :], axis=1, keepdims=KEEP)
        part = MSA_WEIGHT * nm / den_m / batch
        es[2 * CLS:47, :] = col_to_row(jnp.sum(dbm_acc[:], axis=1, keepdims=KEEP), L) + jnp.where(end, part, 0.0)
        es[47:48, :] = jnp.zeros((1, L), F32)

        @pl.when(dp == 0)
        def _():
            pl.semaphore_wait(ready, 4)

        soon = reduction(es, ea, eh, ex, ec, eb, ef, 7)
        next(soon)

        own_off = pl.multiple_of(H * core, H)
        oth_off = pl.multiple_of(H * (1 - core), H)
        loc[9].wait()
        for q in QUARTERS:
            swap(zv[:, pl.ds(pl.multiple_of(H * d + 16 * q, 16), 16), :], ntn, q, own_off)
        for q in QUARTERS:
            nc[q].wait_recv()
            swap(rn[q], ntn, q, oth_off)
        lax.fori_loop(0, Q, near_tile, 0, unroll=4)

        next(soon)
        for q in QUARTERS:
            for k in FAR:
                own_tiles(k, q)
                give(k, q, SENT)

        wd = ps.shape[0]
        ps[:H, :] = dwd_acc[:H, :] + dwd_acc[H:L, :]
        ps[H:wd, :] = jnp.zeros((wd - H, L), F32)
        nd = jnp.sum(nll_acc[:1, :], axis=1, keepdims=KEEP)
        part = DIST_WEIGHT * nd / den_d / batch
        ps[H:H + 1, :] = col_to_row(jnp.sum(dbd_acc[:], axis=1, keepdims=KEEP), L) + jnp.where(end, part, 0.0)
        late = reduction(ps, pa, ph, px, pc, pb, pf, 0)
        next(late)
        next(soon)
        next(late)
        for q in QUARTERS:
            for k in FAR:
                give(k, q, KEPT)
        for k in FAR:
            take(k, 0)
        next(soon)
        next(late)
        for k in FAR:
            take(k, 1)
        for k in FAR:
            take(k, 2)
        next(late)
        for k in FAR:
            vc[k, LAST].wait_recv()
            dc[k, LAST].wait_recv()
        dwd_o[:] = pf[:H, :]
        dwm_o[:, :L] = ef[:CLS, :]
        dwm_o[:, L:N] = ef[CLS:2 * CLS, :]
        row = pf[H:H + 1, :]
        mrow = ef[2 * CLS:47, :]
        dbd_o[:] = row[:, :H]
        dbm_o[:] = mrow[:, :CLS]
        loss_o[:] = pltpu.roll(row + mrow, 1, 1)[:, :1]

        for k in PEERS:
            cc[k].wait_send()
            lc[k].wait_send()
        for c in (*nc.values(), *zc.values(), *vc.values(), *dc.values()):
            c.wait_send()

    return kernel


def flush_kernel(loss_i, dz_i, dm_i, dwd_i, dbd_i, dwm_i, dbm_i, vl, dl, tl, w2,
                 loss_o, dz_o, dm_o, dwd_o, dbd_o, dwm_o, dbm_o, f0, f1, late, sem):
    d = lax.axis_index("dap")
    chip, core = d // 2, d % 2
    phalf = (1 - chip, chip)
    copies = []

    def put(src, dst):
        c = pltpu.make_async_copy(src, dst, sem.at[len(copies)])
        c.start()
        copies.append(c)

    def put_dz(r, rows, c, cols):
        put(dz_i.at[pl.ds(r, rows), pl.ds(c, cols), :], dz_o.at[pl.ds(r, rows), pl.ds(c, cols), :])

    for n in QUARTERS:
        put(dm_i.at[pl.ds(KIB * n, KIB), :], dm_o.at[pl.ds(KIB * n, KIB), :])
    for n in QUARTERS:
        put_dz(16 * n, 16, pl.multiple_of(L * chip, L), L)
    spots = {}
    for k, there in ((0, core), (1, 1 - core)):
        start = pl.multiple_of((1 - chip) * L + H * there, H)
        for b in BOTH:
            mid = pl.multiple_of(start + Q * phalf[b], Q)
            put_dz(Q * b, Q, mid, 24)
            put_dz(Q * b, Q, pl.multiple_of(start + Q * phalf[1 - b], Q), Q)
            spots[k, b] = pl.multiple_of(mid + 24, 8)
    for src, dst in ((loss_i, loss_o), (dwd_i, dwd_o), (dbd_i, dbd_o), (dwm_i, dwm_o), (dbm_i, dbm_o)):
        put(src, dst)
    for k in BOTH:
        returned_pairs(vl.at[k], dl.at[k], tl.at[0, k], tl.at[1, k], 0, w2, f0, f1)
        for b, f in ((0, f0), (1, f1)):
            late[k, b] = f[:].reshape(Q, 8, L).astype(BF16)
            put(late.at[k, b], dz_o.at[pl.ds(Q * b, Q), pl.ds(spots[k, b], 8), :])
    for c in copies:
        c.wait()


def solution(mesh):
    dp_size = mesh.shape["dp"]
    pair_spec = P("dp", "dap", None, None)
    pair_int_spec = P("dp", "dap", None)
    msa_spec = P("dp", None, "dap", None)
    msa_int_spec = P("dp", None, "dap")
    V = pltpu.VMEM

    def local_step(z, mask, tb, m, mt, bm, wd, bd, wm, bmb):
        args = (z.reshape(H, N, L), mask.reshape(H, N), tb.reshape(H, N), m.reshape(4096, N),
                mt.reshape(H, H), bm.reshape(H, H), wd.T, bd.reshape(1, H), wm.T, bmb.reshape(1, CLS))
        args = tuple(pltpu.with_memory_space_constraint(a, pltpu.HBM) for a in args)
        shapes = [((1, 1), F32), ((H, N, L), BF16), ((4096, N), BF16), ((H, L), F32), ((1, H), F32),
                  ((CLS, N), F32), ((1, CLS), F32)]
        scratch = [
            V((H, N, L), BF16), V((4096, N), BF16), *[V((H, N), I32)] * 2, V((H, H), I32),
            V((H, H), I32), V((H, L), BF16), V((1, H), F32), V((CLS, N), BF16), V((1, CLS), F32),
            V((N, H), BF16), V((Q, N), BF16), V((N, Q), BF16), V((H, L), F32), V((Q, L), F32),
            V((H, N), I32), V((N, L), F32), V((4, Q, L), F32), V((3, Q, L), F32), V((H, L), I32), V((H, L), I32),
            *[V((2, Q, L), I32)] * 4, V((Q, L), I32),
            V((16, L), F32), V((3, 16, L), F32), V((4, H, 16, L), BF16), V((2, 4, 2, Q, 8, L), BF16),
            V((512, L), F32), V((512, L), F32), V((H, L, L), BF16), V((2, 16, L, L), BF16),
            V((2, 4, 4, H, L), BF16), V((2, 3, 4, H, L), BF16), V((2, 4, 8, L), F32), V((2, 4, 8, L), BF16), V((2, 3, 8, L), BF16),
            V((L, L), F32), V((Q, N), F32), V((H, L), F32), V((Q, L), F32), V((8, L), F32),
            *(V((*lead, rows * n, L), F32) for n in (40, 24)
              for lead, rows in (((), 2), ((3,), 1), ((), 1), ((), 1), ((), 1), ((3,), 1), ((), 2))),
            DSEM((10,)), *[DSEM((3,))] * 4, DSEM((4,)), DSEM((4,)),
            *[DSEM((2, 4, 2))] * 2, *[DSEM((2, 4))] * 4,
            *[DSEM((14,))] * 2, pltpu.SemaphoreType.REGULAR,
        ]
        extra = [((2, 4, H, L), BF16), ((2, 8, L), BF16), ((2, 2, 8, L), I32), ((L, L), BF16)]
        vmem = [pl.BlockSpec(memory_space=pltpu.VMEM)]
        hbm = [pl.BlockSpec(memory_space=pltpu.HBM)]
        outs = pl.pallas_call(
            make_kernel(dp_size),
            out_shape=[pltpu.VMEM(s, t) for s, t in shapes + extra],
            in_specs=hbm * 10,
            out_specs=vmem * 11,
            scratch_shapes=scratch,
            compiler_params=pltpu.CompilerParams(collective_id=0, has_side_effects=True,
                                                 vmem_limit_bytes=44 * KIB * KIB),
        )(*args)
        outs = pl.pallas_call(
            flush_kernel,
            out_shape=[jax.ShapeDtypeStruct(s, t) for s, t in shapes],
            in_specs=vmem * 11,
            out_specs=hbm * 7,
            scratch_shapes=[V((N, L), F32), V((N, L), F32), V((2, 2, Q, 8, L), BF16), DSEM((25,))],
            compiler_params=pltpu.CompilerParams(vmem_limit_bytes=8 * KIB * KIB),
        )(*outs)
        loss, dz, dm, dwd, dbd, dwm, dbm = outs
        return (loss.reshape(()), dz.reshape(1, H, N, L), dm.reshape(1, H, H, N), dwd.T, dbd.reshape(H),
                dwm.T, dbm.reshape(CLS))

    return jax.shard_map(local_step, mesh=mesh,
                         in_specs=(pair_spec, pair_int_spec, pair_int_spec, msa_spec, msa_int_spec, msa_int_spec,
                                   P(), P(), P(), P()),
                         out_specs=(P(), pair_spec, msa_spec, P(), P(), P(), P()),
                         check_vma=False)
```

```python
import jax
import jax.numpy as jnp
from jax import lax
from jax.experimental import pallas as pl
from jax.experimental.pallas import tpu as pltpu
from jax.sharding import PartitionSpec as P

LOSS_SCALE = 2.0 ** 16
DIST_WEIGHT = 0.3
MSA_WEIGHT = 2.0
DIST_EPS = 1e-6
MSA_EPS = 1e-8
MESH = pl.DeviceIdType.MESH
DSEM = pltpu.SemaphoreType.DMA
KEEP = True
CLS = 23
Q = 32
EARLY = 4
SPLIT = (4,)
SENT, KEPT = True, False
PEERS = (1, 2, 3)
FAR = (2, 3)
BOTH = (0, 1)
QUARTERS = range(4)
KIB = 1024
LAST = 3
H = 64
L = 128
N = 256
F32 = jnp.float32
BF16 = jnp.bfloat16
I32 = jnp.int32


def dot(a, b, ca, cb):
    return lax.dot_general(a, b, (((ca,), (cb,)), ((), ())), preferred_element_type=F32)


def eye(n, m):
    return lax.broadcasted_iota(I32, (n, m), 0) == lax.broadcasted_iota(I32, (n, m), 1)


def row_to_col(row, n):
    return jnp.sum(jnp.where(eye(n, row.shape[1]), row, 0.0), axis=1, keepdims=KEEP)


def col_to_row(col, m):
    return jnp.sum(jnp.where(eye(col.shape[0], m), col, 0.0), axis=0, keepdims=KEEP)


def lanes2(ref, i):
    return jnp.concatenate([ref[pl.ds(2 * i, 1), :], ref[pl.ds(2 * i + 1, 1), :]], axis=1)


def returned_pairs(v_ref, mine, peers, first, w2, f0, f1):
    bins = lax.broadcasted_iota(I32, (H, N), 0)
    dv = v_ref[N:, :].astype(F32)
    for j in BOTH:
        v = jnp.concatenate([v_ref[L * j:L * j + H, :], v_ref[L * j + H:L * j + L, :]], axis=1).astype(F32)
        gs = []
        for table, row in ((mine, 4 + 2 * j), (peers, 2 * j)):
            t = lanes2(table, first + j)
            on = jnp.concatenate([dv[row:row + 1, :], dv[row + 1:row + 2, :]], axis=1)
            gs.append((jnp.where(bins == t, on, v) * (t < H).astype(F32)).astype(BF16))
        dz = dot(jnp.concatenate(gs, axis=0), w2[:], 0, 0)
        for tt in BOTH:
            for u in BOTH:
                for f, r in ((f0, L * tt + H * u), (f1, L * tt + H * u + Q)):
                    f[pl.ds(4 * u + 2 * j + tt, Q, stride=8), :] = dz[r:r + Q, :]


def make_kernel(batch):
    def kernel(z_h, mask_h, tb_h, m_h, mt_h, bm_h, wd_h, bd_h, wm_h, bmb_h,
               loss_o, dz_o, dm_o, dwd_o, dbd_o, dwm_o, dbm_o, vl_o, tl_o, w2,
               zv, mv, mask_v, tb_v, mt_v, bm_v, wd_v, bd_v, wm_v, bmb_v,
               wt2, wmt, wmn, bias_c, mbias_c, lab, lts, ltp, ltr, l1n, l2n, t1o, t2o, t1r, t2r, mlab,
               cnt_s, cnt_r, rn, rz, f0, f1, ntn, ntf, vb, vr, db, dwd_acc, dwm_acc, dbd_acc, dbm_acc, nll_acc,
               ps, pa, ph, px, pc, pb, pf, es, ea, eh, ex, ec, eb, ef,
               lsem, cs, cr, ls, lr, ns, nr, zs, zr, vs, vrs, ars, arr, ready):
        dp = lax.axis_index("dp")
        d = lax.axis_index("dap")
        chip, core = d // 2, d % 2
        dap_peer = {1: chip * 2 + (1 - core), 2: (1 - chip) * 2 + core, 3: (1 - chip) * 2 + (1 - core)}
        pz, py = dp // 2, dp % 2
        dp_peer = {1: pz * 2 + (1 - py), 2: (1 - pz) * 2 + py, 3: (1 - pz) * 2 + (1 - py)}
        near = pl.multiple_of(chip * L, L)
        far = pl.multiple_of((1 - chip) * L, L)
        half = (chip, 1 - chip)
        phalf = (1 - chip, chip)
        base = {k: pl.multiple_of(H * dap_peer[k], H) for k in PEERS}

        loc = []
        for n, (src, dst) in enumerate([(mask_h, mask_v), (tb_h, tb_v), (bm_h, bm_v), (mt_h, mt_v), (wd_h, wd_v),
                                        (bd_h, bd_v), (wm_h, wm_v), (bmb_h, bmb_v), (m_h, mv), (z_h, zv)]):
            c = pltpu.make_async_copy(src, dst, lsem.at[n])
            c.start()
            loc.append(c)

        bar = pltpu.get_barrier_semaphore()
        for k in PEERS:
            pl.semaphore_signal(bar, inc=1, device_id=(dp, dap_peer[k]), device_id_type=MESH)
        for k in (1, 2):
            @pl.when(dp_peer[k] > 0)
            def _():
                for there in (d, dap_peer[1]):
                    pl.semaphore_signal(bar, inc=1, device_id=(dp_peer[k], there), device_id_type=MESH)

        for n in QUARTERS:
            loc[n].wait()
        maskf = mask_v[:].astype(F32)
        bertf = bm_v[:].astype(F32)
        cd = jnp.sum(jnp.sum(maskf, axis=0, keepdims=KEEP), axis=1, keepdims=KEEP)
        cm = jnp.sum(jnp.sum(bertf, axis=0, keepdims=KEEP), axis=1, keepdims=KEEP)
        cnt_s[:8, :] = jnp.broadcast_to(cd, (8, L))
        cnt_s[8:16, :] = jnp.broadcast_to(cm, (8, L))
        labv = jnp.where(mask_v[:] > 0, tb_v[:], H)
        lab[:] = labv
        labf = labv.astype(F32)
        lts[:] = jnp.concatenate([labf, labf], axis=0).T
        low = lax.broadcasted_iota(I32, (Q, L), 1) < H
        for p in QUARTERS:
            ltp[p] = jnp.where(low, lts[H * p:H * p + Q, :], lts[H * p + Q:H * p + H, :])

        pl.semaphore_wait(bar, 3 + 4 * ((dp + 3) // 4))
        for k in (1, 2):
            @pl.when(dp_peer[k] == 0)
            def _():
                for there in (d, dap_peer[1]):
                    pl.semaphore_signal(ready, inc=1, device_id=(dp_peer[k], there), device_id_type=MESH)

        def rcopy(src, dst, s, r, dpi, dapi):
            return pltpu.make_async_remote_copy(src_ref=src, dst_ref=dst, send_sem=s, recv_sem=r,
                                                device_id=(dpi, dapi), device_id_type=MESH)

        cc, lc, zc = {}, {}, {}
        for k in (2, 3, 1):
            cc[k] = rcopy(cnt_s, cnt_r.at[k - 1], cs.at[k - 1], cr.at[k - 1], dp, dap_peer[k])
            cc[k].start()
        for k in (2, 3, 1):
            lc[k] = rcopy(ltp.at[dap_peer[k]], ltr.at[k - 1],
                          ls.at[k - 1], lr.at[k - 1], dp, dap_peer[k])
            lc[k].start()
        nc = {}
        for q in QUARTERS:
            nc[q] = rcopy(z_h.at[:, pl.ds(pl.multiple_of(base[1] + 16 * q, 16), 16), :], rn.at[q],
                          ns.at[q], nr.at[q], dp, dap_peer[1])
            for k in FAR:
                for b in BOTH:
                    cols = pl.multiple_of(base[k] + Q * phalf[b] + 8 * q, 8)
                    zc[k, q, b] = rcopy(z_h.at[Q * b:Q * b + Q, pl.ds(cols, 8), :], rz.at[k - 2, q, b],
                                        zs.at[k - 2, q, b], zr.at[k - 2, q, b], dp, dap_peer[k])
                    zc[k, q, b].start()
            nc[q].start()
        for n in range(4, 8):
            loc[n].wait()
        wt = wd_v[:]
        nat = wt.astype(F32).T.astype(BF16)
        wt2[:L, :] = nat
        wt2[L:N, :] = nat
        w2[:H, :] = wt
        w2[H:L, :] = wt
        wmt[:] = jnp.zeros_like(wmt)
        wmt[:CLS, :] = wm_v[:]
        wmn[:] = wmt[:].astype(F32).T.astype(BF16)
        bias_c[:] = jnp.broadcast_to(row_to_col(bd_v[:], H), (H, L))
        pad = lax.broadcasted_iota(I32, (Q, 1), 0) >= CLS
        mbias_c[:] = jnp.broadcast_to(jnp.where(pad, -1e30, row_to_col(bmb_v[:], Q)), (Q, L))
        l1n[:] = lab[:, pl.ds(near, L)]
        mlv = jnp.where(bm_v[:] > 0, mt_v[:], H)
        bm_v[:] = mlv
        mlab[:] = jnp.concatenate([bm_v[pl.ds(0, Q, stride=2), :], bm_v[pl.ds(1, Q, stride=2), :]], axis=1)
        for a in (dwd_acc, dwm_acc, dbd_acc, dbm_acc, nll_acc):
            a[:] = jnp.zeros_like(a)

        for k in PEERS:
            cc[k].wait_recv()
        tot = (cnt_s[:] + cnt_r[0]) + (cnt_r[1] + cnt_r[2])
        den_d = DIST_EPS + tot[:1, :]
        den_m = MSA_EPS + tot[8:9, :]
        cvd = (LOSS_SCALE * DIST_WEIGHT / batch) / den_d
        cvm = (LOSS_SCALE * MSA_WEIGHT / batch) / den_m
        cd2 = jnp.concatenate([cvd, cvd], axis=1)
        cm2 = jnp.concatenate([cvm, cvm], axis=1)

        def fold(a):
            return a[:, :L] + a[:, L:N]


        loc[8].wait()

        def msa(i, carry):
            m = mv[pl.ds(pl.multiple_of(N * i, N), N), :]
            b = mbias_c[:]
            l = dot(m, wmn[:], 1, 0).T + jnp.concatenate([b, b], axis=1)
            t = lanes2(mlab, i)
            mx = jnp.max(l, axis=0, keepdims=KEEP)
            e = jnp.exp(l - mx)
            s = jnp.sum(e, axis=0, keepdims=KEEP)
            eq = lax.broadcasted_iota(I32, (Q, N), 0) == t
            mk = (t < H).astype(F32)
            c = cm2 * mk
            h = (e * (c / s) - jnp.where(eq, c, 0.0)).astype(BF16)
            lt = jnp.sum(jnp.where(eq, l, 0.0), axis=0, keepdims=KEEP)
            nll_acc[1:2, :] += fold(mk * (mx + jnp.log(s)) - lt)
            dbm_acc[:] += fold(h.astype(F32))
            dm_o[pl.ds(pl.multiple_of(N * i, N), N), :] = dot(h, wmt[:], 0, 0).astype(BF16)
            dwm_acc[:] += dot(h, m, 1, 0)
            return carry

        lax.fori_loop(0, 16, msa, 0, unroll=4)


        for k in PEERS:
            lc[k].wait_recv()
        def turn(a):
            return pltpu.roll(a, H, 1)

        def unpack(p):
            return jnp.concatenate([jnp.where(low, p, turn(p)), jnp.where(low, turn(p), p)], axis=0)

        def paired(a):
            back = jnp.concatenate([pltpu.roll(a[8 * q:8 * q + 8, :], 4, 0) for q in QUARTERS], axis=0)
            return jnp.where(low, a, back).astype(I32)

        lane = lax.broadcasted_iota(I32, (Q, L), 1)
        upper = (lane % H >= Q).astype(I32)
        mine_low = upper == chip
        peer_low = upper == 1 - chip
        wide = lax.broadcasted_iota(I32, (H, L), 1) < H
        own_lt = lts[pl.ds(pl.multiple_of(H * d, H), H), :]
        l2n[:] = jnp.where(wide == (core == 0), own_lt, unpack(ltr[0])).astype(I32)
        l1f = lab[:, pl.ds(far, L)].astype(F32)
        for k in FAR:
            a = jnp.where(wide == (dap_peer[k] % 2 == 0), l1f, turn(l1f))
            t1o[k - 2] = paired(jnp.where(mine_low, a[:Q, :], a[Q:H, :]))
            got = ltr[k - 1]
            t2o[k - 2] = paired(jnp.where(low == mine_low, got, turn(got)))
            sent = ltp[dap_peer[k]]
            t1r[k - 2] = paired(jnp.where(low == peer_low, sent, turn(sent)))
            u = unpack(got)
            u = jnp.concatenate([u, u], axis=0).T
            t2r[k - 2] = paired(jnp.where(peer_low, u[:Q, :], u[Q:H, :]))
            tl_o[0, k - 2] = t1r[k - 2, 8 * LAST:Q, :]
            tl_o[1, k - 2] = t2r[k - 2, 8 * LAST:Q, :]

        def swap(src, nt, q, off):
            chunk = src.astype(F32)
            f0[:] = chunk[:, :8, :].reshape(512, L)
            f1[:] = chunk[:, 8:16, :].reshape(512, L)
            for t in range(8):
                nt[16 * q + t, pl.ds(off, H), :] = f0[pl.ds(t, H, stride=8), :].astype(BF16)
                nt[16 * q + 8 + t, pl.ds(off, H), :] = f1[pl.ds(t, H, stride=8), :].astype(BF16)

        bins = lax.broadcasted_iota(I32, (H, N), 0)

        def softmax_terms(zx, nx):
            b = bias_c[:]
            l = dot(jnp.concatenate([zx, nx], axis=1), wt2[:], 1, 0).T + jnp.concatenate([b, b], axis=1)
            mx = jnp.max(l, axis=0, keepdims=KEEP)
            e = jnp.exp(l - mx)
            s = jnp.sum(e, axis=0, keepdims=KEEP)
            return l, e, s, mx + jnp.log(s)

        def near_tile(i, carry):
            zx = zv[pl.ds(2 * i, 2), pl.ds(near, L), :].reshape(N, L)
            nx = ntn[pl.ds(2 * i, 2), :, :].reshape(N, L)
            l, e, s, lse = softmax_terms(zx, nx)
            t1 = lanes2(l1n, i)
            t2 = lanes2(l2n, i)
            eq1 = bins == t1
            m1 = (t1 < H).astype(F32)
            c1 = cd2 * m1
            c2 = cd2 * (t2 < H).astype(F32)
            g1 = (e * (c1 / s) - jnp.where(eq1, c1, 0.0)).astype(BF16)
            g2 = (e * (c2 / s) - jnp.where(bins == t2, c2, 0.0)).astype(BF16)
            lt = jnp.sum(jnp.where(eq1, l, 0.0), axis=0, keepdims=KEEP)
            nll_acc[:1, :] += fold(m1 * lse - lt)
            dbd_acc[:] += fold(g1.astype(F32))
            g = jnp.concatenate([g1, g2], axis=0)
            dz_o[pl.ds(2 * i, 2), pl.ds(near, L), :] = dot(g, w2[:], 0, 0).astype(BF16).reshape(2, L, L)
            dwd_acc[:] += dot(g, zx, 1, 0)
            return carry

        def own_tiles(k, q):
            for b in BOTH:
                zc[k, q, b].wait_recv()
                f0[:N, :] = rz[k - 2, q, b].astype(F32).reshape(N, L)
                for t in range(8):
                    r = H * (t // 4) + Q * b
                    ntf[k - 2, 4 * q + t % 4, r:r + Q, :] = f0[pl.ds(t, Q, stride=8), :].astype(BF16)

            def body(j, carry):
                spots = [(8 * q + 4 * u + 2 * j + tt + Q * half[b], pl.multiple_of(base[k] + Q * b, Q))
                         for tt in BOTH for u in BOTH for b in BOTH]
                zx = jnp.concatenate([zv[r, pl.ds(c, Q), :] for r, c in spots], axis=0)
                nx = ntf[k - 2, pl.ds(4 * q + 2 * j, 2), :, :].reshape(N, L)
                l, e, s, lse = softmax_terms(zx, nx)
                t1 = lanes2(t1o.at[k - 2], 4 * q + j)
                t2 = lanes2(t2o.at[k - 2], 4 * q + j)
                eq1 = bins == t1
                eq2 = bins == t2
                m1 = (t1 < H).astype(F32)
                m2 = (t2 < H).astype(F32)
                v = e * (cd2 / s)
                w = v - cd2
                d1 = jnp.sum(jnp.where(eq1, w, 0.0), axis=0, keepdims=KEEP)
                d2 = jnp.sum(jnp.where(eq2, w, 0.0), axis=0, keepdims=KEEP)
                g1 = (jnp.where(eq1, w, v) * m1).astype(BF16)
                g2 = (jnp.where(eq2, w, v) * m2).astype(BF16)
                lt = jnp.sum(jnp.where(eq1, l, 0.0) + jnp.where(eq2, l, 0.0), axis=0, keepdims=KEEP)
                nll_acc[:1, :] += fold((m1 + m2) * lse - lt)
                dbd_acc[:] += fold(g1.astype(F32) + g2.astype(F32))
                vh = v.astype(BF16)
                for tt in BOTH:
                    cut = slice(L * tt, L * tt + L)
                    vb[k - 2, q, pl.ds(pl.multiple_of(L * j + H * tt, H), H), :] = vh[:, cut]
                    db[k - 2, q, pl.ds(2 * j + tt, 1), :] = d1[:, cut]
                    db[k - 2, q, pl.ds(4 + 2 * j + tt, 1), :] = d2[:, cut]
                g = jnp.concatenate([g1, g2], axis=0)
                dz = dot(g, w2[:], 0, 0).astype(BF16)
                for n, (r, c) in enumerate(spots):
                    dz_o[r, pl.ds(c, Q), :] = dz[Q * n:Q * n + Q, :]
                dwd_acc[:] += dot(g, zx, 1, 0) + dot(g, nx, 1, 0)
                return carry

            lax.fori_loop(0, 2, body, 0, unroll=2)
            vb[k - 2, q, N:, :] = db[k - 2, q].astype(BF16)

        vc = {}

        def give(k, q, when):
            unit = 2 * q + k - 2
            if when == SENT:
                v_to = vr.at[k - 2, q] if q < LAST else vl_o.at[k - 2]
                vc[k, q] = rcopy(vb.at[k - 2, q], v_to, vs.at[k - 2, q], vrs.at[k - 2, q], dp, dap_peer[k])

            def start():
                vc[k, q].start()

            if (unit < EARLY) == when and unit not in SPLIT:
                start()
            if unit in SPLIT:
                pl.when((dp == 0) if when == SENT else (dp > 0))(start)

        def take(k, q):
            vc[k, q].wait_recv()
            returned_pairs(vr.at[k - 2, q], t1r.at[k - 2], t2r.at[k - 2], 4 * q, w2, f0, f1)
            for b, f in ((0, f0), (1, f1)):
                cols = pl.multiple_of(base[k] + Q * phalf[b] + 8 * q, 8)
                dz_o[Q * b:Q * b + Q, pl.ds(cols, 8), :] = f[:N, :].reshape(Q, 8, L).astype(BF16)

        def reduction(src, ra, rh, rx, rc, rb, full, first):
            n = rh.shape[0]
            mine = pl.ds(pl.multiple_of(n * core, 8), n)
            other = pl.ds(pl.multiple_of(n * (1 - core), 8), n)

            def trio(halves, a, dst, sem, k):
                there = ((dp, dap_peer[1]), (dp_peer[k], d), (dp_peer[k], dap_peer[1]))
                group = [rcopy(a.at[rows, :], dst.at[m], ars.at[sem + m], arr.at[sem + m], *to)
                         for m, (rows, to) in enumerate(zip(halves, there))]
                for c in group:
                    c.start()
                return group

            one = trio((other, mine, other), src, ra, first, 1)
            yield
            for c in one:
                c.wait_recv()
            rh[:] = (src[mine, :] + ra[0]) + (ra[1] + ra[2])
            two = rcopy(rh, rx, ars.at[first + 6], arr.at[first + 6], dp, dap_peer[2])
            two.start()
            yield
            two.wait_recv()
            rc[:] = rh[:] + rx[:]
            three = trio((pl.ds(0, n),) * 3, rc, rb, first + 3, 2)
            yield
            for c in three:
                c.wait_recv()
            full[mine, :] = rc[:] + rb[1]
            full[other, :] = rb[0] + rb[2]
            for c in (*one, two, *three):
                c.wait_send()
            yield

        end = lax.broadcasted_iota(I32, (1, L), 1) == L - 1
        es[:CLS, :] = dwm_acc[:CLS, :L]
        es[CLS:2 * CLS, :] = dwm_acc[:CLS, L:N]
        nm = jnp.sum(nll_acc[1:2, :], axis=1, keepdims=KEEP)
        part = MSA_WEIGHT * nm / den_m / batch
        es[2 * CLS:47, :] = col_to_row(jnp.sum(dbm_acc[:], axis=1, keepdims=KEEP), L) + jnp.where(end, part, 0.0)
        es[47:48, :] = jnp.zeros((1, L), F32)

        @pl.when(dp == 0)
        def _():
            pl.semaphore_wait(ready, 4)

        soon = reduction(es, ea, eh, ex, ec, eb, ef, 7)
        next(soon)

        own_off = pl.multiple_of(H * core, H)
        oth_off = pl.multiple_of(H * (1 - core), H)
        loc[9].wait()
        for q in QUARTERS:
            swap(zv[:, pl.ds(pl.multiple_of(H * d + 16 * q, 16), 16), :], ntn, q, own_off)
        for q in QUARTERS:
            nc[q].wait_recv()
            swap(rn[q], ntn, q, oth_off)
        lax.fori_loop(0, Q, near_tile, 0, unroll=4)

        next(soon)
        for q in QUARTERS:
            for k in FAR:
                own_tiles(k, q)
                give(k, q, SENT)

        wd = ps.shape[0]
        ps[:H, :] = dwd_acc[:H, :] + dwd_acc[H:L, :]
        ps[H:wd, :] = jnp.zeros((wd - H, L), F32)
        nd = jnp.sum(nll_acc[:1, :], axis=1, keepdims=KEEP)
        part = DIST_WEIGHT * nd / den_d / batch
        ps[H:H + 1, :] = col_to_row(jnp.sum(dbd_acc[:], axis=1, keepdims=KEEP), L) + jnp.where(end, part, 0.0)
        late = reduction(ps, pa, ph, px, pc, pb, pf, 0)
        next(late)
        next(soon)
        next(late)
        for q in QUARTERS:
            for k in FAR:
                give(k, q, KEPT)
        for k in FAR:
            take(k, 0)
        next(soon)
        next(late)
        for k in FAR:
            take(k, 1)
        for k in FAR:
            take(k, 2)
        next(late)
        for k in FAR:
            vc[k, LAST].wait_recv()
        dwd_o[:] = pf[:H, :]
        dwm_o[:, :L] = ef[:CLS, :]
        dwm_o[:, L:N] = ef[CLS:2 * CLS, :]
        row = pf[H:H + 1, :]
        mrow = ef[2 * CLS:47, :]
        dbd_o[:] = row[:, :H]
        dbm_o[:] = mrow[:, :CLS]
        loss_o[:] = pltpu.roll(row + mrow, 1, 1)[:, :1]

        for k in PEERS:
            cc[k].wait_send()
            lc[k].wait_send()
        for c in (*nc.values(), *zc.values(), *vc.values()):
            c.wait_send()

    return kernel


def flush_kernel(loss_i, dz_i, dm_i, dwd_i, dbd_i, dwm_i, dbm_i, vl, tl, w2,
                 loss_o, dz_o, dm_o, dwd_o, dbd_o, dwm_o, dbm_o, f0, f1, late, sem):
    d = lax.axis_index("dap")
    chip, core = d // 2, d % 2
    phalf = (1 - chip, chip)
    copies = []

    def put(src, dst):
        c = pltpu.make_async_copy(src, dst, sem.at[len(copies)])
        c.start()
        copies.append(c)

    def put_dz(r, rows, c, cols):
        put(dz_i.at[pl.ds(r, rows), pl.ds(c, cols), :], dz_o.at[pl.ds(r, rows), pl.ds(c, cols), :])

    for n in QUARTERS:
        put(dm_i.at[pl.ds(KIB * n, KIB), :], dm_o.at[pl.ds(KIB * n, KIB), :])
    for n in QUARTERS:
        put_dz(16 * n, 16, pl.multiple_of(L * chip, L), L)
    spots = {}
    for k, there in ((0, core), (1, 1 - core)):
        start = pl.multiple_of((1 - chip) * L + H * there, H)
        for b in BOTH:
            mid = pl.multiple_of(start + Q * phalf[b], Q)
            put_dz(Q * b, Q, mid, 24)
            put_dz(Q * b, Q, pl.multiple_of(start + Q * phalf[1 - b], Q), Q)
            spots[k, b] = pl.multiple_of(mid + 24, 8)
    for src, dst in ((loss_i, loss_o), (dwd_i, dwd_o), (dbd_i, dbd_o), (dwm_i, dwm_o), (dbm_i, dbm_o)):
        put(src, dst)
    for k in BOTH:
        returned_pairs(vl.at[k], tl.at[0, k], tl.at[1, k], 0, w2, f0, f1)
        for b, f in ((0, f0), (1, f1)):
            late[k, b] = f[:].reshape(Q, 8, L).astype(BF16)
            put(late.at[k, b], dz_o.at[pl.ds(Q * b, Q), pl.ds(spots[k, b], 8), :])
    for c in copies:
        c.wait()


def solution(mesh):
    dp_size = mesh.shape["dp"]
    pair_spec = P("dp", "dap", None, None)
    pair_int_spec = P("dp", "dap", None)
    msa_spec = P("dp", None, "dap", None)
    msa_int_spec = P("dp", None, "dap")
    V = pltpu.VMEM

    def local_step(z, mask, tb, m, mt, bm, wd, bd, wm, bmb):
        args = (z.reshape(H, N, L), mask.reshape(H, N), tb.reshape(H, N), m.reshape(4096, N),
                mt.reshape(H, H), bm.reshape(H, H), wd.T, bd.reshape(1, H), wm.T, bmb.reshape(1, CLS))
        args = tuple(pltpu.with_memory_space_constraint(a, pltpu.HBM) for a in args)
        shapes = [((1, 1), F32), ((H, N, L), BF16), ((4096, N), BF16), ((H, L), F32), ((1, H), F32),
                  ((CLS, N), F32), ((1, CLS), F32)]
        scratch = [
            V((H, N, L), BF16), V((4096, N), BF16), *[V((H, N), I32)] * 2, V((H, H), I32),
            V((H, H), I32), V((H, L), BF16), V((1, H), F32), V((CLS, N), BF16), V((1, CLS), F32),
            V((N, H), BF16), V((Q, N), BF16), V((N, Q), BF16), V((H, L), F32), V((Q, L), F32),
            V((H, N), I32), V((N, L), F32), V((4, Q, L), F32), V((3, Q, L), F32), V((H, L), I32), V((H, L), I32),
            *[V((2, Q, L), I32)] * 4, V((Q, L), I32),
            V((16, L), F32), V((3, 16, L), F32), V((4, H, 16, L), BF16), V((2, 4, 2, Q, 8, L), BF16),
            V((512, L), F32), V((512, L), F32), V((H, L, L), BF16), V((2, 16, L, L), BF16),
            V((2, 4, N + 8, L), BF16), V((2, 3, N + 8, L), BF16), V((2, 4, 8, L), F32),
            V((L, L), F32), V((Q, N), F32), V((H, L), F32), V((Q, L), F32), V((8, L), F32),
            *(V((*lead, rows * n, L), F32) for n in (40, 24)
              for lead, rows in (((), 2), ((3,), 1), ((), 1), ((), 1), ((), 1), ((3,), 1), ((), 2))),
            DSEM((10,)), *[DSEM((3,))] * 4, DSEM((4,)), DSEM((4,)),
            *[DSEM((2, 4, 2))] * 2, *[DSEM((2, 4))] * 2,
            *[DSEM((14,))] * 2, pltpu.SemaphoreType.REGULAR,
        ]
        extra = [((2, N + 8, L), BF16), ((2, 2, 8, L), I32), ((L, L), BF16)]
        vmem = [pl.BlockSpec(memory_space=pltpu.VMEM)]
        hbm = [pl.BlockSpec(memory_space=pltpu.HBM)]
        outs = pl.pallas_call(
            make_kernel(dp_size),
            out_shape=[pltpu.VMEM(s, t) for s, t in shapes + extra],
            in_specs=hbm * 10,
            out_specs=vmem * 10,
            scratch_shapes=scratch,
            compiler_params=pltpu.CompilerParams(collective_id=0, has_side_effects=True,
                                                 vmem_limit_bytes=44 * KIB * KIB),
        )(*args)
        outs = pl.pallas_call(
            flush_kernel,
            out_shape=[jax.ShapeDtypeStruct(s, t) for s, t in shapes],
            in_specs=vmem * 10,
            out_specs=hbm * 7,
            scratch_shapes=[V((N, L), F32), V((N, L), F32), V((2, 2, Q, 8, L), BF16), DSEM((25,))],
            compiler_params=pltpu.CompilerParams(vmem_limit_bytes=8 * KIB * KIB),
        )(*outs)
        loss, dz, dm, dwd, dbd, dwm, dbm = outs
        return (loss.reshape(()), dz.reshape(1, H, N, L), dm.reshape(1, H, H, N), dwd.T, dbd.reshape(H),
                dwm.T, dbm.reshape(CLS))

    return jax.shard_map(local_step, mesh=mesh,
                         in_specs=(pair_spec, pair_int_spec, pair_int_spec, msa_spec, msa_int_spec, msa_int_spec,
                                   P(), P(), P(), P()),
                         out_specs=(P(), pair_spec, msa_spec, P(), P(), P(), P()),
                         check_vma=False)
```

```python
import jax
import jax.numpy as jnp
from jax import lax
from jax.experimental import pallas as pl
from jax.experimental.pallas import tpu as pltpu
from jax.sharding import PartitionSpec as P

LOSS_SCALE = 2.0 ** 16
DIST_WEIGHT = 0.3
MSA_WEIGHT = 2.0
DIST_EPS = 1e-6
MSA_EPS = 1e-8
MESH = pl.DeviceIdType.MESH
DSEM = pltpu.SemaphoreType.DMA
KEEP = True
CLS = 23
Q = 32
EARLY = 4
SPLIT = (4,)
SENT, KEPT = True, False
PEERS = (1, 2, 3)
FAR = (2, 3)
BOTH = (0, 1)
QUARTERS = range(4)
KIB = 1024
LAST = 3
H = 64
L = 128
N = 256
F32 = jnp.float32
BF16 = jnp.bfloat16
I32 = jnp.int32


def dot(a, b, ca, cb):
    return lax.dot_general(a, b, (((ca,), (cb,)), ((), ())), preferred_element_type=F32)


def eye(n, m):
    return lax.broadcasted_iota(I32, (n, m), 0) == lax.broadcasted_iota(I32, (n, m), 1)


def row_to_col(row, n):
    return jnp.sum(jnp.where(eye(n, row.shape[1]), row, 0.0), axis=1, keepdims=KEEP)


def col_to_row(col, m):
    return jnp.sum(jnp.where(eye(col.shape[0], m), col, 0.0), axis=0, keepdims=KEEP)


def lanes2(ref, i):
    return jnp.concatenate([ref[pl.ds(2 * i, 1), :], ref[pl.ds(2 * i + 1, 1), :]], axis=1)


def returned_pairs(v_ref, mine, peers, first, w2, f0, f1):
    bins = lax.broadcasted_iota(I32, (H, N), 0)
    dv = v_ref[N:, :].astype(F32)
    for j in BOTH:
        v = jnp.concatenate([v_ref[L * j:L * j + H, :], v_ref[L * j + H:L * j + L, :]], axis=1).astype(F32)
        gs = []
        for table, row in ((mine, 4 + 2 * j), (peers, 2 * j)):
            t = lanes2(table, first + j)
            on = jnp.concatenate([dv[row:row + 1, :], dv[row + 1:row + 2, :]], axis=1)
            gs.append((jnp.where(bins == t, on, v) * (t < H).astype(F32)).astype(BF16))
        dz = dot(jnp.concatenate(gs, axis=0), w2[:], 0, 0)
        for tt in BOTH:
            for u in BOTH:
                for f, r in ((f0, L * tt + H * u), (f1, L * tt + H * u + Q)):
                    f[pl.ds(4 * u + 2 * j + tt, Q, stride=8), :] = dz[r:r + Q, :]


def make_kernel(batch):
    def kernel(z_h, mask_h, tb_h, m_h, mt_h, bm_h, wd_h, bd_h, wm_h, bmb_h,
               loss_o, dz_o, dm_o, dwd_o, dbd_o, dwm_o, dbm_o, vl_o, tl_o, w2,
               zv, mv, mask_v, tb_v, mt_v, bm_v, wd_v, bd_v, wm_v, bmb_v,
               wt2, wmt, wmn, bias_c, mbias_c, lab, lts, ltp, ltr, l1n, l2n, t1o, t2o, t1r, t2r, mlab,
               cnt_s, cnt_r, rn, rz, f0, f1, ntn, ntf, vb, vr, db, dwd_acc, dwm_acc, dbd_acc, dbm_acc, nll_acc,
               ps, pa, ph, px, pc, pb, pf, es, ea, eh, ex, ec, eb, ef,
               lsem, cs, cr, ls, lr, ns, nr, zs, zr, vs, vrs, ars, arr, ready):
        dp = lax.axis_index("dp")
        d = lax.axis_index("dap")
        chip, core = d // 2, d % 2
        dap_peer = {1: chip * 2 + (1 - core), 2: (1 - chip) * 2 + core, 3: (1 - chip) * 2 + (1 - core)}
        pz, py = dp // 2, dp % 2
        dp_peer = {1: pz * 2 + (1 - py), 2: (1 - pz) * 2 + py, 3: (1 - pz) * 2 + (1 - py)}
        near = pl.multiple_of(chip * L, L)
        far = pl.multiple_of((1 - chip) * L, L)
        half = (chip, 1 - chip)
        phalf = (1 - chip, chip)
        base = {k: pl.multiple_of(H * dap_peer[k], H) for k in PEERS}

        loc = []
        for n, (src, dst) in enumerate([(mask_h, mask_v), (tb_h, tb_v), (bm_h, bm_v), (mt_h, mt_v), (wd_h, wd_v),
                                        (bd_h, bd_v), (wm_h, wm_v), (bmb_h, bmb_v), (m_h, mv), (z_h, zv)]):
            c = pltpu.make_async_copy(src, dst, lsem.at[n])
            c.start()
            loc.append(c)

        bar = pltpu.get_barrier_semaphore()
        for k in PEERS:
            pl.semaphore_signal(bar, inc=1, device_id=(dp, dap_peer[k]), device_id_type=MESH)
        for k in (1, 2):
            @pl.when(dp_peer[k] > 0)
            def _():
                for there in (d, dap_peer[1]):
                    pl.semaphore_signal(bar, inc=1, device_id=(dp_peer[k], there), device_id_type=MESH)

        for n in QUARTERS:
            loc[n].wait()
        maskf = mask_v[:].astype(F32)
        bertf = bm_v[:].astype(F32)
        cd = jnp.sum(jnp.sum(maskf, axis=0, keepdims=KEEP), axis=1, keepdims=KEEP)
        cm = jnp.sum(jnp.sum(bertf, axis=0, keepdims=KEEP), axis=1, keepdims=KEEP)
        cnt_s[:1, :] = jnp.broadcast_to(cd, (1, L))
        cnt_s[1:2, :] = jnp.broadcast_to(cm, (1, L))
        labv = jnp.where(mask_v[:] > 0, tb_v[:], H)
        lab[:] = labv
        labf = labv.astype(F32)
        lts[:] = jnp.concatenate([labf, labf], axis=0).T
        low = lax.broadcasted_iota(I32, (Q, L), 1) < H
        for p in QUARTERS:
            ltp[p] = jnp.where(low, lts[H * p:H * p + Q, :], lts[H * p + Q:H * p + H, :])

        pl.semaphore_wait(bar, 3 + 4 * ((dp + 3) // 4))
        for k in (1, 2):
            @pl.when(dp_peer[k] == 0)
            def _():
                for there in (d, dap_peer[1]):
                    pl.semaphore_signal(ready, inc=1, device_id=(dp_peer[k], there), device_id_type=MESH)

        def rcopy(src, dst, s, r, dpi, dapi):
            return pltpu.make_async_remote_copy(src_ref=src, dst_ref=dst, send_sem=s, recv_sem=r,
                                                device_id=(dpi, dapi), device_id_type=MESH)

        cc, lc, zc = {}, {}, {}
        for k in (2, 3, 1):
            cc[k] = rcopy(cnt_s, cnt_r.at[k - 1], cs.at[k - 1], cr.at[k - 1], dp, dap_peer[k])
            cc[k].start()
        for k in (2, 3, 1):
            lc[k] = rcopy(ltp.at[dap_peer[k]], ltr.at[k - 1],
                          ls.at[k - 1], lr.at[k - 1], dp, dap_peer[k])
            lc[k].start()
        nc = {}
        for q in QUARTERS:
            nc[q] = rcopy(z_h.at[:, pl.ds(pl.multiple_of(base[1] + 16 * q, 16), 16), :], rn.at[q],
                          ns.at[q], nr.at[q], dp, dap_peer[1])
            for k in FAR:
                for b in BOTH:
                    cols = pl.multiple_of(base[k] + Q * phalf[b] + 8 * q, 8)
                    zc[k, q, b] = rcopy(z_h.at[Q * b:Q * b + Q, pl.ds(cols, 8), :], rz.at[k - 2, q, b],
                                        zs.at[k - 2, q, b], zr.at[k - 2, q, b], dp, dap_peer[k])
                    zc[k, q, b].start()
            nc[q].start()
        for n in range(4, 8):
            loc[n].wait()
        wt = wd_v[:]
        nat = wt.astype(F32).T.astype(BF16)
        wt2[:L, :] = nat
        wt2[L:N, :] = nat
        w2[:H, :] = wt
        w2[H:L, :] = wt
        wmt[:] = jnp.zeros_like(wmt)
        wmt[:CLS, :] = wm_v[:]
        wmn[:] = wmt[:].astype(F32).T.astype(BF16)
        bias_c[:] = jnp.broadcast_to(row_to_col(bd_v[:], H), (H, L))
        pad = lax.broadcasted_iota(I32, (Q, 1), 0) >= CLS
        mbias_c[:] = jnp.broadcast_to(jnp.where(pad, -1e30, row_to_col(bmb_v[:], Q)), (Q, L))
        l1n[:] = lab[:, pl.ds(near, L)]
        mlv = jnp.where(bm_v[:] > 0, mt_v[:], H)
        bm_v[:] = mlv
        mlab[:] = jnp.concatenate([bm_v[pl.ds(0, Q, stride=2), :], bm_v[pl.ds(1, Q, stride=2), :]], axis=1)
        for a in (dwd_acc, dwm_acc, dbd_acc, dbm_acc, nll_acc):
            a[:] = jnp.zeros_like(a)

        for k in PEERS:
            cc[k].wait_recv()
        tot = (cnt_s[:] + cnt_r[0]) + (cnt_r[1] + cnt_r[2])
        den_d = DIST_EPS + tot[:1, :]
        den_m = MSA_EPS + tot[1:2, :]
        cvd = (LOSS_SCALE * DIST_WEIGHT / batch) / den_d
        cvm = (LOSS_SCALE * MSA_WEIGHT / batch) / den_m
        cd2 = jnp.concatenate([cvd, cvd], axis=1)
        cm2 = jnp.concatenate([cvm, cvm], axis=1)

        def fold(a):
            return a[:, :L] + a[:, L:N]


        loc[8].wait()

        def msa(i, carry):
            m = mv[pl.ds(pl.multiple_of(N * i, N), N), :]
            b = mbias_c[:]
            l = dot(m, wmn[:], 1, 0).T + jnp.concatenate([b, b], axis=1)
            t = lanes2(mlab, i)
            mx = jnp.max(l, axis=0, keepdims=KEEP)
            e = jnp.exp(l - mx)
            s = jnp.sum(e, axis=0, keepdims=KEEP)
            eq = lax.broadcasted_iota(I32, (Q, N), 0) == t
            mk = (t < H).astype(F32)
            c = cm2 * mk
            h = (e * (c / s) - jnp.where(eq, c, 0.0)).astype(BF16)
            lt = jnp.sum(jnp.where(eq, l, 0.0), axis=0, keepdims=KEEP)
            nll_acc[1:2, :] += fold(mk * (mx + jnp.log(s)) - lt)
            dbm_acc[:] += fold(h.astype(F32))
            dm_o[pl.ds(pl.multiple_of(N * i, N), N), :] = dot(h, wmt[:], 0, 0).astype(BF16)
            dwm_acc[:] += dot(h, m, 1, 0)
            return carry

        lax.fori_loop(0, 16, msa, 0, unroll=4)


        for k in PEERS:
            lc[k].wait_recv()
        def turn(a):
            return pltpu.roll(a, H, 1)

        def unpack(p):
            return jnp.concatenate([jnp.where(low, p, turn(p)), jnp.where(low, turn(p), p)], axis=0)

        def paired(a):
            back = jnp.concatenate([pltpu.roll(a[8 * q:8 * q + 8, :], 4, 0) for q in QUARTERS], axis=0)
            return jnp.where(low, a, back).astype(I32)

        lane = lax.broadcasted_iota(I32, (Q, L), 1)
        upper = (lane % H >= Q).astype(I32)
        mine_low = upper == chip
        peer_low = upper == 1 - chip
        wide = lax.broadcasted_iota(I32, (H, L), 1) < H
        own_lt = lts[pl.ds(pl.multiple_of(H * d, H), H), :]
        l2n[:] = jnp.where(wide == (core == 0), own_lt, unpack(ltr[0])).astype(I32)
        l1f = lab[:, pl.ds(far, L)].astype(F32)
        for k in FAR:
            a = jnp.where(wide == (dap_peer[k] % 2 == 0), l1f, turn(l1f))
            t1o[k - 2] = paired(jnp.where(mine_low, a[:Q, :], a[Q:H, :]))
            got = ltr[k - 1]
            t2o[k - 2] = paired(jnp.where(low == mine_low, got, turn(got)))
            sent = ltp[dap_peer[k]]
            t1r[k - 2] = paired(jnp.where(low == peer_low, sent, turn(sent)))
            u = unpack(got)
            u = jnp.concatenate([u, u], axis=0).T
            t2r[k - 2] = paired(jnp.where(peer_low, u[:Q, :], u[Q:H, :]))
            tl_o[0, k - 2] = t1r[k - 2, 8 * LAST:Q, :]
            tl_o[1, k - 2] = t2r[k - 2, 8 * LAST:Q, :]

        def swap(src, nt, q, off):
            chunk = src.astype(F32)
            f0[:] = chunk[:, :8, :].reshape(512, L)
            f1[:] = chunk[:, 8:16, :].reshape(512, L)
            for t in range(8):
                nt[16 * q + t, pl.ds(off, H), :] = f0[pl.ds(t, H, stride=8), :].astype(BF16)
                nt[16 * q + 8 + t, pl.ds(off, H), :] = f1[pl.ds(t, H, stride=8), :].astype(BF16)

        bins = lax.broadcasted_iota(I32, (H, N), 0)

        def softmax_terms(zx, nx):
            b = bias_c[:]
            l = dot(jnp.concatenate([zx, nx], axis=1), wt2[:], 1, 0).T + jnp.concatenate([b, b], axis=1)
            mx = jnp.max(l, axis=0, keepdims=KEEP)
            e = jnp.exp(l - mx)
            s = jnp.sum(e, axis=0, keepdims=KEEP)
            return l, e, s, mx + jnp.log(s)

        def near_tile(i, carry):
            zx = zv[pl.ds(2 * i, 2), pl.ds(near, L), :].reshape(N, L)
            nx = ntn[pl.ds(2 * i, 2), :, :].reshape(N, L)
            l, e, s, lse = softmax_terms(zx, nx)
            t1 = lanes2(l1n, i)
            t2 = lanes2(l2n, i)
            eq1 = bins == t1
            m1 = (t1 < H).astype(F32)
            c1 = cd2 * m1
            c2 = cd2 * (t2 < H).astype(F32)
            g1 = (e * (c1 / s) - jnp.where(eq1, c1, 0.0)).astype(BF16)
            g2 = (e * (c2 / s) - jnp.where(bins == t2, c2, 0.0)).astype(BF16)
            lt = jnp.sum(jnp.where(eq1, l, 0.0), axis=0, keepdims=KEEP)
            nll_acc[:1, :] += fold(m1 * lse - lt)
            dbd_acc[:] += fold(g1.astype(F32))
            g = jnp.concatenate([g1, g2], axis=0)
            dz_o[pl.ds(2 * i, 2), pl.ds(near, L), :] = dot(g, w2[:], 0, 0).astype(BF16).reshape(2, L, L)
            dwd_acc[:] += dot(g, zx, 1, 0)
            return carry

        def own_tiles(k, q):
            for b in BOTH:
                zc[k, q, b].wait_recv()
                f0[:N, :] = rz[k - 2, q, b].astype(F32).reshape(N, L)
                for t in range(8):
                    r = H * (t // 4) + Q * b
                    ntf[k - 2, 4 * q + t % 4, r:r + Q, :] = f0[pl.ds(t, Q, stride=8), :].astype(BF16)

            def body(j, carry):
                spots = [(8 * q + 4 * u + 2 * j + tt + Q * half[b], pl.multiple_of(base[k] + Q * b, Q))
                         for tt in BOTH for u in BOTH for b in BOTH]
                zx = jnp.concatenate([zv[r, pl.ds(c, Q), :] for r, c in spots], axis=0)
                nx = ntf[k - 2, pl.ds(4 * q + 2 * j, 2), :, :].reshape(N, L)
                l, e, s, lse = softmax_terms(zx, nx)
                t1 = lanes2(t1o.at[k - 2], 4 * q + j)
                t2 = lanes2(t2o.at[k - 2], 4 * q + j)
                eq1 = bins == t1
                eq2 = bins == t2
                m1 = (t1 < H).astype(F32)
                m2 = (t2 < H).astype(F32)
                v = e * (cd2 / s)
                w = v - cd2
                d1 = jnp.sum(jnp.where(eq1, w, 0.0), axis=0, keepdims=KEEP)
                d2 = jnp.sum(jnp.where(eq2, w, 0.0), axis=0, keepdims=KEEP)
                g1 = (jnp.where(eq1, w, v) * m1).astype(BF16)
                g2 = (jnp.where(eq2, w, v) * m2).astype(BF16)
                lt = jnp.sum(jnp.where(eq1, l, 0.0) + jnp.where(eq2, l, 0.0), axis=0, keepdims=KEEP)
                nll_acc[:1, :] += fold((m1 + m2) * lse - lt)
                dbd_acc[:] += fold(g1.astype(F32) + g2.astype(F32))
                vh = v.astype(BF16)
                for tt in BOTH:
                    cut = slice(L * tt, L * tt + L)
                    vb[k - 2, q, pl.ds(pl.multiple_of(L * j + H * tt, H), H), :] = vh[:, cut]
                    db[k - 2, q, pl.ds(2 * j + tt, 1), :] = d1[:, cut]
                    db[k - 2, q, pl.ds(4 + 2 * j + tt, 1), :] = d2[:, cut]
                g = jnp.concatenate([g1, g2], axis=0)
                dz = dot(g, w2[:], 0, 0).astype(BF16)
                for n, (r, c) in enumerate(spots):
                    dz_o[r, pl.ds(c, Q), :] = dz[Q * n:Q * n + Q, :]
                dwd_acc[:] += dot(g, zx, 1, 0) + dot(g, nx, 1, 0)
                return carry

            lax.fori_loop(0, 2, body, 0, unroll=2)
            vb[k - 2, q, N:, :] = db[k - 2, q].astype(BF16)

        vc = {}

        def give(k, q, when):
            unit = 2 * q + k - 2
            if when == SENT:
                v_to = vr.at[k - 2, q] if q < LAST else vl_o.at[k - 2]
                vc[k, q] = rcopy(vb.at[k - 2, q], v_to, vs.at[k - 2, q], vrs.at[k - 2, q], dp, dap_peer[k])

            def start():
                vc[k, q].start()

            if (unit < EARLY) == when and unit not in SPLIT:
                start()
            if unit in SPLIT:
                pl.when((dp == 0) if when == SENT else (dp > 0))(start)

        def take(k, q):
            vc[k, q].wait_recv()
            returned_pairs(vr.at[k - 2, q], t1r.at[k - 2], t2r.at[k - 2], 4 * q, w2, f0, f1)
            for b, f in ((0, f0), (1, f1)):
                cols = pl.multiple_of(base[k] + Q * phalf[b] + 8 * q, 8)
                dz_o[Q * b:Q * b + Q, pl.ds(cols, 8), :] = f[:N, :].reshape(Q, 8, L).astype(BF16)

        def reduction(src, ra, rh, rx, rc, rb, full, first):
            n = rh.shape[0]
            mine = pl.ds(pl.multiple_of(n * core, 8), n)
            other = pl.ds(pl.multiple_of(n * (1 - core), 8), n)

            def trio(halves, a, dst, sem, k):
                there = ((dp, dap_peer[1]), (dp_peer[k], d), (dp_peer[k], dap_peer[1]))
                group = [rcopy(a.at[rows, :], dst.at[m], ars.at[sem + m], arr.at[sem + m], *to)
                         for m, (rows, to) in enumerate(zip(halves, there))]
                for c in group:
                    c.start()
                return group

            one = trio((other, mine, other), src, ra, first, 1)
            yield
            for c in one:
                c.wait_recv()
            rh[:] = (src[mine, :] + ra[0]) + (ra[1] + ra[2])
            two = rcopy(rh, rx, ars.at[first + 6], arr.at[first + 6], dp, dap_peer[2])
            two.start()
            yield
            two.wait_recv()
            rc[:] = rh[:] + rx[:]
            three = trio((pl.ds(0, n),) * 3, rc, rb, first + 3, 2)
            yield
            for c in three:
                c.wait_recv()
            full[mine, :] = rc[:] + rb[1]
            full[other, :] = rb[0] + rb[2]
            for c in (*one, two, *three):
                c.wait_send()
            yield

        end = lax.broadcasted_iota(I32, (1, L), 1) == L - 1
        es[:CLS, :] = dwm_acc[:CLS, :L]
        es[CLS:2 * CLS, :] = dwm_acc[:CLS, L:N]
        nm = jnp.sum(nll_acc[1:2, :], axis=1, keepdims=KEEP)
        part = MSA_WEIGHT * nm / den_m / batch
        es[2 * CLS:47, :] = col_to_row(jnp.sum(dbm_acc[:], axis=1, keepdims=KEEP), L) + jnp.where(end, part, 0.0)
        es[47:48, :] = jnp.zeros((1, L), F32)

        @pl.when(dp == 0)
        def _():
            pl.semaphore_wait(ready, 4)

        soon = reduction(es, ea, eh, ex, ec, eb, ef, 7)
        next(soon)

        own_off = pl.multiple_of(H * core, H)
        oth_off = pl.multiple_of(H * (1 - core), H)
        loc[9].wait()
        for q in QUARTERS:
            swap(zv[:, pl.ds(pl.multiple_of(H * d + 16 * q, 16), 16), :], ntn, q, own_off)
        for q in QUARTERS:
            nc[q].wait_recv()
            swap(rn[q], ntn, q, oth_off)
        lax.fori_loop(0, Q, near_tile, 0, unroll=4)

        next(soon)
        for q in QUARTERS:
            for k in FAR:
                own_tiles(k, q)
                give(k, q, SENT)

        wd = ps.shape[0]
        ps[:H, :] = dwd_acc[:H, :] + dwd_acc[H:L, :]
        ps[H:wd, :] = jnp.zeros((wd - H, L), F32)
        nd = jnp.sum(nll_acc[:1, :], axis=1, keepdims=KEEP)
        part = DIST_WEIGHT * nd / den_d / batch
        ps[H:H + 1, :] = col_to_row(jnp.sum(dbd_acc[:], axis=1, keepdims=KEEP), L) + jnp.where(end, part, 0.0)
        late = reduction(ps, pa, ph, px, pc, pb, pf, 0)
        next(late)
        next(soon)
        next(late)
        for q in QUARTERS:
            for k in FAR:
                give(k, q, KEPT)
        for k in FAR:
            take(k, 0)
        next(soon)
        next(late)
        for k in FAR:
            take(k, 1)
        for k in FAR:
            take(k, 2)
        next(late)
        for k in FAR:
            vc[k, LAST].wait_recv()
        dwd_o[:] = pf[:H, :]
        dwm_o[:, :L] = ef[:CLS, :]
        dwm_o[:, L:N] = ef[CLS:2 * CLS, :]
        row = pf[H:H + 1, :]
        mrow = ef[2 * CLS:47, :]
        dbd_o[:] = row[:, :H]
        dbm_o[:] = mrow[:, :CLS]
        loss_o[:] = pltpu.roll(row + mrow, 1, 1)[:, :1]

        for k in PEERS:
            cc[k].wait_send()
            lc[k].wait_send()
        for c in (*nc.values(), *zc.values(), *vc.values()):
            c.wait_send()

    return kernel


def flush_kernel(loss_i, dz_i, dm_i, dwd_i, dbd_i, dwm_i, dbm_i, vl, tl, w2,
                 loss_o, dz_o, dm_o, dwd_o, dbd_o, dwm_o, dbm_o, f0, f1, late, sem):
    d = lax.axis_index("dap")
    chip, core = d // 2, d % 2
    phalf = (1 - chip, chip)
    copies = []

    def put(src, dst):
        c = pltpu.make_async_copy(src, dst, sem.at[len(copies)])
        c.start()
        copies.append(c)

    def put_dz(r, rows, c, cols):
        put(dz_i.at[pl.ds(r, rows), pl.ds(c, cols), :], dz_o.at[pl.ds(r, rows), pl.ds(c, cols), :])

    for n in QUARTERS:
        put(dm_i.at[pl.ds(KIB * n, KIB), :], dm_o.at[pl.ds(KIB * n, KIB), :])
    for n in QUARTERS:
        put_dz(16 * n, 16, pl.multiple_of(L * chip, L), L)
    spots = {}
    for k, there in ((0, core), (1, 1 - core)):
        start = pl.multiple_of((1 - chip) * L + H * there, H)
        for b in BOTH:
            mid = pl.multiple_of(start + Q * phalf[b], Q)
            put_dz(Q * b, Q, mid, 24)
            put_dz(Q * b, Q, pl.multiple_of(start + Q * phalf[1 - b], Q), Q)
            spots[k, b] = pl.multiple_of(mid + 24, 8)
    for src, dst in ((loss_i, loss_o), (dwd_i, dwd_o), (dbd_i, dbd_o), (dwm_i, dwm_o), (dbm_i, dbm_o)):
        put(src, dst)
    for k in BOTH:
        returned_pairs(vl.at[k], tl.at[0, k], tl.at[1, k], 0, w2, f0, f1)
        for b, f in ((0, f0), (1, f1)):
            late[k, b] = f[:].reshape(Q, 8, L).astype(BF16)
            put(late.at[k, b], dz_o.at[pl.ds(Q * b, Q), pl.ds(spots[k, b], 8), :])
    for c in copies:
        c.wait()


def solution(mesh):
    dp_size = mesh.shape["dp"]
    pair_spec = P("dp", "dap", None, None)
    pair_int_spec = P("dp", "dap", None)
    msa_spec = P("dp", None, "dap", None)
    msa_int_spec = P("dp", None, "dap")
    V = pltpu.VMEM

    def local_step(z, mask, tb, m, mt, bm, wd, bd, wm, bmb):
        args = (z.reshape(H, N, L), mask.reshape(H, N), tb.reshape(H, N), m.reshape(4096, N),
                mt.reshape(H, H), bm.reshape(H, H), wd.T, bd.reshape(1, H), wm.T, bmb.reshape(1, CLS))
        args = tuple(pltpu.with_memory_space_constraint(a, pltpu.HBM) for a in args)
        shapes = [((1, 1), F32), ((H, N, L), BF16), ((4096, N), BF16), ((H, L), F32), ((1, H), F32),
                  ((CLS, N), F32), ((1, CLS), F32)]
        scratch = [
            V((H, N, L), BF16), V((4096, N), BF16), *[V((H, N), I32)] * 2, V((H, H), I32),
            V((H, H), I32), V((H, L), BF16), V((1, H), F32), V((CLS, N), BF16), V((1, CLS), F32),
            V((N, H), BF16), V((Q, N), BF16), V((N, Q), BF16), V((H, L), F32), V((Q, L), F32),
            V((H, N), I32), V((N, L), F32), V((4, Q, L), F32), V((3, Q, L), F32), V((H, L), I32), V((H, L), I32),
            *[V((2, Q, L), I32)] * 4, V((Q, L), I32),
            V((2, L), F32), V((3, 2, L), F32), V((4, H, 16, L), BF16), V((2, 4, 2, Q, 8, L), BF16),
            V((512, L), F32), V((512, L), F32), V((H, L, L), BF16), V((2, 16, L, L), BF16),
            V((2, 4, N + 8, L), BF16), V((2, 3, N + 8, L), BF16), V((2, 4, 8, L), F32),
            V((L, L), F32), V((Q, N), F32), V((H, L), F32), V((Q, L), F32), V((8, L), F32),
            *(V((*lead, rows * n, L), F32) for n in (40, 24)
              for lead, rows in (((), 2), ((3,), 1), ((), 1), ((), 1), ((), 1), ((3,), 1), ((), 2))),
            DSEM((10,)), *[DSEM((3,))] * 4, DSEM((4,)), DSEM((4,)),
            *[DSEM((2, 4, 2))] * 2, *[DSEM((2, 4))] * 2,
            *[DSEM((14,))] * 2, pltpu.SemaphoreType.REGULAR,
        ]
        extra = [((2, N + 8, L), BF16), ((2, 2, 8, L), I32), ((L, L), BF16)]
        vmem = [pl.BlockSpec(memory_space=pltpu.VMEM)]
        hbm = [pl.BlockSpec(memory_space=pltpu.HBM)]
        outs = pl.pallas_call(
            make_kernel(dp_size),
            out_shape=[pltpu.VMEM(s, t) for s, t in shapes + extra],
            in_specs=hbm * 10,
            out_specs=vmem * 10,
            scratch_shapes=scratch,
            compiler_params=pltpu.CompilerParams(collective_id=0, has_side_effects=True,
                                                 vmem_limit_bytes=44 * KIB * KIB),
        )(*args)
        outs = pl.pallas_call(
            flush_kernel,
            out_shape=[jax.ShapeDtypeStruct(s, t) for s, t in shapes],
            in_specs=vmem * 10,
            out_specs=hbm * 7,
            scratch_shapes=[V((N, L), F32), V((N, L), F32), V((2, 2, Q, 8, L), BF16), DSEM((25,))],
            compiler_params=pltpu.CompilerParams(vmem_limit_bytes=8 * KIB * KIB),
        )(*outs)
        loss, dz, dm, dwd, dbd, dwm, dbm = outs
        return (loss.reshape(()), dz.reshape(1, H, N, L), dm.reshape(1, H, H, N), dwd.T, dbd.reshape(H),
                dwm.T, dbm.reshape(CLS))

    return jax.shard_map(local_step, mesh=mesh,
                         in_specs=(pair_spec, pair_int_spec, pair_int_spec, msa_spec, msa_int_spec, msa_int_spec,
                                   P(), P(), P(), P()),
                         out_specs=(P(), pair_spec, msa_spec, P(), P(), P(), P()),
                         check_vma=False)
```
